32 devices in a mesh: row: 2 (over y), phi: 16 (over z, x, core).
Axes of the slice: x: 2, y: 2, z: 4, core: 2. Of those that a mesh axis runs over, the one named last changes fastest.
Arguments:
- density: float32 [32, 2048, 512], P('row', 'phi'), may hold values from 0.3 to 3
- velocity: float32 [3, 32, 2048, 512], P(None, 'row', 'phi'), may hold values from -3 to 3
- magnetic: float32 [3, 32, 2048, 512], P(None, 'row', 'phi'), may hold values from -6 to 6
Outputs:
- density_next: float32 [32, 2048, 512], P('row', 'phi')
- magnetic_next: float32 [3, 32, 2048, 512], P(None, 'row', 'phi')
The draws below stay inside these ranges and needn't reach their ends.
All inputs are finite; a program needn't handle non-finite values.
Results may differ from the reference program's by a relative error of at most 0.0003.
Values sent between devices are 32-bit elements; how exact they have to be, the bound alone decides.
A program may use at most 256 MiB of HBM per device.

```python
import math
from functools import partial
import jax
import jax.numpy as jnp
from jax import lax

NP = 2048
NT = 512
NPOL = 128
NR = 32


def block_levels(key, dims, shards, low, largest):
    factor_of = 1.0
    for dim, parts in shards:
        draws = jax.random.uniform(jax.random.fold_in(jax.random.fold_in(key, 6), dim), (parts,), jnp.float32, low / len(shards), largest / len(shards))
        factor_of = factor_of * jnp.repeat(jnp.exp(draws), dims[dim] // parts).reshape((-1,) + (1,) * (len(dims) - 1 - dim))
    return factor_of


def centred(own_key, extent, scale, most, split=(), dtype=jnp.bfloat16):
    result = jax.random.normal(own_key, extent, jnp.float32) * scale
    if len(split) > 0:
        result = block_levels(own_key, extent, split, -0.22, 0.18) * result
    return jnp.clip(result, min=-most, max=most).astype(dtype)


def setup_inputs(seed: int = 0) -> dict:
    arg_keys = jax.random.split(jax.random.key(seed), 4)
    return {
        "density": jnp.clip(jnp.exp(math.log(3.0) - 2.3025851 * jax.random.uniform(arg_keys[0], (NR, NP, NT), jnp.float32) ** block_levels(arg_keys[0], (NR, NP, NT), ((0, 2), (1, 16)), -0.2, 0.2)), 0.3, 3.0),
        "velocity": centred(arg_keys[1], (3, NR, NP, NT), 0.5, 3.0, ((1, 2), (2, 16)), jnp.float32),
        "magnetic": centred(arg_keys[2], (3, NR, NP, NT), 1.0, 6.0, ((1, 2), (2, 16)), jnp.float32),
    }


COURANT_RAD = 0.3
COURANT_POL = 0.25
COURANT_AZI = 0.35
SOUND_SPEED = 1.0


def shift_theta(values, offset):
    if offset == 0:
        return values
    if offset > 0:
        border = jnp.repeat(values[..., -1:], offset, axis=-1)
        return jnp.concatenate([values[..., offset:], border], axis=-1)
    border = jnp.repeat(values[..., :1], -offset, axis=-1)
    return jnp.concatenate([border, values[..., :offset]], axis=-1)


def interface_value(outer_left, inner_left, inner_right, outer_right):
    guess = (7.0 / 12.0) * (inner_left + inner_right) - (1.0 / 12.0) * (outer_left + outer_right)
    return jnp.clip(guess, jnp.minimum(inner_left, inner_right), jnp.maximum(inner_left, inner_right))


def edge_values(nearby):
    centre = nearby(0)
    left_face = interface_value(nearby(-2), nearby(-1), centre, nearby(1))
    right_face = interface_value(nearby(-1), centre, nearby(1), nearby(2))
    to_left = left_face - centre
    to_right = right_face - centre
    left_limited = jnp.clip(to_left, -2.0 * jnp.abs(to_right), 2.0 * jnp.abs(to_right))
    right_limited = jnp.clip(to_right, -2.0 * jnp.abs(to_left), 2.0 * jnp.abs(to_left))
    return centre + left_limited, centre + right_limited


def hll_flux(dens_left, dens_right, speed_left, speed_right):
    slowest = jnp.minimum(jnp.minimum(speed_left, speed_right) - SOUND_SPEED, 0.0)
    fastest = jnp.maximum(jnp.maximum(speed_left, speed_right) + SOUND_SPEED, 0.0)
    upwind = fastest * dens_left * speed_left - slowest * dens_right * speed_right
    return (upwind + slowest * fastest * (dens_right - dens_left)) / (fastest - slowest)


def axis_divergence(dens, speed, axis, count, ghost):
    def picker(field):
        def nearby(offset):
            return lax.slice_in_dim(field, ghost - 1 + offset, ghost + 1 + offset + count, axis=axis)
        return nearby

    def window(values, start, stop):
        return lax.slice_in_dim(values, start, stop, axis=axis)

    dens_left, dens_right = edge_values(picker(dens))
    speed_left, speed_right = edge_values(picker(speed))
    flux = hll_flux(window(dens_right, 0, count + 1), window(dens_left, 1, count + 2),
                    window(speed_right, 0, count + 1), window(speed_left, 1, count + 2))
    return window(flux, 1, count + 1) - window(flux, 0, count)


def theta_divergence(dens, speed):
    dens_left, dens_right = edge_values(partial(shift_theta, dens))
    speed_left, speed_right = edge_values(partial(shift_theta, speed))
    flux = hll_flux(shift_theta(dens_right, -1), dens_left, shift_theta(speed_right, -1), speed_left)
    position = lax.broadcasted_iota(jnp.int32, flux.shape, flux.ndim - 1)
    flux = jnp.where(position == 0, jnp.zeros_like(flux), flux)
    upper_flux = jnp.concatenate([flux[..., 1:], jnp.zeros_like(flux[..., :1])], axis=-1)
    return upper_flux - flux


def advance(primitive, magnetic, ghost, face_ghost, radial, azimuth):
    dens = primitive[0]
    radial_speed = primitive[1]
    polar_speed = primitive[2]
    azimuth_speed = primitive[3]

    def inner(values, width):
        return values[width:width + radial, width:width + azimuth]

    def box(values, width):
        return values[width - 1:width + radial + 1, width - 1:width + azimuth + 1]

    rad_term = axis_divergence(dens[:, ghost:ghost + azimuth], radial_speed[:, ghost:ghost + azimuth], 0, radial, ghost)
    azi_term = axis_divergence(dens[ghost:ghost + radial], azimuth_speed[ghost:ghost + radial], 1, azimuth, ghost)
    dens_inner = inner(dens, ghost)
    pol_term = theta_divergence(dens_inner, inner(polar_speed, ghost))
    density_next = dens_inner - COURANT_RAD * rad_term - COURANT_POL * pol_term - COURANT_AZI * azi_term

    radial_span = magnetic[0][face_ghost - 1:face_ghost + radial + 2, face_ghost - 1:face_ghost + azimuth + 1]
    radial_cell = 0.5 * (radial_span[:-1] + radial_span[1:])
    azimuth_span = magnetic[2][face_ghost - 1:face_ghost + radial + 1, face_ghost - 1:face_ghost + azimuth + 2]
    azimuth_cell = 0.5 * (azimuth_span[:, :-1] + azimuth_span[:, 1:])
    polar_box = box(magnetic[1], face_ghost)
    polar_cell = 0.5 * (polar_box + shift_theta(polar_box, 1))
    speed_r = box(radial_speed, ghost)
    speed_t = box(polar_speed, ghost)
    speed_p = box(azimuth_speed, ghost)
    radial_emf = -(speed_t * azimuth_cell - speed_p * polar_cell)
    polar_emf = -(speed_p * radial_cell - speed_r * azimuth_cell)
    azimuth_emf = -(speed_r * polar_cell - speed_t * radial_cell)

    radial_edge = 0.5 * (radial_emf[1:radial + 1, :-1] + radial_emf[1:radial + 1, 1:])
    radial_below = 0.5 * (shift_theta(radial_edge, -1) + radial_edge)
    radial_above = 0.5 * (radial_edge + shift_theta(radial_edge, 1))
    azimuth_edge = 0.5 * (azimuth_emf[:-1, 1:azimuth + 1] + azimuth_emf[1:, 1:azimuth + 1])
    azimuth_below = 0.5 * (shift_theta(azimuth_edge, -1) + azimuth_edge)
    azimuth_above = 0.5 * (azimuth_edge + shift_theta(azimuth_edge, 1))
    polar_edge = 0.25 * (polar_emf[:-1, :-1] + polar_emf[1:, :-1] + polar_emf[:-1, 1:] + polar_emf[1:, 1:])

    radial_next = inner(magnetic[0], face_ghost) - COURANT_POL * (azimuth_above[:radial] - azimuth_below[:radial]) \
        + COURANT_AZI * (polar_edge[:radial, 1:] - polar_edge[:radial, :-1])
    polar_next = inner(magnetic[1], face_ghost) - COURANT_AZI * (radial_below[:, 1:] - radial_below[:, :-1]) \
        + COURANT_RAD * (azimuth_below[1:] - azimuth_below[:-1])
    azimuth_next = inner(magnetic[2], face_ghost) - COURANT_RAD * (polar_edge[1:, :azimuth] - polar_edge[:-1, :azimuth]) \
        + COURANT_POL * (radial_above[:, :azimuth] - radial_below[:, :azimuth])
    return density_next, jnp.stack([radial_next, polar_next, azimuth_next])


def pad_reference(values, width):
    values = jnp.pad(values, ((0, 0), (width, width), (0, 0), (0, 0)), mode="edge")
    return jnp.pad(values, ((0, 0), (0, 0), (width, width), (0, 0)), mode="wrap")


def reference(density, velocity, magnetic):
    half_polar = NPOL // 2
    primitive = jnp.concatenate([density[None], velocity], axis=0)
    polar_rows = jnp.concatenate([primitive[..., :half_polar], primitive[..., NT - half_polar:]], axis=-1)
    theta_row = jnp.concatenate([jnp.arange(half_polar), jnp.arange(NT - half_polar, NT)]).astype(jnp.float32)
    row_sine = jnp.sin(jnp.pi * (theta_row + 0.5) / NT)
    edge_sine = jnp.sin(jnp.pi * (half_polar + 0.5) / NT)
    mode_sine = jnp.sin(jnp.pi * jnp.arange(NP // 2 + 1).astype(jnp.float32) / NP)
    row_square = (row_sine * row_sine)[None, :]
    mode_square = (edge_sine * mode_sine)[:, None]
    damping = row_square / jnp.maximum(row_square, mode_square * mode_square)
    spectrum = jnp.fft.rfft(polar_rows, axis=2)
    smoothed = jnp.fft.irfft(spectrum * damping[None, None], n=NP, axis=2).astype(jnp.float32)
    primitive = jnp.concatenate([smoothed[..., :half_polar], primitive[..., half_polar:NT - half_polar],
                                 smoothed[..., half_polar:]], axis=-1)
    state = pad_reference(jnp.concatenate([primitive, magnetic], axis=0), 3)
    return advance(state[:4], state[4:], 3, 3, NR, NP)
```

```python
import math

import jax
import jax.numpy as jnp
import numpy as np
from jax import lax
from jax.experimental import pallas as pl
from jax.experimental.pallas import tpu as pltpu
from jax.sharding import PartitionSpec as P

NPOL = 128
RADIX = 16
FRONT = 16
TILE = 8
HALO = 8
REACH = 3

COURANT_RAD = 0.3
COURANT_POL = 0.25
COURANT_AZI = 0.35
SOUND_SPEED = 1.0


def rotate(value, angle):
    re, im = value
    c, s = math.cos(angle), math.sin(angle)
    if im is None:
        return (re * c, re * s)
    return (re * c - im * s, re * s + im * c)


def add(a, b, sign=1.0):
    def part(x, y):
        if y is None:
            return x
        if x is None:
            return y if sign > 0 else -y
        return x + y if sign > 0 else x - y

    return (part(a[0], b[0]), part(a[1], b[1]))


def conj(a):
    return (a[0], None if a[1] is None else -a[1])


def real_fft(xs):
    n = len(xs)
    if n == 1:
        return [(xs[0], None)]
    if n == 2:
        return [(xs[0] + xs[1], None), (xs[0] - xs[1], None)]
    even, odd = real_fft(xs[0::2]), real_fft(xs[1::2])
    half = n // 2

    def at(spec, k):
        return spec[k] if k <= half // 2 else conj(spec[half - k])

    result = []
    for k in range(half + 1):
        e, o = at(even, k % half), at(odd, k % half)
        if k == 0:
            result.append(add(e, o))
        elif k == half:
            result.append(add(e, o, -1.0))
        elif 4 * k == n:
            result.append((e[0], -o[0]))
        else:
            result.append(add(e, rotate(o, -2.0 * math.pi * k / n)))
    return result


def real_ifft(spec, n):
    if n == 2:
        a, b = spec[0][0], spec[1][0]
        return [a + b, a - b]
    half = n // 2
    even, odd = [], []
    for k in range(half // 2 + 1):
        a, b = spec[k], conj(spec[half - k])
        if k == 0:
            a, b = (spec[0][0], None), (spec[half][0], None)
            even.append(add(a, b))
            odd.append(add(a, b, -1.0))
        elif 4 * k == n:
            even.append((2.0 * spec[k][0], None))
            odd.append((-2.0 * spec[k][1], None))
        else:
            even.append(add(a, b))
            odd.append(rotate(add(a, b, -1.0), 2.0 * math.pi * k / n))
    evens, odds = real_ifft(even, half), real_ifft(odd, half)
    return [v for pair in zip(evens, odds) for v in pair]


def filter_tables(cells, theta_count):
    inner = cells // RADIX
    half_polar = NPOL // 2
    k2 = np.arange(RADIX // 2 + 1)[:, None]
    mode = k2 + RADIX * np.arange(inner)[None, :]
    angle = 2.0 * np.pi / cells * ((mode[:, :, None] * np.arange(inner)) % cells)
    cos, sin = np.cos(angle), np.sin(angle)
    forward = np.concatenate(
        [np.concatenate([cos, sin], 2), np.concatenate([-sin, cos], 2)], 1
    ).astype(np.float32)
    rows = np.arange(NPOL)
    theta = np.where(rows < half_polar, rows, theta_count - NPOL + rows)
    row_square = np.sin(np.pi * (theta + 0.5) / theta_count) ** 2
    edge = np.sin(np.pi * (half_polar + 0.5) / theta_count)
    mode_square = (edge * np.sin(np.pi * mode / cells)) ** 2
    damping = row_square / np.maximum(row_square, mode_square[:, :, None])
    return forward, (damping / cells).astype(np.float32)


def filter_kernel(group, inner, blocks, x_ref, basis_ref, damp_ref, out_ref):
    devices, _, azimuth, _ = x_ref.shape

    def slab(d):
        parts = [
            x_ref[d * blocks : (d + 1) * blocks, g].reshape(inner, NPOL) for g in range(group)
        ]
        return jnp.concatenate(parts, axis=1) if group > 1 else parts[0]

    spectrum = real_fft([slab(d) for d in range(RADIX)])
    filtered = []
    for k, (re, im) in enumerate(spectrum):
        basis = basis_ref[k]
        if im is None:
            forward = basis[:, :inner]
            stacked = re
        else:
            forward = basis
            stacked = jnp.concatenate([re, im], axis=0)
        modes = jnp.dot(
            forward, stacked, precision=lax.Precision.HIGHEST, preferred_element_type=jnp.float32
        )
        damp = damp_ref[k]
        damp = jnp.concatenate([damp, damp], axis=0)
        if group > 1:
            damp = jnp.concatenate([damp] * group, axis=1)
        back = lax.dot_general(
            forward,
            modes * damp,
            (((0,), (0,)), ((), ())),
            precision=lax.Precision.HIGHEST,
            preferred_element_type=jnp.float32,
        )
        filtered.append((back, None) if im is None else (back[:inner], back[inner:]))
    for d, value in enumerate(real_ifft(filtered, RADIX)):
        for g in range(group):
            out_ref[d * blocks : (d + 1) * blocks, g, :azimuth] = value[
                :, g * NPOL : (g + 1) * NPOL
            ].reshape(blocks, azimuth, NPOL)
    blank = jnp.zeros((HALO - 2 * REACH, NPOL), jnp.float32)
    for d in range(devices):
        for g in range(group):
            below = out_ref[(d - 1) % devices, g, azimuth - REACH : azimuth]
            above = out_ref[(d + 1) % devices, g, :REACH]
            out_ref[d, g, azimuth:] = jnp.concatenate([below, above, blank], axis=0)


def filter_lines(lines, theta_count):
    devices, pairs, azimuth, _ = lines.shape
    cells = devices * azimuth
    inner = cells // RADIX
    blocks = inner // azimuth
    group = 2 if pairs % 2 == 0 else 1
    forward, damping = filter_tables(cells, theta_count)
    spec = pl.BlockSpec((devices, group, azimuth, NPOL), lambda p: (0, p, 0, 0))
    out = pl.BlockSpec((devices, group, azimuth + HALO, NPOL), lambda p: (0, p, 0, 0))
    return pl.pallas_call(
        lambda *refs: filter_kernel(group, inner, blocks, *refs),
        grid=(pairs // group,),
        in_specs=[
            spec,
            pl.BlockSpec(forward.shape, lambda p: (0, 0, 0)),
            pl.BlockSpec(damping.shape, lambda p: (0, 0, 0)),
        ],
        out_specs=out,
        out_shape=jax.ShapeDtypeStruct((devices, pairs, azimuth + HALO, NPOL), jnp.float32),
        compiler_params=pltpu.CompilerParams(vmem_limit_bytes=56 * 1024 * 1024),
        cost_estimate=pl.CostEstimate(
            flops=32 * inner * cells * NPOL * pairs, bytes_accessed=8 * lines.size, transcendentals=0
        ),
        name="polar_filter",
    )(lines, jnp.asarray(forward), jnp.asarray(damping))


def pack_lines(density, velocity, first, layers):
    _, azimuth, width = density.shape
    half = NPOL // 2
    last = width // NPOL - 1
    step = 2 if layers % 2 == 0 and first % 2 == 0 else 1

    def kernel(d0, d1, v0, v1, out):
        lane = lax.broadcasted_iota(jnp.int32, (azimuth, NPOL), 1)
        for i in range(step):
            out[0, i] = jnp.where(lane < half, d0[i], d1[i])
            for c in range(3):
                out[1 + c, i] = jnp.where(lane < half, v0[c, i], v1[c, i])

    def dens(tile):
        return pl.BlockSpec((step, azimuth, NPOL), lambda t: (first // step + t, 0, tile))

    def vel(tile):
        return pl.BlockSpec((3, step, azimuth, NPOL), lambda t: (0, first // step + t, 0, tile))

    return pl.pallas_call(
        kernel,
        grid=(layers // step,),
        in_specs=[dens(0), dens(last), vel(0), vel(last)],
        out_specs=pl.BlockSpec((4, step, azimuth, NPOL), lambda t: (0, t, 0, 0)),
        out_shape=jax.ShapeDtypeStruct((4, layers, azimuth, NPOL), jnp.float32),
        name="pack_lines",
    )(density, density, velocity, velocity)


def pack_sides(density, velocity, magnetic):
    radial, azimuth, width = density.shape
    last = azimuth // TILE - 1

    def kernel(d0, d1, v0, v1, m0, m1, low, high):
        def rows(dens, vel, mag, pick, wide):
            parts = [dens[0, pick(REACH)], vel[2, 0, pick(REACH)], vel[0, 0, pick(1)], vel[1, 0, pick(1)]]
            parts += [mag[0, 0, pick(1)], mag[1, 0, pick(1)], mag[2, 0, pick(wide)]]
            used = sum(p.shape[0] for p in parts)
            parts.append(jnp.zeros((PACKED - used, width), jnp.float32))
            return jnp.concatenate(parts, axis=0)

        low[0] = rows(d0, v0, m0, lambda n: slice(0, n), 2)
        high[0] = rows(d1, v1, m1, lambda n: slice(TILE - n, TILE), 1)

    def three(b):
        return pl.BlockSpec((3, 1, TILE, width), lambda t: (0, t, b, 0))

    def one(b):
        return pl.BlockSpec((1, TILE, width), lambda t: (t, b, 0))

    return pl.pallas_call(
        kernel,
        grid=(radial,),
        in_specs=[one(0), one(last), three(0), three(last), three(0), three(last)],
        out_specs=[pl.BlockSpec((1, PACKED, width), lambda t: (t, 0, 0))] * 2,
        out_shape=[jax.ShapeDtypeStruct((radial, PACKED, width), jnp.float32)] * 2,
        name="pack_sides",
    )(density, density, velocity, velocity, magnetic, magnetic)


def interface_value(outer_left, inner_left, inner_right, outer_right):
    guess = 7.0 / 12.0 * (inner_left + inner_right) - 1.0 / 12.0 * (outer_left + outer_right)
    low = jnp.minimum(inner_left, inner_right)
    return jnp.minimum(jnp.maximum(guess, low), jnp.maximum(inner_left, inner_right))


def limited(centre, left_face, right_face):
    to_left = left_face - centre
    to_right = right_face - centre
    reach_right = 2.0 * jnp.abs(to_right)
    reach_left = 2.0 * jnp.abs(to_left)
    left = jnp.minimum(jnp.maximum(to_left, -reach_right), reach_right)
    right = jnp.minimum(jnp.maximum(to_right, -reach_left), reach_left)
    return centre + left, centre + right


def edges(q):
    left_face = interface_value(q[0], q[1], q[2], q[3])
    right_face = interface_value(q[1], q[2], q[3], q[4])
    return limited(q[2], left_face, right_face)


def hll_flux(dens_left, dens_right, speed_left, speed_right):
    slowest = jnp.minimum(jnp.minimum(speed_left, speed_right) - SOUND_SPEED, 0.0)
    fastest = jnp.maximum(jnp.maximum(speed_left, speed_right) + SOUND_SPEED, 0.0)
    upwind = fastest * dens_left * speed_left - slowest * dens_right * speed_right
    return (upwind + slowest * fastest * (dens_right - dens_left)) / (fastest - slowest)


PRIM_ROWS = ((0, 0, 3), (3, 3, 3), (1, 6, 1), (2, 7, 1))
MAG_ROWS_LOW = ((4, 8, 1), (5, 9, 1), (6, 10, 1))
MAG_ROWS_HIGH = ((4, 8, 1), (5, 9, 1), (6, 10, 2))
PACKED = 16


def stencil_kernel(middle, azimuth, chunk, count, starts, refs, outs, scratch):
    (s0, s1, s2, s3, s4, s5, s6, er, et, ep, carry_rho, carry_u, carry_flux) = scratch
    state = (s0, s1, s2, s3, s4, s5, s6)
    t = pl.program_id(0)
    width = s0.shape[-1]
    half = NPOL // 2
    slot = lax.rem(t, 8)
    own = slice(FRONT, FRONT + azimuth)
    dens_out, mag_out = outs

    def low_lanes(rows):
        return lax.broadcasted_iota(jnp.int32, (rows, NPOL), 1) < half

    if middle:
        dens, vel, mag, side_low, side_high = refs

        def ring(x):
            full = x.shape[1]
            mixed = jnp.where(low_lanes(x.shape[0]), x[:, full - NPOL :], x[:, :NPOL])
            return jnp.concatenate([x[:, NPOL : full - NPOL], mixed], axis=1)

        def merge(x, pol):
            return ring(x)

        s0[slot, own] = ring(dens[0])
        for c in range(3):
            state[1 + c][slot, own] = ring(vel[c, 0])
            state[4 + c][slot, own] = ring(mag[c, 0])
        pol_low = pol_high = None
    else:
        d0, d1, v0, v1, m0, m1, pols, side_low, side_high, mid_dens, mid_mag = refs

        def merge(x, pol):
            lanes = low_lanes(x.shape[0])
            a, b = x[:, :NPOL], x[:, x.shape[1] - NPOL :]
            if pol is None:
                return jnp.concatenate([a, b], axis=1)
            return jnp.concatenate([jnp.where(lanes, pol, a), jnp.where(lanes, b, pol)], axis=1)

        def fill(pol):
            lanes = low_lanes(azimuth)
            for c in range(4):
                a, b = (d0[0], d1[0]) if c == 0 else (v0[c - 1, 0], v1[c - 1, 0])
                p = pol[c, 0, :azimuth]
                state[c][slot, own, :NPOL] = jnp.where(lanes, p, a)
                state[c][slot, own, NPOL:] = jnp.where(lanes, b, p)
            for f, row, n in PRIM_ROWS:
                edge = azimuth + REACH
                low = merge(side_low[0, row : row + n], pol[f, 0, edge - n : edge])
                high = merge(side_high[0, row : row + n], pol[f, 0, edge : edge + n])
                state[f][slot, FRONT - n : FRONT] = low
                state[f][slot, FRONT + azimuth : FRONT + azimuth + n] = high

        if len(pols) == 1:
            fill(pols[0])
        else:
            layer = starts[0] + t - 3
            for i, pol in enumerate(pols):
                inside = True
                if i > 0:
                    inside = layer >= i * chunk
                if i < len(pols) - 1:
                    inside = (layer < (i + 1) * chunk) & inside
                pl.when(inside)(lambda pol=pol: fill(pol))
        for c in range(3):
            state[4 + c][slot, own, :NPOL] = m0[c, 0]
            state[4 + c][slot, own, NPOL:] = m1[c, 0]

    if middle:
        for f, row, n in PRIM_ROWS:
            state[f][slot, FRONT - n : FRONT] = ring(side_low[0, row : row + n])
            state[f][slot, FRONT + azimuth : FRONT + azimuth + n] = ring(side_high[0, row : row + n])
    for f, row, n in MAG_ROWS_LOW:
        state[f][slot, FRONT - n : FRONT] = merge(side_low[0, row : row + n], None)
    for f, row, n in MAG_ROWS_HIGH:
        state[f][slot, FRONT + azimuth : FRONT + azimuth + n] = merge(
            side_high[0, row : row + n], None
        )

    shape = (TILE, width)
    lane = lax.broadcasted_iota(jnp.int32, shape, 1)
    sub = lax.broadcasted_iota(jnp.int32, shape, 0)

    def shifted(ref, index, base, off):
        here = ref[index, pl.ds(base, TILE), :]
        if off > 0:
            other = ref[index, pl.ds(base + TILE, TILE), :]
            return pltpu.roll(jnp.where(sub < off, other, here), TILE - off, 0)
        if off < 0:
            other = ref[index, pl.ds(base - TILE, TILE), :]
            return pltpu.roll(jnp.where(sub >= TILE + off, other, here), -off, 0)
        return here

    def at(ref, d, base, off=0):
        return shifted(ref, lax.rem(t - 3 + d + 8, 8), base, off)

    def up(x):
        rolled = pltpu.roll(x, width - 1, 1)
        return rolled if middle else jnp.where(lane == width - 1, x, rolled)

    def down(x):
        rolled = pltpu.roll(x, 1, 1)
        return rolled if middle else jnp.where(lane == 0, x, rolled)

    def before(x, previous):
        return jnp.where(sub == 0, pltpu.roll(previous, 1, 0), pltpu.roll(x, 1, 0))

    def azimuth_step(base, right_rho, right_u):
        left_r, next_r = edges([at(s0, 0, base, o) for o in (-1, 0, 1, 2, 3)])
        left_u, next_u = edges([at(s3, 0, base, o) for o in (-1, 0, 1, 2, 3)])
        flux = hll_flux(before(next_r, right_rho), left_r, before(next_u, right_u), left_u)
        return next_r, next_u, flux

    def theta_edges(q):
        below = down(q)
        face = interface_value(down(below), below, q, up(q))
        rolled = pltpu.roll(face, width - 1, 1)
        above = rolled if middle else jnp.where(lane == width - 1, q, rolled)
        return limited(q, face, above)

    here = lax.rem(t, 4)

    def emf_tile(j, _):
        base = pl.multiple_of(FRONT - TILE + j * TILE, TILE)
        u_r, u_t, u_p = (at(s, 1, base) for s in (s1, s2, s3))
        b_r = 0.5 * (at(s4, 1, base) + at(s4, 2, base))
        b_t = at(s5, 1, base)
        b_t = 0.5 * (b_t + up(b_t))
        b_p = 0.5 * (at(s6, 1, base) + at(s6, 1, base, 1))
        rows = pl.ds(base, TILE)
        er[here, rows, :] = u_p * b_t - u_t * b_p
        et[here, rows, :] = u_r * b_p - u_p * b_r
        ep[here, rows, :] = u_t * b_r - u_r * b_t
        return 0

    @pl.when(t >= 4)
    def _():
        lax.fori_loop(0, azimuth // TILE + 2, emf_tile, 0)

    def emf(ref, d, base, off=0):
        return shifted(ref, lax.rem(t - 1 + d + 4, 4), base, off)

    def radial_step(rows, base):
        left_r, right_r = edges([at(s0, d, base) for d in (-1, 0, 1, 2, 3)])
        left_u, right_v = edges([at(s1, d, base) for d in (-1, 0, 1, 2, 3)])
        flux = hll_flux(carry_rho[rows, :], left_r, carry_u[rows, :], left_u)
        total = COURANT_RAD * (flux - carry_flux[rows, :])
        carry_rho[rows, :] = right_r
        carry_u[rows, :] = right_v
        carry_flux[rows, :] = flux
        return total

    def put(ref, index, rows, value, mid):
        if middle:
            ref[index + (rows, slice(None))] = value
            return
        inner = width + NPOL
        keep = lax.broadcasted_iota(jnp.int32, (TILE, NPOL), 1)
        mixed = mid[:, inner - NPOL :]
        quarter = half // 2
        first = jnp.where(keep < half + quarter, value[:, :NPOL], mixed)
        last = jnp.where(keep >= quarter, value[:, NPOL:], mixed)
        ref[index + (rows, slice(0, NPOL))] = first
        ref[index + (rows, slice(NPOL, inner))] = mid[:, : inner - NPOL]
        ref[index + (rows, slice(inner, inner + NPOL))] = last

    def middle_of(rows, c=None):
        if middle:
            return None
        return mid_dens[0, rows, :] if c is None else mid_mag[c, 0, rows, :]

    def tile(j, carry):
        right_rho, right_u, flux_low = carry
        start = pl.multiple_of(j * TILE, TILE)
        base = pl.multiple_of(FRONT + j * TILE, TILE)
        rows = pl.ds(start, TILE)

        total = radial_step(rows, base)

        right_rho, right_u, flux = azimuth_step(base, right_rho, right_u)
        total = total + COURANT_AZI * (flux - before(flux, flux_low))
        flux_low = flux

        rho = at(s0, 0, base)
        left_r, right_r = theta_edges(rho)
        left_u, right_v = theta_edges(at(s2, 0, base))
        theta_flux = hll_flux(down(right_r), left_r, down(right_v), left_u)
        if not middle:
            theta_flux = jnp.where(lane == 0, 0.0, theta_flux)
        above = pltpu.roll(theta_flux, width - 1, 1)
        if not middle:
            above = jnp.where(lane == width - 1, 0.0, above)
        total = total + COURANT_POL * (above - theta_flux)
        put(dens_out, (0,), rows, rho - total, middle_of(rows))

        er_low, er_here, er_high = (emf(er, 0, base, o) for o in (-1, 0, 1))
        ep_low, ep_here, ep_high = (emf(ep, d, base) for d in (-1, 0, 1))
        below_k = emf(et, -1, base, -1)
        edge_a = 0.5 * (ep_low + ep_here)
        edge_r = 0.5 * (er_low + er_here)
        mixed = (0.5 * COURANT_RAD) * (ep_high - ep_low) - (0.5 * COURANT_AZI) * (er_high - er_low)
        across = emf(et, -1, base, 1) + emf(et, 0, base, 1) - below_k - emf(et, 0, base, -1)
        along = emf(et, 1, base, -1) + emf(et, 1, base) - below_k - emf(et, -1, base)
        put(mag_out, (0, 0), rows,
            at(s4, 0, base)
            - (0.5 * COURANT_POL) * (up(edge_a) - down(edge_a))
            + (0.25 * COURANT_AZI) * across, middle_of(rows, 0))
        put(mag_out, (1, 0), rows, at(s5, 0, base) + 0.5 * (down(mixed) + mixed), middle_of(rows, 1))
        put(mag_out, (2, 0), rows,
            at(s6, 0, base)
            - (0.25 * COURANT_RAD) * along
            + (0.5 * COURANT_POL) * (up(edge_r) - down(edge_r)), middle_of(rows, 2))
        return right_rho, right_u, flux_low

    @pl.when((t >= 4) & (t < 6))
    def _():
        def warm(j, _):
            start = pl.multiple_of(j * TILE, TILE)
            radial_step(pl.ds(start, TILE), pl.multiple_of(FRONT + j * TILE, TILE))
            return 0

        lax.fori_loop(0, azimuth // TILE, warm, 0)

    @pl.when(t >= 6)
    def _():
        zero = jnp.zeros(shape, jnp.float32)
        first = azimuth_step(FRONT - TILE, zero, zero)
        lax.fori_loop(0, azimuth // TILE, tile, first)


def stencil(middle, count, starts, radial_out, fields, sides, polar=None, mids=None, into=None):
    density, velocity, magnetic = fields
    radial, azimuth, width = density.shape
    tiles = width // NPOL

    def own(t, s):
        return jnp.clip(s[0] + t - 3, 0, radial - 1)

    def out(t, s):
        return s[1] + jnp.clip(t - 6, 0, count - 1)

    def one(w, index=0):
        return pl.BlockSpec((1, azimuth, w), lambda t, s: (own(t, s), 0, index))

    def three(w, index=0):
        return pl.BlockSpec((3, 1, azimuth, w), lambda t, s: (0, own(t, s), 0, index))

    side = pl.BlockSpec((1, PACKED, width), lambda t, s: (own(t, s), 0, 0))
    chunk = 0
    if middle:
        ring = width - NPOL
        out_width = ring
        args = [density, velocity, magnetic, *sides]
        specs = [one(width), three(width), three(width), side, side]
    else:
        ring = 2 * NPOL
        out_width = width
        chunk = polar[0].shape[1]
        args = [density, density, velocity, velocity, magnetic, magnetic, *polar, *sides, *mids]
        specs = [one(NPOL), one(NPOL, tiles - 1), three(NPOL), three(NPOL, tiles - 1),
                 three(NPOL), three(NPOL, tiles - 1)]
        for i, p in enumerate(polar):
            specs.append(pl.BlockSpec(
                (4, 1, azimuth + HALO, NPOL),
                lambda t, s, i=i: (0, jnp.clip(own(t, s) - i * chunk, 0, chunk - 1), 0, 0)))
        specs += [side, side]
        mid_width = width - NPOL
        specs += [pl.BlockSpec((1, azimuth, mid_width), lambda t, s: (out(t, s), 0, 0)),
                  pl.BlockSpec((3, 1, azimuth, mid_width), lambda t, s: (0, out(t, s), 0, 0))]
    used = len(args)
    aliases = {}
    if into is not None:
        for i, x in enumerate(into):
            aliases[1 + len(args)] = i
            args.append(x)
            specs.append(pl.BlockSpec(memory_space=pl.ANY))

    def kernel(starts, *refs):
        ins, outs, scratch = refs[:used], refs[len(args) : len(args) + 2], refs[len(args) + 2 :]
        if not middle:
            n = len(polar)
            ins = ins[:6] + (ins[6 : 6 + n],) + ins[6 + n :]
        stencil_kernel(middle, azimuth, chunk, count, starts, ins, outs, scratch)

    rows = FRONT + azimuth + 2 * TILE
    scratch = (
        [pltpu.VMEM((8, rows, ring), jnp.float32)] * 7
        + [pltpu.VMEM((4, rows, ring), jnp.float32)] * 3
        + [pltpu.VMEM((azimuth, ring), jnp.float32)] * 3
    )
    return pl.pallas_call(
        kernel,
        grid_spec=pltpu.PrefetchScalarGridSpec(
            num_scalar_prefetch=1,
            grid=(count + 6,),
            in_specs=specs,
            out_specs=[
                pl.BlockSpec((1, azimuth, out_width), lambda t, s: (out(t, s), 0, 0)),
                pl.BlockSpec((3, 1, azimuth, out_width), lambda t, s: (0, out(t, s), 0, 0)),
            ],
            scratch_shapes=scratch,
        ),
        out_shape=[
            jax.ShapeDtypeStruct((radial_out, azimuth, out_width), jnp.float32),
            jax.ShapeDtypeStruct((3, radial_out, azimuth, out_width), jnp.float32),
        ],
        input_output_aliases=aliases,
        compiler_params=pltpu.CompilerParams(
            dimension_semantics=("arbitrary",), vmem_limit_bytes=62 * 1024 * 1024
        ),
        cost_estimate=pl.CostEstimate(
            flops=1000 * count * azimuth * ring, bytes_accessed=48 * count * azimuth * width,
            transcendentals=0,
        ),
        name="section_mid" if middle else "section_polar",
    )(starts, *args)


def chain(devices, wrap):
    up = [(i, (i + 1) % devices) for i in range(devices if wrap else devices - 1)]
    return up, [(j, i) for i, j in up]


def swap_rows(x):
    return lax.ppermute(x, "row", [(0, 1), (1, 0)])


def windowed(own, ghost, axis, low):
    reach = REACH
    size = own.shape[axis]
    start = jnp.where(low, size - 2 * reach, 0)
    kept = lax.dynamic_slice_in_dim(own, start, 2 * reach, axis)
    both = jnp.concatenate([ghost, kept, ghost], axis=axis)
    return lax.dynamic_slice_in_dim(both, jnp.where(low, reach, 0), 3 * reach, axis)


def per_device(density, velocity, magnetic):
    radial, azimuth, width = density.shape
    devices = lax.axis_size("phi")
    pairs = 4 * radial // devices
    chunks = 2 if pairs % 2 == 0 else 1
    layers = radial // chunks
    low = lax.axis_index("row") == 0
    deep = radial - REACH

    lines = []
    for c in range(chunks):
        packed = pack_lines(density, velocity, c * layers, layers)
        packed = packed.reshape(devices, pairs // chunks, azimuth, NPOL)
        lines.append(lax.all_to_all(packed, "phi", split_axis=0, concat_axis=0, tiled=True))

    first_rows, last_rows = pack_sides(density, velocity, magnetic)
    up, down = chain(devices, True)
    sides = (lax.ppermute(last_rows, "phi", up), lax.ppermute(first_rows, "phi", down))

    starts = jnp.where(low, jnp.array([0, 0], jnp.int32), jnp.array([REACH, REACH], jnp.int32))
    fields = (density, velocity, magnetic)
    mids = stencil(True, deep, starts, radial, fields, sides)

    polar = []
    for c in range(chunks):
        done = filter_lines(lines[c], width)
        done = lax.all_to_all(done, "phi", split_axis=0, concat_axis=0, tiled=True)
        polar.append(done.reshape(4, layers, azimuth + HALO, NPOL))

    far = jnp.where(low, deep, 0)
    near = jnp.where(low, radial - 1, 0)
    pair = jnp.where(low, radial - 2, 0)

    def take(x, start, n, axis=0):
        return lax.dynamic_slice_in_dim(x, start, n, axis)

    planes = jnp.concatenate(
        [take(density, far, 3), take(velocity[0], far, 3), take(velocity[1], near, 1),
         take(velocity[2], near, 1), take(magnetic[0], pair, 2), take(magnetic[1], near, 1),
         take(magnetic[2], near, 1)], axis=0)
    planes = swap_rows(planes)
    corner = swap_rows(jnp.concatenate([take(s, pair, 2) for s in sides], axis=0))
    wide = lambda x: jnp.broadcast_to(x, (REACH,) + x.shape[1:])
    duo = lambda x: jnp.concatenate([x[:1], x[:1], x[1:]], axis=0)
    duo_high = lambda x: jnp.concatenate([x[:1], x[1:], x[1:]], axis=0)
    ghost_m0 = jnp.where(low, duo_high(planes[8:10]), duo(planes[8:10]))
    ghost_v = jnp.stack([planes[3:6], wide(planes[6:7]), wide(planes[7:8])])
    ghost_m = jnp.stack([ghost_m0, wide(planes[10:11]), wide(planes[11:12])])
    corners = [jnp.where(low, duo_high(c), duo(c)) for c in (corner[:2], corner[2:])]
    window = (
        windowed(density, planes[:3], 0, low),
        windowed(velocity, ghost_v, 1, low),
        windowed(magnetic, ghost_m, 1, low),
    )
    window_sides = tuple(windowed(s, c, 0, low) for s, c in zip(sides, corners))
    edge = jnp.where(low, jnp.array([REACH, deep], jnp.int32), jnp.array([REACH, 0], jnp.int32))
    mids = stencil(True, REACH, edge, radial, window, window_sides, into=mids)

    out = stencil(False, deep, starts, radial, fields, sides, polar=polar, mids=mids)

    sent = jnp.where(low, polar[-1][:, layers - 3 :], polar[0][:, :3])
    close = jnp.where(low, polar[-1][2:, layers - 1 :], polar[0][2:, :1])
    got = swap_rows(jnp.concatenate([sent[0], sent[1], close[0], close[1]], axis=0))
    ghost_p = jnp.stack([got[:3], got[3:6], wide(got[6:7]), wide(got[7:8])])
    kept = jnp.where(low, polar[-1][:, layers - 2 * REACH :], polar[0][:, : 2 * REACH])
    both = jnp.concatenate([ghost_p, kept, ghost_p], axis=1)
    window_polar = take(both, jnp.where(low, REACH, 0), 3 * REACH, 1)
    out = stencil(False, REACH, edge, radial, window, window_sides, polar=[window_polar],
                  mids=mids, into=out)
    return tuple(out)


def solution(mesh):
    placed = (P("row", "phi", None), P(None, "row", "phi", None), P(None, "row", "phi", None))
    return jax.shard_map(
        per_device,
        mesh=mesh,
        in_specs=placed,
        out_specs=(P("row", "phi", None), P(None, "row", "phi", None)),
        check_vma=False,
    )
```

```python
import math

import jax
import jax.numpy as jnp
import numpy as np
from jax import lax
from jax.experimental import pallas as pl
from jax.experimental.pallas import tpu as pltpu
from jax.sharding import PartitionSpec as P

NPOL = 128
RADIX = 16
FRONT = 16
TILE = 8
HALO = 8
REACH = 3

COURANT_RAD = 0.3
COURANT_POL = 0.25
COURANT_AZI = 0.35
SOUND_SPEED = 1.0


def rotate(value, angle):
    re, im = value
    c, s = math.cos(angle), math.sin(angle)
    if im is None:
        return (re * c, re * s)
    return (re * c - im * s, re * s + im * c)


def add(a, b, sign=1.0):
    def part(x, y):
        if y is None:
            return x
        if x is None:
            return y if sign > 0 else -y
        return x + y if sign > 0 else x - y

    return (part(a[0], b[0]), part(a[1], b[1]))


def conj(a):
    return (a[0], None if a[1] is None else -a[1])


def real_fft(xs):
    n = len(xs)
    if n == 1:
        return [(xs[0], None)]
    if n == 2:
        return [(xs[0] + xs[1], None), (xs[0] - xs[1], None)]
    even, odd = real_fft(xs[0::2]), real_fft(xs[1::2])
    half = n // 2

    def at(spec, k):
        return spec[k] if k <= half // 2 else conj(spec[half - k])

    result = []
    for k in range(half + 1):
        e, o = at(even, k % half), at(odd, k % half)
        if k == 0:
            result.append(add(e, o))
        elif k == half:
            result.append(add(e, o, -1.0))
        elif 4 * k == n:
            result.append((e[0], -o[0]))
        else:
            result.append(add(e, rotate(o, -2.0 * math.pi * k / n)))
    return result


def real_ifft(spec, n):
    if n == 2:
        a, b = spec[0][0], spec[1][0]
        return [a + b, a - b]
    half = n // 2
    even, odd = [], []
    for k in range(half // 2 + 1):
        a, b = spec[k], conj(spec[half - k])
        if k == 0:
            a, b = (spec[0][0], None), (spec[half][0], None)
            even.append(add(a, b))
            odd.append(add(a, b, -1.0))
        elif 4 * k == n:
            even.append((2.0 * spec[k][0], None))
            odd.append((-2.0 * spec[k][1], None))
        else:
            even.append(add(a, b))
            odd.append(rotate(add(a, b, -1.0), 2.0 * math.pi * k / n))
    evens, odds = real_ifft(even, half), real_ifft(odd, half)
    return [v for pair in zip(evens, odds) for v in pair]


def filter_tables(cells, theta_count):
    inner = cells // RADIX
    half_polar = NPOL // 2
    k2 = np.arange(RADIX // 2 + 1)[:, None]
    mode = k2 + RADIX * np.arange(inner)[None, :]
    angle = 2.0 * np.pi / cells * ((mode[:, :, None] * np.arange(inner)) % cells)
    cos, sin = np.cos(angle), np.sin(angle)
    forward = np.concatenate(
        [np.concatenate([cos, sin], 2), np.concatenate([-sin, cos], 2)], 1
    ).astype(np.float32)
    rows = np.arange(NPOL)
    theta = np.where(rows < half_polar, rows, theta_count - NPOL + rows)
    row_square = np.sin(np.pi * (theta + 0.5) / theta_count) ** 2
    edge = np.sin(np.pi * (half_polar + 0.5) / theta_count)
    mode_square = (edge * np.sin(np.pi * mode / cells)) ** 2
    damping = row_square / np.maximum(row_square, mode_square[:, :, None])
    return forward, (damping / cells).astype(np.float32)


def filter_kernel(group, inner, blocks, x_ref, basis_ref, damp_ref, out_ref):
    devices, _, azimuth, _ = x_ref.shape

    def slab(d):
        parts = [
            x_ref[d * blocks : (d + 1) * blocks, g].reshape(inner, NPOL) for g in range(group)
        ]
        return jnp.concatenate(parts, axis=1) if group > 1 else parts[0]

    spectrum = real_fft([slab(d) for d in range(RADIX)])
    filtered = []
    for k, (re, im) in enumerate(spectrum):
        basis = basis_ref[k]
        if im is None:
            forward = basis[:, :inner]
            stacked = re
        else:
            forward = basis
            stacked = jnp.concatenate([re, im], axis=0)
        modes = jnp.dot(
            forward, stacked, precision=lax.Precision.HIGHEST, preferred_element_type=jnp.float32
        )
        damp = damp_ref[k]
        damp = jnp.concatenate([damp, damp], axis=0)
        if group > 1:
            damp = jnp.concatenate([damp] * group, axis=1)
        back = lax.dot_general(
            forward,
            modes * damp,
            (((0,), (0,)), ((), ())),
            precision=lax.Precision.HIGHEST,
            preferred_element_type=jnp.float32,
        )
        filtered.append((back, None) if im is None else (back[:inner], back[inner:]))
    for d, value in enumerate(real_ifft(filtered, RADIX)):
        for g in range(group):
            out_ref[d * blocks : (d + 1) * blocks, g, :azimuth] = value[
                :, g * NPOL : (g + 1) * NPOL
            ].reshape(blocks, azimuth, NPOL)
    blank = jnp.zeros((HALO - 2 * REACH, NPOL), jnp.float32)
    for d in range(devices):
        for g in range(group):
            below = out_ref[(d - 1) % devices, g, azimuth - REACH : azimuth]
            above = out_ref[(d + 1) % devices, g, :REACH]
            out_ref[d, g, azimuth:] = jnp.concatenate([below, above, blank], axis=0)


def filter_lines(lines, theta_count):
    devices, pairs, azimuth, _ = lines.shape
    cells = devices * azimuth
    inner = cells // RADIX
    blocks = inner // azimuth
    group = 2 if pairs % 2 == 0 else 1
    forward, damping = filter_tables(cells, theta_count)
    spec = pl.BlockSpec((devices, group, azimuth, NPOL), lambda p: (0, p, 0, 0))
    out = pl.BlockSpec((devices, group, azimuth + HALO, NPOL), lambda p: (0, p, 0, 0))
    return pl.pallas_call(
        lambda *refs: filter_kernel(group, inner, blocks, *refs),
        grid=(pairs // group,),
        in_specs=[
            spec,
            pl.BlockSpec(forward.shape, lambda p: (0, 0, 0)),
            pl.BlockSpec(damping.shape, lambda p: (0, 0, 0)),
        ],
        out_specs=out,
        out_shape=jax.ShapeDtypeStruct((devices, pairs, azimuth + HALO, NPOL), jnp.float32),
        compiler_params=pltpu.CompilerParams(vmem_limit_bytes=56 * 1024 * 1024),
        cost_estimate=pl.CostEstimate(
            flops=32 * inner * cells * NPOL * pairs, bytes_accessed=8 * lines.size, transcendentals=0
        ),
        name="polar_filter",
    )(lines, jnp.asarray(forward), jnp.asarray(damping))


def pack_lines(density, velocity, first, layers):
    _, azimuth, width = density.shape
    half = NPOL // 2
    last = width // NPOL - 1
    step = 2 if layers % 2 == 0 else 1

    def kernel(start, d0, d1, v0, v1, out):
        lane = lax.broadcasted_iota(jnp.int32, (azimuth, NPOL), 1)
        for i in range(step):
            out[0, i] = jnp.where(lane < half, d0[i], d1[i])
            for c in range(3):
                out[1 + c, i] = jnp.where(lane < half, v0[c, i], v1[c, i])

    def dens(tile):
        return pl.BlockSpec((step, azimuth, NPOL), lambda t, s: (s[0] + t, 0, tile))

    def vel(tile):
        return pl.BlockSpec((3, step, azimuth, NPOL), lambda t, s: (0, s[0] + t, 0, tile))

    return pl.pallas_call(
        kernel,
        grid_spec=pltpu.PrefetchScalarGridSpec(
            num_scalar_prefetch=1,
            grid=(layers // step,),
            in_specs=[dens(0), dens(last), vel(0), vel(last)],
            out_specs=pl.BlockSpec((4, step, azimuth, NPOL), lambda t, s: (0, t, 0, 0)),
        ),
        out_shape=jax.ShapeDtypeStruct((4, layers, azimuth, NPOL), jnp.float32),
        name="pack_lines",
    )(jnp.reshape(first // step, (1,)), density, density, velocity, velocity)


def pack_sides(density, velocity, magnetic):
    radial, azimuth, width = density.shape
    last = azimuth // TILE - 1
    step = 4 if radial % 4 == 0 else 1

    def kernel(d0, d1, v0, v1, m0, m1, low, high):
        def rows(i, dens, vel, mag, pick, wide):
            parts = [dens[i, pick(REACH)], vel[2, i, pick(REACH)], vel[0, i, pick(1)], vel[1, i, pick(1)]]
            parts += [mag[0, i, pick(1)], mag[1, i, pick(1)], mag[2, i, pick(wide)]]
            used = sum(p.shape[0] for p in parts)
            parts.append(jnp.zeros((PACKED - used, width), jnp.float32))
            return jnp.concatenate(parts, axis=0)

        for i in range(step):
            low[i] = rows(i, d0, v0, m0, lambda n: slice(0, n), 2)
            high[i] = rows(i, d1, v1, m1, lambda n: slice(TILE - n, TILE), 1)

    def three(b):
        return pl.BlockSpec((3, step, TILE, width), lambda t: (0, t, b, 0))

    def one(b):
        return pl.BlockSpec((step, TILE, width), lambda t: (t, b, 0))

    return pl.pallas_call(
        kernel,
        grid=(radial // step,),
        in_specs=[one(0), one(last), three(0), three(last), three(0), three(last)],
        out_specs=[pl.BlockSpec((step, PACKED, width), lambda t: (t, 0, 0))] * 2,
        out_shape=[jax.ShapeDtypeStruct((radial, PACKED, width), jnp.float32)] * 2,
        name="pack_sides",
    )(density, density, velocity, velocity, magnetic, magnetic)


def interface_value(outer_left, inner_left, inner_right, outer_right):
    guess = 7.0 / 12.0 * (inner_left + inner_right) - 1.0 / 12.0 * (outer_left + outer_right)
    low = jnp.minimum(inner_left, inner_right)
    return jnp.minimum(jnp.maximum(guess, low), jnp.maximum(inner_left, inner_right))


def limited(centre, left_face, right_face):
    to_left = left_face - centre
    to_right = right_face - centre
    reach_right = 2.0 * jnp.abs(to_right)
    reach_left = 2.0 * jnp.abs(to_left)
    left = jnp.minimum(jnp.maximum(to_left, -reach_right), reach_right)
    right = jnp.minimum(jnp.maximum(to_right, -reach_left), reach_left)
    return centre + left, centre + right


def edges(q):
    left_face = interface_value(q[0], q[1], q[2], q[3])
    right_face = interface_value(q[1], q[2], q[3], q[4])
    return limited(q[2], left_face, right_face)


def hll_flux(dens_left, dens_right, speed_left, speed_right):
    slowest = jnp.minimum(jnp.minimum(speed_left, speed_right) - SOUND_SPEED, 0.0)
    fastest = jnp.maximum(jnp.maximum(speed_left, speed_right) + SOUND_SPEED, 0.0)
    upwind = fastest * dens_left * speed_left - slowest * dens_right * speed_right
    return (upwind + slowest * fastest * (dens_right - dens_left)) / (fastest - slowest)


PRIM_ROWS = ((0, 0, 3), (3, 3, 3), (1, 6, 1), (2, 7, 1))
MAG_ROWS_LOW = ((4, 8, 1), (5, 9, 1), (6, 10, 1))
MAG_ROWS_HIGH = ((4, 8, 1), (5, 9, 1), (6, 10, 2))
PACKED = 16


def stencil_kernel(middle, radial, azimuth, chunk, count, starts, refs, ghosts, outs, scratch):
    (s0, s1, s2, s3, s4, s5, s6, er, et, ep, carry_rho, carry_u, carry_flux) = scratch
    state = (s0, s1, s2, s3, s4, s5, s6)
    t = pl.program_id(0)
    width = s0.shape[-1]
    half = NPOL // 2
    slot = lax.rem(t, 8)
    layer = starts[0] + t - 3
    own = slice(FRONT, FRONT + azimuth)
    dens_out, mag_out = outs

    def low_lanes(rows):
        return lax.broadcasted_iota(jnp.int32, (rows, NPOL), 1) < half

    def ring(x):
        full = x.shape[1]
        mixed = jnp.where(low_lanes(x.shape[0]), x[:, full - NPOL :], x[:, :NPOL])
        return jnp.concatenate([x[:, NPOL : full - NPOL], mixed], axis=1)

    def outer(x, pol=None):
        lanes = low_lanes(x.shape[0])
        a, b = x[:, :NPOL], x[:, x.shape[1] - NPOL :]
        if pol is not None:
            a, b = jnp.where(lanes, pol, a), jnp.where(lanes, b, pol)
        return jnp.concatenate([a, b], axis=1)

    edge = azimuth + REACH

    def fill(fields, pols, low, high):
        for f, x in enumerate(fields):
            if middle:
                state[f][slot, own] = ring(x())
            elif f < 4:
                state[f][slot, own] = outer(x(), pols[f][:azimuth])
            else:
                state[f][slot, own] = outer(x())
        for f, row, n in PRIM_ROWS:
            a, b = low[row : row + n], high[row : row + n]
            if middle:
                a, b = ring(a), ring(b)
            else:
                a = outer(a, pols[f][edge - n : edge])
                b = outer(b, pols[f][edge : edge + n])
            state[f][slot, FRONT - n : FRONT] = a
            state[f][slot, FRONT + azimuth : FRONT + azimuth + n] = b
        shape = ring if middle else outer
        for f, row, n in MAG_ROWS_LOW:
            state[f][slot, FRONT - n : FRONT] = shape(low[row : row + n])
        for f, row, n in MAG_ROWS_HIGH:
            state[f][slot, FRONT + azimuth : FRONT + azimuth + n] = shape(high[row : row + n])

    mid_dens = mid_mag = None
    if middle:
        dens, vel, mag, side_low, side_high = refs
        fields = [lambda: dens[0]]
        fields += [lambda c=c: vel[c, 0] for c in range(3)]
        fields += [lambda c=c: mag[c, 0] for c in range(3)]
        choices = [(None, None)]
    else:
        d0, d1, v0, v1, m0, m1, pols, side_low, side_high, mid_dens, mid_mag = refs

        def both(a, b):
            return jnp.concatenate([a, b], axis=1)

        fields = [lambda: both(d0[0], d1[0])]
        fields += [lambda c=c: both(v0[c, 0], v1[c, 0]) for c in range(3)]
        fields += [lambda c=c: both(m0[c, 0], m1[c, 0]) for c in range(3)]
        choices = []
        for i, pol in enumerate(pols):
            inside = None
            if len(pols) > 1:
                at_layer = jnp.clip(layer, 0, radial - 1) - starts[2 + i]
                inside = (at_layer >= 0) & (at_layer < chunk)
            choices.append((pol, inside))
    mine = None if ghosts is None else (layer >= 0) & (layer < radial)
    for pol, inside in choices:
        def load(pol=pol):
            pieces = None if pol is None else [pol.at[c, 0] for c in range(4)]
            fill(fields, pieces, side_low.at[0], side_high.at[0])

        cond = mine if inside is None else inside if mine is None else mine & inside
        if cond is None:
            load()
        else:
            pl.when(cond)(load)
    if ghosts is not None:
        @pl.when(jnp.logical_not(mine))
        def _():
            planes = [lambda r=r: r[0] for r in ghosts[:7]]
            pieces = [r.at[0] for r in ghosts[9:]]
            fill(planes, pieces, ghosts[7].at[0], ghosts[8].at[0])

    shape = (TILE, width)
    lane = lax.broadcasted_iota(jnp.int32, shape, 1)
    sub = lax.broadcasted_iota(jnp.int32, shape, 0)

    def shifted(ref, index, base, off):
        here = ref[index, pl.ds(base, TILE), :]
        if off > 0:
            other = ref[index, pl.ds(base + TILE, TILE), :]
            return pltpu.roll(jnp.where(sub < off, other, here), TILE - off, 0)
        if off < 0:
            other = ref[index, pl.ds(base - TILE, TILE), :]
            return pltpu.roll(jnp.where(sub >= TILE + off, other, here), -off, 0)
        return here

    def at(ref, d, base, off=0):
        return shifted(ref, lax.rem(t - 3 + d + 8, 8), base, off)

    def up(x):
        rolled = pltpu.roll(x, width - 1, 1)
        return rolled if middle else jnp.where(lane == width - 1, x, rolled)

    def down(x):
        rolled = pltpu.roll(x, 1, 1)
        return rolled if middle else jnp.where(lane == 0, x, rolled)

    def before(x, previous):
        return jnp.where(sub == 0, pltpu.roll(previous, 1, 0), pltpu.roll(x, 1, 0))

    def azimuth_step(base, right_rho, right_u):
        left_r, next_r = edges([at(s0, 0, base, o) for o in (-1, 0, 1, 2, 3)])
        left_u, next_u = edges([at(s3, 0, base, o) for o in (-1, 0, 1, 2, 3)])
        flux = hll_flux(before(next_r, right_rho), left_r, before(next_u, right_u), left_u)
        return next_r, next_u, flux

    def theta_edges(q):
        below = down(q)
        face = interface_value(down(below), below, q, up(q))
        rolled = pltpu.roll(face, width - 1, 1)
        above = rolled if middle else jnp.where(lane == width - 1, q, rolled)
        return limited(q, face, above)

    here = lax.rem(t, 4)

    def emf_tile(j, _):
        base = pl.multiple_of(FRONT - TILE + j * TILE, TILE)
        u_r, u_t, u_p = (at(s, 1, base) for s in (s1, s2, s3))
        b_r = 0.5 * (at(s4, 1, base) + at(s4, 2, base))
        b_t = at(s5, 1, base)
        b_t = 0.5 * (b_t + up(b_t))
        b_p = 0.5 * (at(s6, 1, base) + at(s6, 1, base, 1))
        rows = pl.ds(base, TILE)
        er[here, rows, :] = u_p * b_t - u_t * b_p
        et[here, rows, :] = u_r * b_p - u_p * b_r
        ep[here, rows, :] = u_t * b_r - u_r * b_t
        return 0

    @pl.when(t >= 4)
    def _():
        lax.fori_loop(0, azimuth // TILE + 2, emf_tile, 0, unroll=2)

    def emf(ref, d, base, off=0):
        return shifted(ref, lax.rem(t - 1 + d + 4, 4), base, off)

    def radial_step(rows, base):
        left_r, right_r = edges([at(s0, d, base) for d in (-1, 0, 1, 2, 3)])
        left_u, right_v = edges([at(s1, d, base) for d in (-1, 0, 1, 2, 3)])
        flux = hll_flux(carry_rho[rows, :], left_r, carry_u[rows, :], left_u)
        total = COURANT_RAD * (flux - carry_flux[rows, :])
        carry_rho[rows, :] = right_r
        carry_u[rows, :] = right_v
        carry_flux[rows, :] = flux
        return total

    def put(ref, index, rows, value, mid):
        if middle:
            ref[index + (rows, slice(None))] = value
            return
        inner = width + NPOL
        keep = lax.broadcasted_iota(jnp.int32, (TILE, NPOL), 1)
        mixed = mid[:, inner - NPOL :]
        quarter = half // 2
        first = jnp.where(keep < half + quarter, value[:, :NPOL], mixed)
        last = jnp.where(keep >= quarter, value[:, NPOL:], mixed)
        ref[index + (rows, slice(0, NPOL))] = first
        ref[index + (rows, slice(NPOL, inner))] = mid[:, : inner - NPOL]
        ref[index + (rows, slice(inner, inner + NPOL))] = last

    def middle_of(rows, c=None):
        if middle:
            return None
        return mid_dens[0, rows, :] if c is None else mid_mag[c, 0, rows, :]

    def tile(j, carry):
        right_rho, right_u, flux_low = carry
        start = pl.multiple_of(j * TILE, TILE)
        base = pl.multiple_of(FRONT + j * TILE, TILE)
        rows = pl.ds(start, TILE)

        total = radial_step(rows, base)

        right_rho, right_u, flux = azimuth_step(base, right_rho, right_u)
        total = total + COURANT_AZI * (flux - before(flux, flux_low))
        flux_low = flux

        rho = at(s0, 0, base)
        left_r, right_r = theta_edges(rho)
        left_u, right_v = theta_edges(at(s2, 0, base))
        theta_flux = hll_flux(down(right_r), left_r, down(right_v), left_u)
        if not middle:
            theta_flux = jnp.where(lane == 0, 0.0, theta_flux)
        above = pltpu.roll(theta_flux, width - 1, 1)
        if not middle:
            above = jnp.where(lane == width - 1, 0.0, above)
        total = total + COURANT_POL * (above - theta_flux)
        put(dens_out, (0,), rows, rho - total, middle_of(rows))

        er_low, er_here, er_high = (emf(er, 0, base, o) for o in (-1, 0, 1))
        ep_low, ep_here, ep_high = (emf(ep, d, base) for d in (-1, 0, 1))
        below_k = emf(et, -1, base, -1)
        edge_a = 0.5 * (ep_low + ep_here)
        edge_r = 0.5 * (er_low + er_here)
        mixed = (0.5 * COURANT_RAD) * (ep_high - ep_low) - (0.5 * COURANT_AZI) * (er_high - er_low)
        across = emf(et, -1, base, 1) + emf(et, 0, base, 1) - below_k - emf(et, 0, base, -1)
        along = emf(et, 1, base, -1) + emf(et, 1, base) - below_k - emf(et, -1, base)
        put(mag_out, (0, 0), rows,
            at(s4, 0, base)
            - (0.5 * COURANT_POL) * (up(edge_a) - down(edge_a))
            + (0.25 * COURANT_AZI) * across, middle_of(rows, 0))
        put(mag_out, (1, 0), rows, at(s5, 0, base) + 0.5 * (down(mixed) + mixed), middle_of(rows, 1))
        put(mag_out, (2, 0), rows,
            at(s6, 0, base)
            - (0.25 * COURANT_RAD) * along
            + (0.5 * COURANT_POL) * (up(edge_r) - down(edge_r)), middle_of(rows, 2))
        return right_rho, right_u, flux_low

    @pl.when((t >= 4) & (t < 6))
    def _():
        def warm(j, _):
            start = pl.multiple_of(j * TILE, TILE)
            radial_step(pl.ds(start, TILE), pl.multiple_of(FRONT + j * TILE, TILE))
            return 0

        lax.fori_loop(0, azimuth // TILE, warm, 0, unroll=2)

    @pl.when(t >= 6)
    def _():
        zero = jnp.zeros(shape, jnp.float32)
        first = azimuth_step(FRONT - TILE, zero, zero)
        lax.fori_loop(0, azimuth // TILE, tile, first, unroll=4)


def stencil(middle, count, starts, fields, sides, ghosts=None, polar=None, mids=None, into=None):
    density, velocity, magnetic = fields
    radial, azimuth, width = density.shape
    tiles = width // NPOL

    def own(t, s):
        return jnp.clip(s[0] + t - 3, 0, radial - 1)

    def out(t, s):
        return s[1] + jnp.clip(t - 6, 0, count - 1)

    def one(w, index=0):
        return pl.BlockSpec((1, azimuth, w), lambda t, s: (own(t, s), 0, index))

    def three(w, index=0):
        return pl.BlockSpec((3, 1, azimuth, w), lambda t, s: (0, own(t, s), 0, index))

    def deep(t, s):
        g = s[0] + t - 3
        return jnp.clip(jnp.where(g < 0, g + 3, g - radial), 0, 2)

    def two(t, s):
        g = s[0] + t - 3
        return jnp.clip(jnp.where(g < 0, g + 2, g - radial), 0, 1)

    side = pl.BlockSpec((1, PACKED, width), lambda t, s: (own(t, s), 0, 0))
    chunk = 0
    if middle:
        ring = width - NPOL
        out_width = ring
        args = [density, velocity, magnetic, *sides]
        specs = [one(width), three(width), three(width), side, side]
    else:
        ring = 2 * NPOL
        out_width = width
        chunk = polar[0].shape[1]
        args = [density, density, velocity, velocity, magnetic, magnetic, *polar, *sides, *mids]
        specs = [one(NPOL), one(NPOL, tiles - 1), three(NPOL), three(NPOL, tiles - 1),
                 three(NPOL), three(NPOL, tiles - 1)]
        for i, p in enumerate(polar):
            specs.append(pl.BlockSpec(
                (4, 1, azimuth + HALO, NPOL),
                lambda t, s, i=i: (0, jnp.clip(own(t, s) - s[2 + i], 0, chunk - 1), 0, 0)))
        specs += [side, side]
        mid_width = width - NPOL
        specs += [pl.BlockSpec((1, azimuth, mid_width), lambda t, s: (out(t, s), 0, 0)),
                  pl.BlockSpec((3, 1, azimuth, mid_width), lambda t, s: (0, out(t, s), 0, 0))]
    used = len(args)
    extra = 0
    if ghosts is not None:
        planes, corner, filtered = ghosts
        where = [lambda t, s: deep(t, s), lambda t, s: 3 + deep(t, s), lambda t, s: 6, lambda t, s: 7]
        index = where + [lambda t, s: 8 + two(t, s), lambda t, s: 10, lambda t, s: 11]
        for f in index:
            args.append(planes)
            specs.append(pl.BlockSpec((1, azimuth, width), lambda t, s, f=f: (f(t, s), 0, 0)))
        for first in (0, 2):
            args.append(corner)
            specs.append(pl.BlockSpec(
                (1, PACKED, width), lambda t, s, first=first: (first + two(t, s), 0, 0)))
        if filtered is not None:
            for f in where:
                args.append(filtered)
                specs.append(pl.BlockSpec(
                    (1, azimuth + HALO, NPOL), lambda t, s, f=f: (f(t, s), 0, 0)))
        extra = len(args) - used
    aliases = {}
    if into is not None:
        for i, x in enumerate(into):
            aliases[1 + len(args)] = i
            args.append(x)
            specs.append(pl.BlockSpec(memory_space=pl.ANY))

    def kernel(starts, *refs):
        ins, outs, scratch = refs[:used], refs[len(args) : len(args) + 2], refs[len(args) + 2 :]
        spare = refs[used : used + extra] if extra else None
        if not middle:
            n = len(polar)
            ins = ins[:6] + (ins[6 : 6 + n],) + ins[6 + n :]
        stencil_kernel(middle, radial, azimuth, chunk, count, starts, ins, spare, outs, scratch)

    rows = FRONT + azimuth + 2 * TILE
    scratch = (
        [pltpu.VMEM((8, rows, ring), jnp.float32)] * 7
        + [pltpu.VMEM((4, rows, ring), jnp.float32)] * 3
        + [pltpu.VMEM((azimuth, ring), jnp.float32)] * 3
    )
    return pl.pallas_call(
        kernel,
        grid_spec=pltpu.PrefetchScalarGridSpec(
            num_scalar_prefetch=1,
            grid=(count + 6,),
            in_specs=specs,
            out_specs=[
                pl.BlockSpec((1, azimuth, out_width), lambda t, s: (out(t, s), 0, 0)),
                pl.BlockSpec((3, 1, azimuth, out_width), lambda t, s: (0, out(t, s), 0, 0)),
            ],
            scratch_shapes=scratch,
        ),
        out_shape=[
            jax.ShapeDtypeStruct((radial, azimuth, out_width), jnp.float32),
            jax.ShapeDtypeStruct((3, radial, azimuth, out_width), jnp.float32),
        ],
        input_output_aliases=aliases,
        compiler_params=pltpu.CompilerParams(
            dimension_semantics=("arbitrary",), vmem_limit_bytes=62 * 1024 * 1024
        ),
        cost_estimate=pl.CostEstimate(
            flops=1000 * count * azimuth * ring, bytes_accessed=48 * count * azimuth * width,
            transcendentals=0,
        ),
        name="section_mid" if middle else "section_polar",
    )(starts, *args)


def swap_rows(x):
    return lax.ppermute(x, "row", [(0, 1), (1, 0)])


def per_device(density, velocity, magnetic):
    radial, azimuth, width = density.shape
    devices = lax.axis_size("phi")
    pairs = 4 * radial // devices
    chunks = 2 if pairs % 2 == 0 else 1
    layers = radial // chunks
    low = lax.axis_index("row") == 0
    fields = (density, velocity, magnetic)

    def pick(a, b):
        return jnp.where(low, jnp.int32(a), jnp.int32(b))

    def transpose(x, rows):
        x = x.reshape(devices, pairs // chunks, rows, NPOL)
        return lax.all_to_all(x, "phi", split_axis=0, concat_axis=0, tiled=True)

    base = [pick(layers * (chunks - 1 - c), layers * c) for c in range(chunks)]
    packed = [pack_lines(density, velocity, base[c], layers) for c in range(chunks)]
    first_rows, last_rows = pack_sides(density, velocity, magnetic)

    far, near, pair = pick(radial - 3, 0), pick(radial - 1, 0), pick(radial - 2, 0)

    def plane(x, c, n, start, size):
        return lax.dynamic_slice(x, (c, start, 0, 0), (n, size, azimuth, width)).reshape(
            n * size, azimuth, width)

    planes = jnp.concatenate(
        [lax.dynamic_slice_in_dim(density, far, 3, 0), plane(velocity, 0, 1, far, 3),
         plane(velocity, 1, 2, near, 1), plane(magnetic, 0, 1, pair, 2),
         plane(magnetic, 1, 2, near, 1)], axis=0)
    around = [(i, (i + 1) % devices) for i in range(devices)]
    back = [(j, i) for i, j in around]

    lines = [transpose(packed[0], azimuth)]
    sides = (lax.ppermute(last_rows, "phi", around), lax.ppermute(first_rows, "phi", back))
    planes = swap_rows(planes)
    if chunks > 1:
        packed[1], sides = lax.optimization_barrier((packed[1], sides))
        lines.append(transpose(packed[1], azimuth))
    corner = swap_rows(
        jnp.concatenate([lax.dynamic_slice_in_dim(x, pair, 2, 0) for x in sides], axis=0))

    def starts(s):
        return jnp.stack([s, s] + base)

    deep = radial - REACH
    early = (deep + 1) // 2
    mids = stencil(True, early, starts(pick(0, REACH)), fields, sides)
    lines[-1], mids = lax.optimization_barrier((lines[-1], tuple(mids)))
    smooth = [filter_lines(x, width) for x in lines]
    polar = [transpose(smooth[0], azimuth + HALO)]
    mids = stencil(True, deep - early, starts(pick(early, early + REACH)), fields, sides, into=mids)
    if chunks > 1:
        smooth[1], mids = lax.optimization_barrier((smooth[1], tuple(mids)))
        polar.append(transpose(smooth[1], azimuth + HALO))
    polar = [p.reshape(4, layers, azimuth + HALO, NPOL) for p in polar]

    first = polar[0]
    far, near = pick(layers - 3, 0), pick(layers - 1, 0)
    sent = lax.dynamic_slice_in_dim(first[:2], far, 3, 1).reshape(6, azimuth + HALO, NPOL)
    close = lax.dynamic_slice_in_dim(first[2:], near, 1, 1).reshape(2, azimuth + HALO, NPOL)
    filtered = swap_rows(jnp.concatenate([sent, close], axis=0))
    mids = stencil(True, REACH, starts(pick(deep, 0)), fields, sides,
                   ghosts=(planes, corner, None), into=mids)

    edge = radial // 2 - REACH
    out = stencil(False, edge, starts(pick(radial - edge, 0)), fields, sides,
                  ghosts=(planes, corner, filtered), polar=polar[:1], mids=mids)
    if chunks > 1:
        polar[1], out = lax.optimization_barrier((polar[1], tuple(out)))
    out = stencil(False, radial - edge, starts(pick(0, edge)), fields, sides, polar=polar,
                  mids=mids, into=out)
    return tuple(out)


def solution(mesh):
    placed = (P("row", "phi", None), P(None, "row", "phi", None), P(None, "row", "phi", None))
    return jax.shard_map(
        per_device,
        mesh=mesh,
        in_specs=placed,
        out_specs=(P("row", "phi", None), P(None, "row", "phi", None)),
        check_vma=False,
    )
```

```python
import math

import jax
import jax.numpy as jnp
import numpy as np
from jax import lax
from jax.experimental import pallas as pl
from jax.experimental.pallas import tpu as pltpu
from jax.sharding import PartitionSpec as P


NPOL = 128
RADIX = 16
FRONT = 16
TILE = 8
HALO = 8
REACH = 3

COURANT_RAD = 0.3
COURANT_POL = 0.25
COURANT_AZI = 0.35
SOUND_SPEED = 1.0


def rotate(value, angle):
    re, im = value
    c, s = math.cos(angle), math.sin(angle)
    if im is None:
        return (re * c, re * s)
    return (re * c - im * s, re * s + im * c)


def add(a, b, sign=1.0):
    def part(x, y):
        if y is None:
            return x
        if x is None:
            return y if sign > 0 else -y
        return x + y if sign > 0 else x - y

    return (part(a[0], b[0]), part(a[1], b[1]))


def conj(a):
    return (a[0], None if a[1] is None else -a[1])


def real_fft(xs):
    n = len(xs)
    if n == 1:
        return [(xs[0], None)]
    if n == 2:
        return [(xs[0] + xs[1], None), (xs[0] - xs[1], None)]
    even, odd = real_fft(xs[0::2]), real_fft(xs[1::2])
    half = n // 2

    def at(spec, k):
        return spec[k] if k <= half // 2 else conj(spec[half - k])

    result = []
    for k in range(half + 1):
        e, o = at(even, k % half), at(odd, k % half)
        if k == 0:
            result.append(add(e, o))
        elif k == half:
            result.append(add(e, o, -1.0))
        elif 4 * k == n:
            result.append((e[0], -o[0]))
        else:
            result.append(add(e, rotate(o, -2.0 * math.pi * k / n)))
    return result


def real_ifft(spec, n):
    if n == 2:
        a, b = spec[0][0], spec[1][0]
        return [a + b, a - b]
    half = n // 2
    even, odd = [], []
    for k in range(half // 2 + 1):
        a, b = spec[k], conj(spec[half - k])
        if k == 0:
            a, b = (spec[0][0], None), (spec[half][0], None)
            even.append(add(a, b))
            odd.append(add(a, b, -1.0))
        elif 4 * k == n:
            even.append((2.0 * spec[k][0], None))
            odd.append((-2.0 * spec[k][1], None))
        else:
            even.append(add(a, b))
            odd.append(rotate(add(a, b, -1.0), 2.0 * math.pi * k / n))
    evens, odds = real_ifft(even, half), real_ifft(odd, half)
    return [v for pair in zip(evens, odds) for v in pair]


def filter_tables(cells, theta_count):
    inner = cells // RADIX
    half_polar = NPOL // 2
    k2 = np.arange(RADIX // 2 + 1)[:, None]
    mode = k2 + RADIX * np.arange(inner)[None, :]
    angle = 2.0 * np.pi / cells * ((mode[:, :, None] * np.arange(inner)) % cells)
    cos, sin = np.cos(angle), np.sin(angle)
    forward = np.concatenate(
        [np.concatenate([cos, sin], 2), np.concatenate([-sin, cos], 2)], 1
    ).astype(np.float32)
    rows = np.arange(NPOL)
    theta = np.where(rows < half_polar, rows, theta_count - NPOL + rows)
    row_square = np.sin(np.pi * (theta + 0.5) / theta_count) ** 2
    edge = np.sin(np.pi * (half_polar + 0.5) / theta_count)
    mode_square = (edge * np.sin(np.pi * mode / cells)) ** 2
    damping = row_square / np.maximum(row_square, mode_square[:, :, None])
    return forward, (damping / cells).astype(np.float32)


def filter_kernel(group, inner, blocks, x_ref, basis_ref, damp_ref, out_ref):
    devices, _, azimuth, _ = x_ref.shape

    def slab(d):
        parts = [
            x_ref[d * blocks : (d + 1) * blocks, g].reshape(inner, NPOL) for g in range(group)
        ]
        return jnp.concatenate(parts, axis=1) if group > 1 else parts[0]

    spectrum = real_fft([slab(d) for d in range(RADIX)])
    filtered = []
    for k, (re, im) in enumerate(spectrum):
        basis = basis_ref[k]
        if im is None:
            forward = basis[:, :inner]
            stacked = re
        else:
            forward = basis
            stacked = jnp.concatenate([re, im], axis=0)
        modes = jnp.dot(
            forward, stacked, precision=lax.Precision.HIGHEST, preferred_element_type=jnp.float32
        )
        damp = damp_ref[k]
        damp = jnp.concatenate([damp, damp], axis=0)
        if group > 1:
            damp = jnp.concatenate([damp] * group, axis=1)
        back = lax.dot_general(
            forward,
            modes * damp,
            (((0,), (0,)), ((), ())),
            precision=lax.Precision.HIGHEST,
            preferred_element_type=jnp.float32,
        )
        filtered.append((back, None) if im is None else (back[:inner], back[inner:]))
    for d, value in enumerate(real_ifft(filtered, RADIX)):
        for g in range(group):
            out_ref[d * blocks : (d + 1) * blocks, g, :azimuth] = value[
                :, g * NPOL : (g + 1) * NPOL
            ].reshape(blocks, azimuth, NPOL)
    blank = jnp.zeros((HALO - 2 * REACH, NPOL), jnp.float32)
    for d in range(devices):
        for g in range(group):
            below = out_ref[(d - 1) % devices, g, azimuth - REACH : azimuth]
            above = out_ref[(d + 1) % devices, g, :REACH]
            out_ref[d, g, azimuth:] = jnp.concatenate([below, above, blank], axis=0)


def filter_lines(lines, theta_count):
    devices, pairs, azimuth, _ = lines.shape
    cells = devices * azimuth
    inner = cells // RADIX
    blocks = inner // azimuth
    group = 2 if pairs % 2 == 0 else 1
    forward, damping = filter_tables(cells, theta_count)
    spec = pl.BlockSpec((devices, group, azimuth, NPOL), lambda p: (0, p, 0, 0))
    out = pl.BlockSpec((devices, group, azimuth + HALO, NPOL), lambda p: (0, p, 0, 0))
    return pl.pallas_call(
        lambda *refs: filter_kernel(group, inner, blocks, *refs),
        grid=(pairs // group,),
        in_specs=[
            spec,
            pl.BlockSpec(forward.shape, lambda p: (0, 0, 0)),
            pl.BlockSpec(damping.shape, lambda p: (0, 0, 0)),
        ],
        out_specs=out,
        out_shape=jax.ShapeDtypeStruct((devices, pairs, azimuth + HALO, NPOL), jnp.float32),
        compiler_params=pltpu.CompilerParams(vmem_limit_bytes=56 * 1024 * 1024),
        cost_estimate=pl.CostEstimate(
            flops=32 * inner * cells * NPOL * pairs, bytes_accessed=8 * lines.size, transcendentals=0
        ),
        name="polar_filter",
    )(lines, jnp.asarray(forward), jnp.asarray(damping))


def pack_lines(density, velocity, first, layers):
    _, azimuth, width = density.shape
    half = NPOL // 2
    last = width // NPOL - 1
    step = 2 if layers % 2 == 0 else 1

    def kernel(start, d0, d1, v0, v1, out):
        lane = lax.broadcasted_iota(jnp.int32, (azimuth, NPOL), 1)
        for i in range(step):
            out[0, i] = jnp.where(lane < half, d0[i], d1[i])
            for c in range(3):
                out[1 + c, i] = jnp.where(lane < half, v0[c, i], v1[c, i])

    def dens(tile):
        return pl.BlockSpec((step, azimuth, NPOL), lambda t, s: (s[0] + t, 0, tile))

    def vel(tile):
        return pl.BlockSpec((3, step, azimuth, NPOL), lambda t, s: (0, s[0] + t, 0, tile))

    return pl.pallas_call(
        kernel,
        grid_spec=pltpu.PrefetchScalarGridSpec(
            num_scalar_prefetch=1,
            grid=(layers // step,),
            in_specs=[dens(0), dens(last), vel(0), vel(last)],
            out_specs=pl.BlockSpec((4, step, azimuth, NPOL), lambda t, s: (0, t, 0, 0)),
        ),
        out_shape=jax.ShapeDtypeStruct((4, layers, azimuth, NPOL), jnp.float32),
        name="pack_lines",
    )(jnp.reshape(first // step, (1,)), density, density, velocity, velocity)


def pack_sides(density, velocity, magnetic):
    radial, azimuth, width = density.shape
    last = azimuth // TILE - 1
    step = 4 if radial % 4 == 0 else 1

    def kernel(d0, d1, v0, v1, m0, m1, low, high):
        def rows(i, dens, vel, mag, pick, wide):
            parts = [dens[i, pick(REACH)], vel[2, i, pick(REACH)], vel[0, i, pick(1)], vel[1, i, pick(1)]]
            parts += [mag[0, i, pick(1)], mag[1, i, pick(1)], mag[2, i, pick(wide)]]
            used = sum(p.shape[0] for p in parts)
            parts.append(jnp.zeros((PACKED - used, width), jnp.float32))
            return jnp.concatenate(parts, axis=0)

        for i in range(step):
            low[i] = rows(i, d0, v0, m0, lambda n: slice(0, n), 2)
            high[i] = rows(i, d1, v1, m1, lambda n: slice(TILE - n, TILE), 1)

    def three(b):
        return pl.BlockSpec((3, step, TILE, width), lambda t: (0, t, b, 0))

    def one(b):
        return pl.BlockSpec((step, TILE, width), lambda t: (t, b, 0))

    return pl.pallas_call(
        kernel,
        grid=(radial // step,),
        in_specs=[one(0), one(last), three(0), three(last), three(0), three(last)],
        out_specs=[pl.BlockSpec((step, PACKED, width), lambda t: (t, 0, 0))] * 2,
        out_shape=[jax.ShapeDtypeStruct((radial, PACKED, width), jnp.float32)] * 2,
        name="pack_sides",
    )(density, density, velocity, velocity, magnetic, magnetic)


def interface_value(outer_left, inner_left, inner_right, outer_right):
    guess = 7.0 / 12.0 * (inner_left + inner_right) - 1.0 / 12.0 * (outer_left + outer_right)
    low = jnp.minimum(inner_left, inner_right)
    return jnp.minimum(jnp.maximum(guess, low), jnp.maximum(inner_left, inner_right))


def limited(centre, left_face, right_face):
    to_left = left_face - centre
    to_right = right_face - centre
    reach_right = 2.0 * jnp.abs(to_right)
    reach_left = 2.0 * jnp.abs(to_left)
    left = jnp.minimum(jnp.maximum(to_left, -reach_right), reach_right)
    right = jnp.minimum(jnp.maximum(to_right, -reach_left), reach_left)
    return centre + left, centre + right


def edges(q):
    left_face = interface_value(q[0], q[1], q[2], q[3])
    right_face = interface_value(q[1], q[2], q[3], q[4])
    return limited(q[2], left_face, right_face)


def hll_flux(dens_left, dens_right, speed_left, speed_right):
    slowest = jnp.minimum(jnp.minimum(speed_left, speed_right) - SOUND_SPEED, 0.0)
    fastest = jnp.maximum(jnp.maximum(speed_left, speed_right) + SOUND_SPEED, 0.0)
    upwind = fastest * dens_left * speed_left - slowest * dens_right * speed_right
    return (upwind + slowest * fastest * (dens_right - dens_left)) / (fastest - slowest)


PRIM_ROWS = ((0, 0, 3), (3, 3, 3), (1, 6, 1), (2, 7, 1))
MAG_ROWS_LOW = ((4, 8, 1), (5, 9, 1), (6, 10, 1))
MAG_ROWS_HIGH = ((4, 8, 1), (5, 9, 1), (6, 10, 2))
PACKED = 16


def stencil_kernel(middle, radial, azimuth, chunk, starts, refs, ghosts, outs, scratch):
    (s0, s1, s2, s3, s4, s5, s6, er, et, ep, carry_rho, carry_u, carry_flux) = scratch
    state = (s0, s1, s2, s3, s4, s5, s6)
    t = pl.program_id(0)
    width = s0.shape[-1]
    half = NPOL // 2
    slot = lax.rem(t, 8)
    layer = starts[0] + t - 3
    own = slice(FRONT, FRONT + azimuth)
    dens_out, mag_out = outs

    def low_lanes(rows):
        return lax.broadcasted_iota(jnp.int32, (rows, NPOL), 1) < half

    def ring(x):
        full = x.shape[1]
        mixed = jnp.where(low_lanes(x.shape[0]), x[:, full - NPOL :], x[:, :NPOL])
        return jnp.concatenate([x[:, NPOL : full - NPOL], mixed], axis=1)

    def outer(x, pol=None):
        lanes = low_lanes(x.shape[0])
        a, b = x[:, :NPOL], x[:, x.shape[1] - NPOL :]
        if pol is not None:
            a, b = jnp.where(lanes, pol, a), jnp.where(lanes, b, pol)
        return jnp.concatenate([a, b], axis=1)

    edge = azimuth + REACH

    def fill(fields, pols, low, high):
        for f, x in enumerate(fields):
            if middle:
                state[f][slot, own] = ring(x())
            elif f < 4:
                state[f][slot, own] = outer(x(), pols[f][:azimuth])
            else:
                state[f][slot, own] = outer(x())
        for f, row, n in PRIM_ROWS:
            a, b = low[row : row + n], high[row : row + n]
            if middle:
                a, b = ring(a), ring(b)
            else:
                a = outer(a, pols[f][edge - n : edge])
                b = outer(b, pols[f][edge : edge + n])
            state[f][slot, FRONT - n : FRONT] = a
            state[f][slot, FRONT + azimuth : FRONT + azimuth + n] = b
        shape = ring if middle else outer
        for f, row, n in MAG_ROWS_LOW:
            state[f][slot, FRONT - n : FRONT] = shape(low[row : row + n])
        for f, row, n in MAG_ROWS_HIGH:
            state[f][slot, FRONT + azimuth : FRONT + azimuth + n] = shape(high[row : row + n])

    mid_dens = mid_mag = None
    if middle:
        dens, vel, mag, side_low, side_high = refs
        fields = [lambda: dens[0]]
        fields += [lambda c=c: vel[c, 0] for c in range(3)]
        fields += [lambda c=c: mag[c, 0] for c in range(3)]
        choices = [(None, None)]
    else:
        d0, d1, v0, v1, m0, m1, pols, side_low, side_high, mid_dens, mid_mag = refs

        def both(a, b):
            return jnp.concatenate([a, b], axis=1)

        fields = [lambda: both(d0[0], d1[0])]
        fields += [lambda c=c: both(v0[c, 0], v1[c, 0]) for c in range(3)]
        fields += [lambda c=c: both(m0[c, 0], m1[c, 0]) for c in range(3)]
        choices = []
        for i, pol in enumerate(pols):
            inside = None
            if len(pols) > 1:
                at_layer = jnp.clip(layer, 0, radial - 1) - starts[2 + i]
                inside = (at_layer >= 0) & (at_layer < chunk)
            choices.append((pol, inside))
    mine = None if ghosts is None else (layer >= 0) & (layer < radial)
    for pol, inside in choices:
        def load(pol=pol):
            pieces = None if pol is None else [pol.at[c, 0] for c in range(4)]
            fill(fields, pieces, side_low.at[0], side_high.at[0])

        cond = mine if inside is None else inside if mine is None else mine & inside
        if cond is None:
            load()
        else:
            pl.when(cond)(load)
    if ghosts is not None:
        @pl.when(jnp.logical_not(mine))
        def _():
            planes = [lambda r=r: r[0] for r in ghosts[:7]]
            pieces = [r.at[0] for r in ghosts[9:]]
            fill(planes, pieces, ghosts[7].at[0], ghosts[8].at[0])

    shape = (TILE, width)
    lane = lax.broadcasted_iota(jnp.int32, shape, 1)
    sub = lax.broadcasted_iota(jnp.int32, shape, 0)

    def shifted(ref, index, base, off):
        here = ref[index, pl.ds(base, TILE), :]
        if off > 0:
            other = ref[index, pl.ds(base + TILE, TILE), :]
            return pltpu.roll(jnp.where(sub < off, other, here), TILE - off, 0)
        if off < 0:
            other = ref[index, pl.ds(base - TILE, TILE), :]
            return pltpu.roll(jnp.where(sub >= TILE + off, other, here), -off, 0)
        return here

    def at(ref, d, base, off=0):
        return shifted(ref, lax.rem(t - 3 + d + 8, 8), base, off)

    def up(x):
        rolled = pltpu.roll(x, width - 1, 1)
        return rolled if middle else jnp.where(lane == width - 1, x, rolled)

    def down(x):
        rolled = pltpu.roll(x, 1, 1)
        return rolled if middle else jnp.where(lane == 0, x, rolled)

    def before(x, previous):
        return jnp.where(sub == 0, pltpu.roll(previous, 1, 0), pltpu.roll(x, 1, 0))

    def azimuth_step(base, right_rho, right_u):
        left_r, next_r = edges([at(s0, 0, base, o) for o in (-1, 0, 1, 2, 3)])
        left_u, next_u = edges([at(s3, 0, base, o) for o in (-1, 0, 1, 2, 3)])
        flux = hll_flux(before(next_r, right_rho), left_r, before(next_u, right_u), left_u)
        return next_r, next_u, flux

    def theta_edges(q):
        below = down(q)
        face = interface_value(down(below), below, q, up(q))
        rolled = pltpu.roll(face, width - 1, 1)
        above = rolled if middle else jnp.where(lane == width - 1, q, rolled)
        return limited(q, face, above)

    here = lax.rem(t, 4)

    def emf_tile(j, _):
        base = pl.multiple_of(FRONT - TILE + j * TILE, TILE)
        u_r, u_t, u_p = (at(s, 1, base) for s in (s1, s2, s3))
        b_r = 0.5 * (at(s4, 1, base) + at(s4, 2, base))
        b_t = at(s5, 1, base)
        b_t = 0.5 * (b_t + up(b_t))
        b_p = 0.5 * (at(s6, 1, base) + at(s6, 1, base, 1))
        rows = pl.ds(base, TILE)
        er[here, rows, :] = u_p * b_t - u_t * b_p
        et[here, rows, :] = u_r * b_p - u_p * b_r
        ep[here, rows, :] = u_t * b_r - u_r * b_t
        return 0

    @pl.when(t >= 4)
    def _():
        lax.fori_loop(0, azimuth // TILE + 2, emf_tile, 0, unroll=2)

    def emf(ref, d, base, off=0):
        return shifted(ref, lax.rem(t - 1 + d + 4, 4), base, off)

    def radial_step(rows, base):
        left_r, right_r = edges([at(s0, d, base) for d in (-1, 0, 1, 2, 3)])
        left_u, right_v = edges([at(s1, d, base) for d in (-1, 0, 1, 2, 3)])
        flux = hll_flux(carry_rho[rows, :], left_r, carry_u[rows, :], left_u)
        total = COURANT_RAD * (flux - carry_flux[rows, :])
        carry_rho[rows, :] = right_r
        carry_u[rows, :] = right_v
        carry_flux[rows, :] = flux
        return total

    def put(ref, index, rows, value, mid):
        if middle:
            ref[index + (rows, slice(None))] = value
            return
        inner = width + NPOL
        keep = lax.broadcasted_iota(jnp.int32, (TILE, NPOL), 1)
        mixed = mid[:, inner - NPOL :]
        quarter = half // 2
        first = jnp.where(keep < half + quarter, value[:, :NPOL], mixed)
        last = jnp.where(keep >= quarter, value[:, NPOL:], mixed)
        ref[index + (rows, slice(0, NPOL))] = first
        ref[index + (rows, slice(NPOL, inner))] = mid[:, : inner - NPOL]
        ref[index + (rows, slice(inner, inner + NPOL))] = last

    def middle_of(rows, c=None):
        if middle:
            return None
        return mid_dens[0, rows, :] if c is None else mid_mag[c, 0, rows, :]

    def tile(j, carry):
        right_rho, right_u, flux_low = carry
        start = pl.multiple_of(j * TILE, TILE)
        base = pl.multiple_of(FRONT + j * TILE, TILE)
        rows = pl.ds(start, TILE)

        total = radial_step(rows, base)

        right_rho, right_u, flux = azimuth_step(base, right_rho, right_u)
        total = total + COURANT_AZI * (flux - before(flux, flux_low))
        flux_low = flux

        rho = at(s0, 0, base)
        left_r, right_r = theta_edges(rho)
        left_u, right_v = theta_edges(at(s2, 0, base))
        theta_flux = hll_flux(down(right_r), left_r, down(right_v), left_u)
        if not middle:
            theta_flux = jnp.where(lane == 0, 0.0, theta_flux)
        above = pltpu.roll(theta_flux, width - 1, 1)
        if not middle:
            above = jnp.where(lane == width - 1, 0.0, above)
        total = total + COURANT_POL * (above - theta_flux)
        put(dens_out, (0,), rows, rho - total, middle_of(rows))

        er_low, er_here, er_high = (emf(er, 0, base, o) for o in (-1, 0, 1))
        ep_low, ep_here, ep_high = (emf(ep, d, base) for d in (-1, 0, 1))
        below_k = emf(et, -1, base, -1)
        edge_a = 0.5 * (ep_low + ep_here)
        edge_r = 0.5 * (er_low + er_here)
        mixed = (0.5 * COURANT_RAD) * (ep_high - ep_low) - (0.5 * COURANT_AZI) * (er_high - er_low)
        across = emf(et, -1, base, 1) + emf(et, 0, base, 1) - below_k - emf(et, 0, base, -1)
        along = emf(et, 1, base, -1) + emf(et, 1, base) - below_k - emf(et, -1, base)
        put(mag_out, (0, 0), rows,
            at(s4, 0, base)
            - (0.5 * COURANT_POL) * (up(edge_a) - down(edge_a))
            + (0.25 * COURANT_AZI) * across, middle_of(rows, 0))
        put(mag_out, (1, 0), rows, at(s5, 0, base) + 0.5 * (down(mixed) + mixed), middle_of(rows, 1))
        put(mag_out, (2, 0), rows,
            at(s6, 0, base)
            - (0.25 * COURANT_RAD) * along
            + (0.5 * COURANT_POL) * (up(edge_r) - down(edge_r)), middle_of(rows, 2))
        return right_rho, right_u, flux_low

    @pl.when((t >= 4) & (t < 6))
    def _():
        def warm(j, _):
            start = pl.multiple_of(j * TILE, TILE)
            radial_step(pl.ds(start, TILE), pl.multiple_of(FRONT + j * TILE, TILE))
            return 0

        lax.fori_loop(0, azimuth // TILE, warm, 0, unroll=2)

    @pl.when(t >= 6)
    def _():
        zero = jnp.zeros(shape, jnp.float32)
        first = azimuth_step(FRONT - TILE, zero, zero)
        lax.fori_loop(0, azimuth // TILE, tile, first, unroll=4)


def stencil(middle, count, starts, fields, sides, ghosts=None, polar=None, mids=None, into=None):
    density, velocity, magnetic = fields
    radial, azimuth, width = density.shape
    tiles = width // NPOL

    def own(t, s):
        return jnp.clip(s[0] + t - 3, 0, radial - 1)

    def out(t, s):
        return s[1] + jnp.clip(t - 6, 0, count - 1)

    def one(w, index=0):
        return pl.BlockSpec((1, azimuth, w), lambda t, s: (own(t, s), 0, index))

    def three(w, index=0):
        return pl.BlockSpec((3, 1, azimuth, w), lambda t, s: (0, own(t, s), 0, index))

    def deep(t, s):
        g = s[0] + t - 3
        return jnp.clip(jnp.where(g < 0, g + 3, g - radial), 0, 2)

    def two(t, s):
        g = s[0] + t - 3
        return jnp.clip(jnp.where(g < 0, g + 2, g - radial), 0, 1)

    side = pl.BlockSpec((1, PACKED, width), lambda t, s: (own(t, s), 0, 0))
    chunk = 0
    if middle:
        ring = width - NPOL
        out_width = ring
        args = [density, velocity, magnetic, *sides]
        specs = [one(width), three(width), three(width), side, side]
    else:
        ring = 2 * NPOL
        out_width = width
        chunk = polar[0].shape[1]
        args = [density, density, velocity, velocity, magnetic, magnetic, *polar, *sides, *mids]
        specs = [one(NPOL), one(NPOL, tiles - 1), three(NPOL), three(NPOL, tiles - 1),
                 three(NPOL), three(NPOL, tiles - 1)]
        for i, p in enumerate(polar):
            specs.append(pl.BlockSpec(
                (4, 1, azimuth + HALO, NPOL),
                lambda t, s, i=i: (0, jnp.clip(own(t, s) - s[2 + i], 0, chunk - 1), 0, 0)))
        specs += [side, side]
        mid_width = width - NPOL
        specs += [pl.BlockSpec((1, azimuth, mid_width), lambda t, s: (out(t, s), 0, 0)),
                  pl.BlockSpec((3, 1, azimuth, mid_width), lambda t, s: (0, out(t, s), 0, 0))]
    used = len(args)
    extra = 0
    if ghosts is not None:
        planes, corner, filtered = ghosts
        where = [lambda t, s: deep(t, s), lambda t, s: 3 + deep(t, s), lambda t, s: 6, lambda t, s: 7]
        index = where + [lambda t, s: 8 + two(t, s), lambda t, s: 10, lambda t, s: 11]
        for f in index:
            args.append(planes)
            specs.append(pl.BlockSpec((1, azimuth, width), lambda t, s, f=f: (f(t, s), 0, 0)))
        for first in (0, 2):
            args.append(corner)
            specs.append(pl.BlockSpec(
                (1, PACKED, width), lambda t, s, first=first: (first + two(t, s), 0, 0)))
        if filtered is not None:
            for f in where:
                args.append(filtered)
                specs.append(pl.BlockSpec(
                    (1, azimuth + HALO, NPOL), lambda t, s, f=f: (f(t, s), 0, 0)))
        extra = len(args) - used
    aliases = {}
    if into is not None:
        for i, x in enumerate(into):
            aliases[1 + len(args)] = i
            args.append(x)
            specs.append(pl.BlockSpec(memory_space=pl.ANY))

    def kernel(starts, *refs):
        ins, outs, scratch = refs[:used], refs[len(args) : len(args) + 2], refs[len(args) + 2 :]
        spare = refs[used : used + extra] if extra else None
        if not middle:
            n = len(polar)
            ins = ins[:6] + (ins[6 : 6 + n],) + ins[6 + n :]
        stencil_kernel(middle, radial, azimuth, chunk, starts, ins, spare, outs, scratch)

    rows = FRONT + azimuth + 2 * TILE
    scratch = (
        [pltpu.VMEM((8, rows, ring), jnp.float32)] * 7
        + [pltpu.VMEM((4, rows, ring), jnp.float32)] * 3
        + [pltpu.VMEM((azimuth, ring), jnp.float32)] * 3
    )
    return pl.pallas_call(
        kernel,
        grid_spec=pltpu.PrefetchScalarGridSpec(
            num_scalar_prefetch=1,
            grid=(count + 6,),
            in_specs=specs,
            out_specs=[
                pl.BlockSpec((1, azimuth, out_width), lambda t, s: (out(t, s), 0, 0)),
                pl.BlockSpec((3, 1, azimuth, out_width), lambda t, s: (0, out(t, s), 0, 0)),
            ],
            scratch_shapes=scratch,
        ),
        out_shape=[
            jax.ShapeDtypeStruct((radial, azimuth, out_width), jnp.float32),
            jax.ShapeDtypeStruct((3, radial, azimuth, out_width), jnp.float32),
        ],
        input_output_aliases=aliases,
        compiler_params=pltpu.CompilerParams(
            dimension_semantics=("arbitrary",), vmem_limit_bytes=62 * 1024 * 1024
        ),
        cost_estimate=pl.CostEstimate(
            flops=1000 * count * azimuth * ring, bytes_accessed=48 * count * azimuth * width,
            transcendentals=0,
        ),
        name="section_mid" if middle else "section_polar",
    )(starts, *args)


def swap_rows(x):
    return lax.ppermute(x, "row", [(0, 1), (1, 0)])


def section(density, velocity, magnetic):
    radial, azimuth, width = density.shape
    devices = lax.axis_size("phi")
    pairs = 4 * radial // devices
    chunks = 2 if pairs % 2 == 0 else 1
    layers = radial // chunks
    low = lax.axis_index("row") == 0
    fields = (density, velocity, magnetic)

    def pick(a, b):
        return jnp.where(low, jnp.int32(a), jnp.int32(b))

    def transpose(x, rows):
        x = x.reshape(devices, pairs // chunks, rows, NPOL)
        return lax.all_to_all(x, "phi", split_axis=0, concat_axis=0, tiled=True)

    base = [pick(layers * (chunks - 1 - c), layers * c) for c in range(chunks)]
    packed = [pack_lines(density, velocity, base[c], layers) for c in range(chunks)]
    first_rows, last_rows = pack_sides(density, velocity, magnetic)

    far, near, pair = pick(radial - 3, 0), pick(radial - 1, 0), pick(radial - 2, 0)

    def plane(x, c, n, start, size):
        return lax.dynamic_slice(x, (c, start, 0, 0), (n, size, azimuth, width)).reshape(
            n * size, azimuth, width)

    planes = jnp.concatenate(
        [lax.dynamic_slice_in_dim(density, far, 3, 0), plane(velocity, 0, 1, far, 3),
         plane(velocity, 1, 2, near, 1), plane(magnetic, 0, 1, pair, 2),
         plane(magnetic, 1, 2, near, 1)], axis=0)
    around = [(i, (i + 1) % devices) for i in range(devices)]
    back = [(j, i) for i, j in around]

    lines = [transpose(packed[0], azimuth)]
    sides = (lax.ppermute(last_rows, "phi", around), lax.ppermute(first_rows, "phi", back))
    if chunks > 1:
        packed[1], sides, planes = lax.optimization_barrier((packed[1], sides, planes))
        lines.append(transpose(packed[1], azimuth))
    planes = swap_rows(planes)
    corner = swap_rows(
        jnp.concatenate([lax.dynamic_slice_in_dim(x, pair, 2, 0) for x in sides], axis=0))

    def starts(s):
        return jnp.stack([s, s] + base)

    deep = radial - REACH
    early = (deep + 1) // 2
    mids = stencil(True, early, starts(pick(0, REACH)), fields, sides)
    smooth = [filter_lines(x, width) for x in lines]
    smooth[0], mids = lax.optimization_barrier((smooth[0], tuple(mids)))
    polar = [transpose(smooth[0], azimuth + HALO)]
    mids = stencil(True, deep - early, starts(pick(early, early + REACH)), fields, sides, into=mids)
    if chunks > 1:
        smooth[1], mids = lax.optimization_barrier((smooth[1], tuple(mids)))
        polar.append(transpose(smooth[1], azimuth + HALO))
    polar = [p.reshape(4, layers, azimuth + HALO, NPOL) for p in polar]

    first = polar[0]
    far, near = pick(layers - 3, 0), pick(layers - 1, 0)
    sent = lax.dynamic_slice_in_dim(first[:2], far, 3, 1).reshape(6, azimuth + HALO, NPOL)
    close = lax.dynamic_slice_in_dim(first[2:], near, 1, 1).reshape(2, azimuth + HALO, NPOL)
    filtered = swap_rows(jnp.concatenate([sent, close], axis=0))
    mids = stencil(True, REACH, starts(pick(deep, 0)), fields, sides,
                   ghosts=(planes, corner, None), into=mids)

    edge = radial // 2 - REACH
    out = stencil(False, edge, starts(pick(radial - edge, 0)), fields, sides,
                  ghosts=(planes, corner, filtered), polar=polar[:1], mids=mids)
    if chunks > 1:
        polar[1], out = lax.optimization_barrier((polar[1], tuple(out)))
    out = stencil(False, radial - edge, starts(pick(0, edge)), fields, sides, polar=polar,
                  mids=mids, into=out)
    return tuple(out)


def solution(mesh):
    placed = (P("row", "phi", None), P(None, "row", "phi", None), P(None, "row", "phi", None))
    return jax.shard_map(
        section,
        mesh=mesh,
        in_specs=placed,
        out_specs=(P("row", "phi", None), P(None, "row", "phi", None)),
        check_vma=False,
    )
```

```python
import math

import jax
import jax.numpy as jnp
import numpy as np
from jax import lax
from jax.experimental import pallas as pl
from jax.experimental.pallas import tpu as pltpu
from jax.sharding import PartitionSpec as P


NPOL = 128
RADIX = 16
FRONT = 16
TILE = 8
HALO = 8
REACH = 3

COURANT_RAD = 0.3
COURANT_POL = 0.25
COURANT_AZI = 0.35
SOUND_SPEED = 1.0


def rotate(value, angle):
    re, im = value
    c, s = math.cos(angle), math.sin(angle)
    if im is None:
        return (re * c, re * s)
    return (re * c - im * s, re * s + im * c)


def add(a, b, sign=1.0):
    def part(x, y):
        if y is None:
            return x
        if x is None:
            return y if sign > 0 else -y
        return x + y if sign > 0 else x - y

    return (part(a[0], b[0]), part(a[1], b[1]))


def conj(a):
    return (a[0], None if a[1] is None else -a[1])


def real_fft(xs):
    n = len(xs)
    if n == 1:
        return [(xs[0], None)]
    if n == 2:
        return [(xs[0] + xs[1], None), (xs[0] - xs[1], None)]
    even, odd = real_fft(xs[0::2]), real_fft(xs[1::2])
    half = n // 2

    def at(spec, k):
        return spec[k] if k <= half // 2 else conj(spec[half - k])

    result = []
    for k in range(half + 1):
        e, o = at(even, k % half), at(odd, k % half)
        if k == 0:
            result.append(add(e, o))
        elif k == half:
            result.append(add(e, o, -1.0))
        elif 4 * k == n:
            result.append((e[0], -o[0]))
        else:
            result.append(add(e, rotate(o, -2.0 * math.pi * k / n)))
    return result


def real_ifft(spec, n):
    if n == 2:
        a, b = spec[0][0], spec[1][0]
        return [a + b, a - b]
    half = n // 2
    even, odd = [], []
    for k in range(half // 2 + 1):
        a, b = spec[k], conj(spec[half - k])
        if k == 0:
            a, b = (spec[0][0], None), (spec[half][0], None)
            even.append(add(a, b))
            odd.append(add(a, b, -1.0))
        elif 4 * k == n:
            even.append((2.0 * spec[k][0], None))
            odd.append((-2.0 * spec[k][1], None))
        else:
            even.append(add(a, b))
            odd.append(rotate(add(a, b, -1.0), 2.0 * math.pi * k / n))
    evens, odds = real_ifft(even, half), real_ifft(odd, half)
    return [v for pair in zip(evens, odds) for v in pair]


def filter_tables(cells, theta_count):
    inner = cells // RADIX
    half_polar = NPOL // 2
    k2 = np.arange(RADIX // 2 + 1)[:, None]
    mode = k2 + RADIX * np.arange(inner)[None, :]
    angle = 2.0 * np.pi / cells * ((mode[:, :, None] * np.arange(inner)) % cells)
    cos, sin = np.cos(angle), np.sin(angle)
    forward = np.concatenate(
        [np.concatenate([cos, sin], 2), np.concatenate([-sin, cos], 2)], 1
    ).astype(np.float32)
    rows = np.arange(NPOL)
    theta = np.where(rows < half_polar, rows, theta_count - NPOL + rows)
    row_square = np.sin(np.pi * (theta + 0.5) / theta_count) ** 2
    edge = np.sin(np.pi * (half_polar + 0.5) / theta_count)
    mode_square = (edge * np.sin(np.pi * mode / cells)) ** 2
    damping = row_square / np.maximum(row_square, mode_square[:, :, None])
    return forward, (damping / cells).astype(np.float32)


def filter_kernel(group, inner, blocks, x_ref, basis_ref, damp_ref, out_ref):
    devices, _, azimuth, _ = x_ref.shape

    def slab(d):
        parts = [
            x_ref[d * blocks : (d + 1) * blocks, g].reshape(inner, NPOL) for g in range(group)
        ]
        return jnp.concatenate(parts, axis=1) if group > 1 else parts[0]

    spectrum = real_fft([slab(d) for d in range(RADIX)])
    filtered = []
    for k, (re, im) in enumerate(spectrum):
        basis = basis_ref[k]
        if im is None:
            forward = basis[:, :inner]
            stacked = re
        else:
            forward = basis
            stacked = jnp.concatenate([re, im], axis=0)
        modes = jnp.dot(
            forward, stacked, precision=lax.Precision.HIGHEST, preferred_element_type=jnp.float32
        )
        damp = damp_ref[k]
        damp = jnp.concatenate([damp, damp], axis=0)
        if group > 1:
            damp = jnp.concatenate([damp] * group, axis=1)
        back = lax.dot_general(
            forward,
            modes * damp,
            (((0,), (0,)), ((), ())),
            precision=lax.Precision.HIGHEST,
            preferred_element_type=jnp.float32,
        )
        filtered.append((back, None) if im is None else (back[:inner], back[inner:]))
    for d, value in enumerate(real_ifft(filtered, RADIX)):
        for g in range(group):
            out_ref[d * blocks : (d + 1) * blocks, g, :azimuth] = value[
                :, g * NPOL : (g + 1) * NPOL
            ].reshape(blocks, azimuth, NPOL)
    blank = jnp.zeros((HALO - 2 * REACH, NPOL), jnp.float32)
    for d in range(devices):
        for g in range(group):
            below = out_ref[(d - 1) % devices, g, azimuth - REACH : azimuth]
            above = out_ref[(d + 1) % devices, g, :REACH]
            out_ref[d, g, azimuth:] = jnp.concatenate([below, above, blank], axis=0)


def filter_lines(lines, theta_count):
    devices, pairs, azimuth, _ = lines.shape
    cells = devices * azimuth
    inner = cells // RADIX
    blocks = inner // azimuth
    group = next(g for g in (3, 2, 1) if pairs % g == 0)
    forward, damping = filter_tables(cells, theta_count)
    spec = pl.BlockSpec((devices, group, azimuth, NPOL), lambda p: (0, p, 0, 0))
    out = pl.BlockSpec((devices, group, azimuth + HALO, NPOL), lambda p: (0, p, 0, 0))
    return pl.pallas_call(
        lambda *refs: filter_kernel(group, inner, blocks, *refs),
        grid=(pairs // group,),
        in_specs=[
            spec,
            pl.BlockSpec(forward.shape, lambda p: (0, 0, 0)),
            pl.BlockSpec(damping.shape, lambda p: (0, 0, 0)),
        ],
        out_specs=out,
        out_shape=jax.ShapeDtypeStruct((devices, pairs, azimuth + HALO, NPOL), jnp.float32),
        compiler_params=pltpu.CompilerParams(vmem_limit_bytes=56 * 1024 * 1024),
        cost_estimate=pl.CostEstimate(
            flops=32 * inner * cells * NPOL * pairs, bytes_accessed=8 * lines.size, transcendentals=0
        ),
        name="polar_filter",
    )(lines, jnp.asarray(forward), jnp.asarray(damping))


def pack_lines(density, velocity, first, layers):
    _, azimuth, width = density.shape
    half = NPOL // 2
    last = width // NPOL - 1
    step = math.gcd(4, math.gcd(layers, density.shape[0]))

    def kernel(start, d0, d1, v0, v1, out):
        lane = lax.broadcasted_iota(jnp.int32, (azimuth, NPOL), 1)
        for i in range(step):
            out[0, i] = jnp.where(lane < half, d0[i], d1[i])
            for c in range(3):
                out[1 + c, i] = jnp.where(lane < half, v0[c, i], v1[c, i])

    def dens(tile):
        return pl.BlockSpec((step, azimuth, NPOL), lambda t, s: (s[0] + t, 0, tile))

    def vel(tile):
        return pl.BlockSpec((3, step, azimuth, NPOL), lambda t, s: (0, s[0] + t, 0, tile))

    return pl.pallas_call(
        kernel,
        grid_spec=pltpu.PrefetchScalarGridSpec(
            num_scalar_prefetch=1,
            grid=(layers // step,),
            in_specs=[dens(0), dens(last), vel(0), vel(last)],
            out_specs=pl.BlockSpec((4, step, azimuth, NPOL), lambda t, s: (0, t, 0, 0)),
        ),
        out_shape=jax.ShapeDtypeStruct((4, layers, azimuth, NPOL), jnp.float32),
        name="pack_lines",
    )(jnp.reshape(first // step, (1,)), density, density, velocity, velocity)


def pack_sides(density, velocity, magnetic):
    radial, azimuth, width = density.shape
    last = azimuth // TILE - 1
    step = 4 if radial % 4 == 0 else 1

    def kernel(d0, d1, v0, v1, m0, m1, low, high):
        def rows(i, dens, vel, mag, pick, wide):
            parts = [dens[i, pick(REACH)], vel[2, i, pick(REACH)], vel[0, i, pick(1)], vel[1, i, pick(1)]]
            parts += [mag[0, i, pick(1)], mag[1, i, pick(1)], mag[2, i, pick(wide)]]
            used = sum(p.shape[0] for p in parts)
            parts.append(jnp.zeros((PACKED - used, width), jnp.float32))
            return jnp.concatenate(parts, axis=0)

        for i in range(step):
            low[i] = rows(i, d0, v0, m0, lambda n: slice(0, n), 2)
            high[i] = rows(i, d1, v1, m1, lambda n: slice(TILE - n, TILE), 1)

    def three(b):
        return pl.BlockSpec((3, step, TILE, width), lambda t: (0, t, b, 0))

    def one(b):
        return pl.BlockSpec((step, TILE, width), lambda t: (t, b, 0))

    return pl.pallas_call(
        kernel,
        grid=(radial // step,),
        in_specs=[one(0), one(last), three(0), three(last), three(0), three(last)],
        out_specs=[pl.BlockSpec((step, PACKED, width), lambda t: (t, 0, 0))] * 2,
        out_shape=[jax.ShapeDtypeStruct((radial, PACKED, width), jnp.float32)] * 2,
        name="pack_sides",
    )(density, density, velocity, velocity, magnetic, magnetic)


def interface_value(outer_left, inner_left, inner_right, outer_right):
    guess = 7.0 / 12.0 * (inner_left + inner_right) - 1.0 / 12.0 * (outer_left + outer_right)
    low = jnp.minimum(inner_left, inner_right)
    return jnp.minimum(jnp.maximum(guess, low), jnp.maximum(inner_left, inner_right))


def limited(centre, left_face, right_face):
    to_left = left_face - centre
    to_right = right_face - centre
    reach_right = 2.0 * jnp.abs(to_right)
    reach_left = 2.0 * jnp.abs(to_left)
    left = jnp.minimum(jnp.maximum(to_left, -reach_right), reach_right)
    right = jnp.minimum(jnp.maximum(to_right, -reach_left), reach_left)
    return centre + left, centre + right


def hll_flux(dens_left, dens_right, speed_left, speed_right):
    slowest = jnp.minimum(jnp.minimum(speed_left, speed_right) - SOUND_SPEED, 0.0)
    fastest = jnp.maximum(jnp.maximum(speed_left, speed_right) + SOUND_SPEED, 0.0)
    from_left = fastest * dens_left * (speed_left - slowest)
    from_right = slowest * dens_right * (speed_right - fastest)
    return (from_left - from_right) / (fastest - slowest)


PRIM_ROWS = ((0, 0, 3), (3, 3, 3), (1, 6, 1), (2, 7, 1))
MAG_ROWS_LOW = ((4, 8, 1), (5, 9, 1), (6, 10, 1))
MAG_ROWS_HIGH = ((4, 8, 1), (5, 9, 1), (6, 10, 2))
PACKED = 16


def stencil_kernel(middle, radial, azimuth, chunks, starts, refs, ghosts, outs, scratch):
    (s0, s1, s2, s3, s4, s5, s6, er, et, ep) = scratch[:10]
    carry_rho, carry_u, carry_flux, face_of_rho, face_of_u = scratch[10:]
    state = (s0, s1, s2, s3, s4, s5, s6)
    t = pl.program_id(0)
    width = s0.shape[-1]
    half = NPOL // 2
    slot = lax.rem(t, 8)
    layer = starts[0] + t - 3
    own = slice(FRONT, FRONT + azimuth)
    dens_out, mag_out = outs

    def low_lanes(rows):
        return lax.broadcasted_iota(jnp.int32, (rows, NPOL), 1) < half

    def ring(x):
        full = x.shape[1]
        mixed = jnp.where(low_lanes(x.shape[0]), x[:, full - NPOL :], x[:, :NPOL])
        return jnp.concatenate([x[:, NPOL : full - NPOL], mixed], axis=1)

    def outer(x, pol=None):
        lanes = low_lanes(x.shape[0])
        a, b = x[:, :NPOL], x[:, x.shape[1] - NPOL :]
        if pol is not None:
            a, b = jnp.where(lanes, pol, a), jnp.where(lanes, b, pol)
        return jnp.concatenate([a, b], axis=1)

    edge = azimuth + REACH

    def fill(fields, pols, low, high):
        for f, x in enumerate(fields):
            if middle:
                state[f][slot, own] = ring(x())
            elif f < 4:
                state[f][slot, own] = outer(x(), pols[f][:azimuth])
            else:
                state[f][slot, own] = outer(x())
        for f, row, n in PRIM_ROWS:
            a, b = low[row : row + n], high[row : row + n]
            if middle:
                a, b = ring(a), ring(b)
            else:
                a = outer(a, pols[f][edge - n : edge])
                b = outer(b, pols[f][edge : edge + n])
            state[f][slot, FRONT - n : FRONT] = a
            state[f][slot, FRONT + azimuth : FRONT + azimuth + n] = b
        shape = ring if middle else outer
        for f, row, n in MAG_ROWS_LOW:
            state[f][slot, FRONT - n : FRONT] = shape(low[row : row + n])
        for f, row, n in MAG_ROWS_HIGH:
            state[f][slot, FRONT + azimuth : FRONT + azimuth + n] = shape(high[row : row + n])

    mid_dens = mid_mag = None
    if middle:
        dens, vel, mag, side_low, side_high = refs
        fields = [lambda: dens[0]]
        fields += [lambda c=c: vel[c, 0] for c in range(3)]
        fields += [lambda c=c: mag[c, 0] for c in range(3)]
        choices = [(None, None)]
    else:
        d0, d1, v0, v1, m0, m1, pols, side_low, side_high, mid_dens, mid_mag = refs

        def both(a, b):
            return jnp.concatenate([a, b], axis=1)

        fields = [lambda: both(d0[0], d1[0])]
        fields += [lambda c=c: both(v0[c, 0], v1[c, 0]) for c in range(3)]
        fields += [lambda c=c: both(m0[c, 0], m1[c, 0]) for c in range(3)]
        choices = []
        for i, pol in enumerate(pols):
            inside = None
            if len(pols) > 1:
                at_layer = jnp.clip(layer, 0, radial - 1) - starts[2 + i]
                inside = (at_layer >= 0) & (at_layer < chunks[i])
            choices.append((pol, inside))
    mine = None if ghosts is None else (layer >= 0) & (layer < radial)
    for pol, inside in choices:
        def load(pol=pol):
            pieces = None if pol is None else [pol.at[c, 0] for c in range(4)]
            fill(fields, pieces, side_low.at[0], side_high.at[0])

        cond = mine if inside is None else inside if mine is None else mine & inside
        if cond is None:
            load()
        else:
            pl.when(cond)(load)
    if ghosts is not None:
        @pl.when(jnp.logical_not(mine))
        def _():
            planes = [lambda r=r: r[0] for r in ghosts[:7]]
            pieces = [r.at[0] for r in ghosts[9:]]
            fill(planes, pieces, ghosts[7].at[0], ghosts[8].at[0])

    shape = (TILE, width)
    lane = lax.broadcasted_iota(jnp.int32, shape, 1)
    sub = lax.broadcasted_iota(jnp.int32, shape, 0)

    def shifted(ref, index, base, off):
        here = ref[index, pl.ds(base, TILE), :]
        if off > 0:
            other = ref[index, pl.ds(base + TILE, TILE), :]
            return pltpu.roll(jnp.where(sub < off, other, here), TILE - off, 0)
        if off < 0:
            other = ref[index, pl.ds(base - TILE, TILE), :]
            return pltpu.roll(jnp.where(sub >= TILE + off, other, here), -off, 0)
        return here

    def at(ref, d, base, off=0):
        return shifted(ref, lax.rem(t - 3 + d + 8, 8), base, off)

    def up(x):
        rolled = pltpu.roll(x, width - 1, 1)
        return rolled if middle else jnp.where(lane == width - 1, x, rolled)

    def down(x):
        rolled = pltpu.roll(x, 1, 1)
        return rolled if middle else jnp.where(lane == 0, x, rolled)

    def before(x, previous):
        return jnp.where(sub == 0, pltpu.roll(previous, 1, 0), pltpu.roll(x, 1, 0))

    def azimuth_step(base, carry):
        rights, lefts, kept = [], [], []
        for field, past_face, past_right in ((s0, carry[0], carry[2]), (s3, carry[1], carry[3])):
            q = [at(field, 0, base, o) for o in (-1, 0, 1, 2)]
            face = interface_value(*q)
            left, right = limited(q[1], before(face, past_face), face)
            rights.append(before(right, past_right))
            lefts.append(left)
            kept.append((face, right))
        flux = hll_flux(rights[0], lefts[0], rights[1], lefts[1])
        return (kept[0][0], kept[1][0], kept[0][1], kept[1][1]), flux

    def theta_edges(q):
        below = down(q)
        face = interface_value(down(below), below, q, up(q))
        rolled = pltpu.roll(face, width - 1, 1)
        above = rolled if middle else jnp.where(lane == width - 1, q, rolled)
        return limited(q, face, above)

    here = lax.rem(t, 4)

    def emf_tile(j, _):
        base = pl.multiple_of(FRONT - TILE + j * TILE, TILE)
        u_r, u_t, u_p = (at(s, 1, base) for s in (s1, s2, s3))
        b_r = at(s4, 1, base) + at(s4, 2, base)
        b_t = at(s5, 1, base)
        b_t = b_t + up(b_t)
        b_p = at(s6, 1, base) + at(s6, 1, base, 1)
        rows = pl.ds(base, TILE)
        er[here, rows, :] = u_p * b_t - u_t * b_p
        et[here, rows, :] = u_r * b_p - u_p * b_r
        ep[here, rows, :] = u_t * b_r - u_r * b_t
        return 0

    @pl.when(t >= 4)
    def _():
        lax.fori_loop(0, azimuth // TILE + 2, emf_tile, 0, unroll=math.gcd(azimuth // TILE + 2, 6))

    def emf(ref, d, base, off=0):
        return shifted(ref, lax.rem(t - 1 + d + 4, 4), base, off)

    def radial_face(field, base):
        return interface_value(*(at(field, d, base) for d in (0, 1, 2, 3)))

    def radial_step(rows, base):
        face_rho, face_u = radial_face(s0, base), radial_face(s1, base)
        left_r, right_r = limited(at(s0, 1, base), face_of_rho[rows, :], face_rho)
        left_u, right_v = limited(at(s1, 1, base), face_of_u[rows, :], face_u)
        flux = hll_flux(carry_rho[rows, :], left_r, carry_u[rows, :], left_u)
        total = COURANT_RAD * (flux - carry_flux[rows, :])
        face_of_rho[rows, :] = face_rho
        face_of_u[rows, :] = face_u
        carry_rho[rows, :] = right_r
        carry_u[rows, :] = right_v
        carry_flux[rows, :] = flux
        return total

    def put(ref, index, rows, value, mid):
        if middle:
            ref[index + (rows, slice(None))] = value
            return
        inner = width + NPOL
        keep = lax.broadcasted_iota(jnp.int32, (TILE, NPOL), 1)
        mixed = mid[:, inner - NPOL :]
        quarter = half // 2
        first = jnp.where(keep < half + quarter, value[:, :NPOL], mixed)
        last = jnp.where(keep >= quarter, value[:, NPOL:], mixed)
        ref[index + (rows, slice(0, NPOL))] = first
        ref[index + (rows, slice(NPOL, inner))] = mid[:, : inner - NPOL]
        ref[index + (rows, slice(inner, inner + NPOL))] = last

    def middle_of(rows, c=None):
        if middle:
            return None
        return mid_dens[0, rows, :] if c is None else mid_mag[c, 0, rows, :]

    def tile(j, carry):
        kept, flux_low = carry
        start = pl.multiple_of(j * TILE, TILE)
        base = pl.multiple_of(FRONT + j * TILE, TILE)
        rows = pl.ds(start, TILE)

        total = radial_step(rows, base)

        kept, flux = azimuth_step(base + TILE, kept)
        flux_high = pltpu.roll(jnp.where(sub < 1, flux, flux_low), TILE - 1, 0)
        total = total + COURANT_AZI * (flux_high - flux_low)
        flux_low = flux

        rho = at(s0, 0, base)
        left_r, right_r = theta_edges(rho)
        left_u, right_v = theta_edges(at(s2, 0, base))
        theta_flux = hll_flux(down(right_r), left_r, down(right_v), left_u)
        if not middle:
            theta_flux = jnp.where(lane == 0, 0.0, theta_flux)
        above = pltpu.roll(theta_flux, width - 1, 1)
        if not middle:
            above = jnp.where(lane == width - 1, 0.0, above)
        total = total + COURANT_POL * (above - theta_flux)
        put(dens_out, (0,), rows, rho - total, middle_of(rows))

        er_low, er_here, er_high = (emf(er, 0, base, o) for o in (-1, 0, 1))
        ep_low, ep_here, ep_high = (emf(ep, d, base) for d in (-1, 0, 1))
        below_k = emf(et, -1, base, -1)
        edge_a = ep_low + ep_here
        edge_r = er_low + er_here
        mixed = (0.125 * COURANT_RAD) * (ep_high - ep_low) - (0.125 * COURANT_AZI) * (er_high - er_low)
        across = emf(et, -1, base, 1) + emf(et, 0, base, 1) - below_k - emf(et, 0, base, -1)
        along = emf(et, 1, base, -1) + emf(et, 1, base) - below_k - emf(et, -1, base)
        put(mag_out, (0, 0), rows,
            at(s4, 0, base)
            - (0.125 * COURANT_POL) * (up(edge_a) - down(edge_a))
            + (0.125 * COURANT_AZI) * across, middle_of(rows, 0))
        put(mag_out, (1, 0), rows, at(s5, 0, base) + (down(mixed) + mixed), middle_of(rows, 1))
        put(mag_out, (2, 0), rows,
            at(s6, 0, base)
            - (0.125 * COURANT_RAD) * along
            + (0.125 * COURANT_POL) * (up(edge_r) - down(edge_r)), middle_of(rows, 2))
        return kept, flux_low

    @pl.when(t == 3)
    def _():
        def warm_face(j, _):
            rows = pl.ds(pl.multiple_of(j * TILE, TILE), TILE)
            base = pl.multiple_of(FRONT + j * TILE, TILE)
            face_of_rho[rows, :] = radial_face(s0, base)
            face_of_u[rows, :] = radial_face(s1, base)
            return 0

        lax.fori_loop(0, azimuth // TILE, warm_face, 0, unroll=2)

    @pl.when((t >= 4) & (t < 6))
    def _():
        def warm(j, _):
            start = pl.multiple_of(j * TILE, TILE)
            radial_step(pl.ds(start, TILE), pl.multiple_of(FRONT + j * TILE, TILE))
            return 0

        lax.fori_loop(0, azimuth // TILE, warm, 0, unroll=2)

    @pl.when(t >= 6)
    def _():
        zero = jnp.zeros(shape, jnp.float32)
        kept, _ = azimuth_step(FRONT - TILE, (zero, zero, zero, zero))
        first = azimuth_step(FRONT, kept)
        unroll = math.gcd(azimuth // TILE, 4 if middle else 8)
        lax.fori_loop(0, azimuth // TILE, tile, first, unroll=unroll)


def stencil(middle, count, starts, fields, sides, ghosts=None, polar=None, mids=None, into=None):
    density, velocity, magnetic = fields
    radial, azimuth, width = density.shape
    tiles = width // NPOL

    def own(t, s):
        return jnp.clip(s[0] + t - 3, 0, radial - 1)

    def out(t, s):
        return s[1] + jnp.clip(t - 6, 0, count - 1)

    def one(w, index=0):
        return pl.BlockSpec((1, azimuth, w), lambda t, s: (own(t, s), 0, index))

    def three(w, index=0):
        return pl.BlockSpec((3, 1, azimuth, w), lambda t, s: (0, own(t, s), 0, index))

    def deep(t, s):
        g = s[0] + t - 3
        return jnp.clip(jnp.where(g < 0, g + 3, g - radial), 0, 2)

    def two(t, s):
        g = s[0] + t - 3
        return jnp.clip(jnp.where(g < 0, g + 2, g - radial), 0, 1)

    side = pl.BlockSpec((1, PACKED, width), lambda t, s: (own(t, s), 0, 0))
    chunks = []
    if middle:
        ring = width - NPOL
        out_width = ring
        args = [density, velocity, magnetic, *sides]
        specs = [one(width), three(width), three(width), side, side]
    else:
        ring = 2 * NPOL
        out_width = width
        chunks = [p.shape[1] for p in polar]
        args = [density, density, velocity, velocity, magnetic, magnetic, *polar, *sides, *mids]
        specs = [one(NPOL), one(NPOL, tiles - 1), three(NPOL), three(NPOL, tiles - 1),
                 three(NPOL), three(NPOL, tiles - 1)]
        for i, p in enumerate(polar):
            specs.append(pl.BlockSpec(
                (4, 1, azimuth + HALO, NPOL),
                lambda t, s, i=i: (0, jnp.clip(own(t, s) - s[2 + i], 0, chunks[i] - 1), 0, 0)))
        specs += [side, side]
        mid_width = width - NPOL
        specs += [pl.BlockSpec((1, azimuth, mid_width), lambda t, s: (out(t, s), 0, 0)),
                  pl.BlockSpec((3, 1, azimuth, mid_width), lambda t, s: (0, out(t, s), 0, 0))]
    used = len(args)
    extra = 0
    if ghosts is not None:
        planes, corner, filtered = ghosts
        where = [lambda t, s: deep(t, s), lambda t, s: 3 + deep(t, s), lambda t, s: 6, lambda t, s: 7]
        index = where + [lambda t, s: 8 + two(t, s), lambda t, s: 10, lambda t, s: 11]
        for f in index:
            args.append(planes)
            specs.append(pl.BlockSpec((1, azimuth, width), lambda t, s, f=f: (f(t, s), 0, 0)))
        for first in (0, 2):
            args.append(corner)
            specs.append(pl.BlockSpec(
                (1, PACKED, width), lambda t, s, first=first: (first + two(t, s), 0, 0)))
        if filtered is not None:
            for f in where:
                args.append(filtered)
                specs.append(pl.BlockSpec(
                    (1, azimuth + HALO, NPOL), lambda t, s, f=f: (f(t, s), 0, 0)))
        extra = len(args) - used
    aliases = {}
    if into is not None:
        for i, x in enumerate(into):
            aliases[1 + len(args)] = i
            args.append(x)
            specs.append(pl.BlockSpec(memory_space=pl.ANY))

    def kernel(starts, *refs):
        ins, outs, scratch = refs[:used], refs[len(args) : len(args) + 2], refs[len(args) + 2 :]
        spare = refs[used : used + extra] if extra else None
        if not middle:
            n = len(polar)
            ins = ins[:6] + (ins[6 : 6 + n],) + ins[6 + n :]
        stencil_kernel(middle, radial, azimuth, chunks, starts, ins, spare, outs, scratch)

    rows = FRONT + azimuth + 2 * TILE
    scratch = (
        [pltpu.VMEM((8, rows, ring), jnp.float32)] * 7
        + [pltpu.VMEM((4, rows, ring), jnp.float32)] * 3
        + [pltpu.VMEM((azimuth, ring), jnp.float32)] * 5
    )
    return pl.pallas_call(
        kernel,
        grid_spec=pltpu.PrefetchScalarGridSpec(
            num_scalar_prefetch=1,
            grid=(count + 6,),
            in_specs=specs,
            out_specs=[
                pl.BlockSpec((1, azimuth, out_width), lambda t, s: (out(t, s), 0, 0)),
                pl.BlockSpec((3, 1, azimuth, out_width), lambda t, s: (0, out(t, s), 0, 0)),
            ],
            scratch_shapes=scratch,
        ),
        out_shape=[
            jax.ShapeDtypeStruct((radial, azimuth, out_width), jnp.float32),
            jax.ShapeDtypeStruct((3, radial, azimuth, out_width), jnp.float32),
        ],
        input_output_aliases=aliases,
        compiler_params=pltpu.CompilerParams(
            dimension_semantics=("arbitrary",), vmem_limit_bytes=62 * 1024 * 1024
        ),
        cost_estimate=pl.CostEstimate(
            flops=1000 * count * azimuth * ring, bytes_accessed=48 * count * azimuth * width,
            transcendentals=0,
        ),
        name="section_mid" if middle else "section_polar",
    )(starts, *args)


def swap_rows(x):
    return lax.ppermute(x, "row", [(0, 1), (1, 0)])


def section(density, velocity, magnetic):
    radial, azimuth, width = density.shape
    devices = lax.axis_size("phi")
    pairs = 4 * radial // devices
    shares = [pairs - 1, 1] if pairs > 1 else [pairs]
    layers = [radial * n // pairs for n in shares]
    split = len(shares) > 1
    low = lax.axis_index("row") == 0
    fields = (density, velocity, magnetic)

    def pick(a, b):
        return jnp.where(low, jnp.int32(a), jnp.int32(b))

    def transpose(x, share, rows):
        x = x.reshape(devices, share, rows, NPOL)
        return lax.all_to_all(x, "phi", split_axis=0, concat_axis=0, tiled=True)

    base = [pick(radial - layers[0], 0)]
    if split:
        base.append(pick(0, layers[0]))
    packed = [pack_lines(density, velocity, b, n) for b, n in zip(base, layers)]
    first_rows, last_rows = pack_sides(density, velocity, magnetic)

    far, near, pair = pick(radial - 3, 0), pick(radial - 1, 0), pick(radial - 2, 0)

    def plane(x, c, n, start, size):
        return lax.dynamic_slice(x, (c, start, 0, 0), (n, size, azimuth, width)).reshape(
            n * size, azimuth, width)

    planes = jnp.concatenate(
        [lax.dynamic_slice_in_dim(density, far, 3, 0), plane(velocity, 0, 1, far, 3),
         plane(velocity, 1, 2, near, 1), plane(magnetic, 0, 1, pair, 2),
         plane(magnetic, 1, 2, near, 1)], axis=0)
    around = [(i, (i + 1) % devices) for i in range(devices)]
    back = [(j, i) for i, j in around]

    side_low = lax.ppermute(last_rows, "phi", around)
    side_high = lax.ppermute(first_rows, "phi", back)
    sides = (side_low, side_high)
    lines = [transpose(packed[0], shares[0], azimuth)]
    planes = swap_rows(planes)

    def starts(s):
        return jnp.stack([s, s] + base)

    deep = radial - REACH
    mids = stencil(True, deep, starts(pick(0, REACH)), fields, sides)
    if split:
        packed[1], mids = lax.optimization_barrier((packed[1], tuple(mids)))
        lines.append(transpose(packed[1], shares[1], azimuth))
    corner = swap_rows(
        jnp.concatenate([lax.dynamic_slice_in_dim(x, pair, 2, 0) for x in sides], axis=0))

    smooth = [filter_lines(x, width) for x in lines]
    polar = [transpose(smooth[0], shares[0], azimuth + HALO)]
    mids = stencil(True, REACH, starts(pick(deep, 0)), fields, sides,
                   ghosts=(planes, corner, None), into=mids)
    if split:
        smooth[1], mids = lax.optimization_barrier((smooth[1], tuple(mids)))
        polar.append(transpose(smooth[1], shares[1], azimuth + HALO))
    polar = [p.reshape(4, n, azimuth + HALO, NPOL) for p, n in zip(polar, layers)]

    first = polar[0]
    far, near = pick(layers[0] - 3, 0), pick(layers[0] - 1, 0)
    sent = lax.dynamic_slice_in_dim(first[:2], far, 3, 1).reshape(6, azimuth + HALO, NPOL)
    close = lax.dynamic_slice_in_dim(first[2:], near, 1, 1).reshape(2, azimuth + HALO, NPOL)
    filtered = swap_rows(jnp.concatenate([sent, close], axis=0))

    edge = layers[0] - REACH
    out = stencil(False, edge, starts(pick(radial - edge, 0)), fields, sides,
                  ghosts=(planes, corner, filtered), polar=polar[:1], mids=mids)
    if split:
        polar[1], out = lax.optimization_barrier((polar[1], tuple(out)))
    out = stencil(False, radial - edge, starts(pick(0, edge)), fields, sides, polar=polar,
                  mids=mids, into=out)
    return tuple(out)


def solution(mesh):
    placed = (P("row", "phi", None), P(None, "row", "phi", None), P(None, "row", "phi", None))
    return jax.shard_map(
        section,
        mesh=mesh,
        in_specs=placed,
        out_specs=(P("row", "phi", None), P(None, "row", "phi", None)),
        check_vma=False,
    )
```

```python
import math

import jax
import jax.numpy as jnp
import numpy as np
from jax import lax
from jax.experimental import pallas as pl
from jax.experimental.pallas import tpu as pltpu
from jax.sharding import PartitionSpec as P


NPOL = 128
RADIX = 16
FRONT = 16
TILE = 8
HALO = 8
REACH = 3

COURANT_RAD = 0.3
COURANT_POL = 0.25
COURANT_AZI = 0.35
SOUND_SPEED = 1.0


def rotate(value, angle):
    re, im = value
    c, s = math.cos(angle), math.sin(angle)
    if im is None:
        return (re * c, re * s)
    return (re * c - im * s, re * s + im * c)


def add(a, b, sign=1.0):
    def part(x, y):
        if y is None:
            return x
        if x is None:
            return y if sign > 0 else -y
        return x + y if sign > 0 else x - y

    return (part(a[0], b[0]), part(a[1], b[1]))


def conj(a):
    return (a[0], None if a[1] is None else -a[1])


def real_fft(xs):
    n = len(xs)
    if n == 1:
        return [(xs[0], None)]
    if n == 2:
        return [(xs[0] + xs[1], None), (xs[0] - xs[1], None)]
    even, odd = real_fft(xs[0::2]), real_fft(xs[1::2])
    half = n // 2

    def at(spec, k):
        return spec[k] if k <= half // 2 else conj(spec[half - k])

    result = []
    for k in range(half + 1):
        e, o = at(even, k % half), at(odd, k % half)
        if k == 0:
            result.append(add(e, o))
        elif k == half:
            result.append(add(e, o, -1.0))
        elif 4 * k == n:
            result.append((e[0], -o[0]))
        else:
            result.append(add(e, rotate(o, -2.0 * math.pi * k / n)))
    return result


def real_ifft(spec, n):
    if n == 2:
        a, b = spec[0][0], spec[1][0]
        return [a + b, a - b]
    half = n // 2
    even, odd = [], []
    for k in range(half // 2 + 1):
        a, b = spec[k], conj(spec[half - k])
        if k == 0:
            a, b = (spec[0][0], None), (spec[half][0], None)
            even.append(add(a, b))
            odd.append(add(a, b, -1.0))
        elif 4 * k == n:
            even.append((2.0 * spec[k][0], None))
            odd.append((-2.0 * spec[k][1], None))
        else:
            even.append(add(a, b))
            odd.append(rotate(add(a, b, -1.0), 2.0 * math.pi * k / n))
    evens, odds = real_ifft(even, half), real_ifft(odd, half)
    return [v for pair in zip(evens, odds) for v in pair]


def filter_tables(cells, theta_count):
    inner = cells // RADIX
    half_polar = NPOL // 2
    k2 = np.arange(RADIX // 2 + 1)[:, None]
    mode = k2 + RADIX * np.arange(inner)[None, :]
    angle = 2.0 * np.pi / cells * ((mode[:, :, None] * np.arange(inner)) % cells)
    cos, sin = np.cos(angle), np.sin(angle)
    forward = np.concatenate(
        [np.concatenate([cos, sin], 2), np.concatenate([-sin, cos], 2)], 1
    ).astype(np.float32)
    rows = np.arange(NPOL)
    theta = np.where(rows < half_polar, rows, theta_count - NPOL + rows)
    row_square = np.sin(np.pi * (theta + 0.5) / theta_count) ** 2
    edge = np.sin(np.pi * (half_polar + 0.5) / theta_count)
    mode_square = (edge * np.sin(np.pi * mode / cells)) ** 2
    damping = row_square / np.maximum(row_square, mode_square[:, :, None])
    return forward, (damping / cells).astype(np.float32)


def filter_kernel(group, inner, blocks, *refs):
    x_refs = refs[:group]
    basis_ref, damp_ref, out_ref = refs[group:]
    devices, _, azimuth, _ = x_refs[0].shape

    def slab(d):
        parts = [
            x_refs[g][d * blocks : (d + 1) * blocks, 0].reshape(inner, NPOL) for g in range(group)
        ]
        return jnp.concatenate(parts, axis=1) if group > 1 else parts[0]

    spectrum = real_fft([slab(d) for d in range(RADIX)])
    filtered = []
    for k, (re, im) in enumerate(spectrum):
        basis = basis_ref[k]
        if im is None:
            forward = basis[:, :inner]
            stacked = re
        else:
            forward = basis
            stacked = jnp.concatenate([re, im], axis=0)
        modes = jnp.dot(
            forward, stacked, precision=lax.Precision.HIGHEST, preferred_element_type=jnp.float32
        )
        damp = damp_ref[k]
        damp = jnp.concatenate([damp, damp], axis=0)
        if group > 1:
            damp = jnp.concatenate([damp] * group, axis=1)
        back = lax.dot_general(
            forward,
            modes * damp,
            (((0,), (0,)), ((), ())),
            precision=lax.Precision.HIGHEST,
            preferred_element_type=jnp.float32,
        )
        filtered.append((back, None) if im is None else (back[:inner], back[inner:]))
    for d, value in enumerate(real_ifft(filtered, RADIX)):
        for g in range(group):
            out_ref[d * blocks : (d + 1) * blocks, g, :azimuth] = value[
                :, g * NPOL : (g + 1) * NPOL
            ].reshape(blocks, azimuth, NPOL)
    blank = jnp.zeros((HALO - 2 * REACH, NPOL), jnp.float32)
    for d in range(devices):
        for g in range(group):
            below = out_ref[(d - 1) % devices, g, azimuth - REACH : azimuth]
            above = out_ref[(d + 1) % devices, g, :REACH]
            out_ref[d, g, azimuth:] = jnp.concatenate([below, above, blank], axis=0)


def filter_lines(lines, first, group, theta_count):
    devices, _, azimuth, _ = lines.shape
    cells = devices * azimuth
    inner = cells // RADIX
    blocks = inner // azimuth
    forward, damping = filter_tables(cells, theta_count)

    def slot(g):
        return pl.BlockSpec((devices, 1, azimuth, NPOL), lambda p: (0, first + g, 0, 0))

    shape = (devices, group, azimuth + HALO, NPOL)
    return pl.pallas_call(
        lambda *refs: filter_kernel(group, inner, blocks, *refs),
        grid=(1,),
        in_specs=[slot(g) for g in range(group)]
        + [
            pl.BlockSpec(forward.shape, lambda p: (0, 0, 0)),
            pl.BlockSpec(damping.shape, lambda p: (0, 0, 0)),
        ],
        out_specs=pl.BlockSpec(shape, lambda p: (0, 0, 0, 0)),
        out_shape=jax.ShapeDtypeStruct(shape, jnp.float32),
        compiler_params=pltpu.CompilerParams(vmem_limit_bytes=56 * 1024 * 1024),
        cost_estimate=pl.CostEstimate(
            flops=32 * inner * cells * NPOL * group, bytes_accessed=8 * lines.size, transcendentals=0
        ),
        name="polar_filter",
    )(*[lines] * group, jnp.asarray(forward), jnp.asarray(damping))


def pack_lines(density, velocity, order, first, slots, depth):
    _, azimuth, width = density.shape
    half = NPOL // 2
    last = width // NPOL - 1

    def kernel(order, d0, d1, v0, v1, out):
        lane = lax.broadcasted_iota(jnp.int32, (azimuth, NPOL), 1)
        for i in range(depth):
            out[0, i, 0] = jnp.where(lane < half, d0[i], d1[i])
            for c in range(3):
                out[1 + c, i, 0] = jnp.where(lane < half, v0[c, i], v1[c, i])

    def block(t, s):
        return s[0] + (first + t) * s[1]

    def dens(tile):
        return pl.BlockSpec((depth, azimuth, NPOL), lambda t, s: (block(t, s), 0, tile))

    def vel(tile):
        return pl.BlockSpec((3, depth, azimuth, NPOL), lambda t, s: (0, block(t, s), 0, tile))

    return pl.pallas_call(
        kernel,
        grid_spec=pltpu.PrefetchScalarGridSpec(
            num_scalar_prefetch=1,
            grid=(slots,),
            in_specs=[dens(0), dens(last), vel(0), vel(last)],
            out_specs=pl.BlockSpec((4, depth, 1, azimuth, NPOL), lambda t, s: (0, 0, t, 0, 0)),
        ),
        out_shape=jax.ShapeDtypeStruct((4, depth, slots, azimuth, NPOL), jnp.float32),
        name="pack_lines",
    )(order, density, density, velocity, velocity)


def pack_sides(density, velocity, magnetic):
    radial, azimuth, width = density.shape
    last = azimuth // TILE - 1
    step = 4 if radial % 4 == 0 else 1

    def kernel(d0, d1, v0, v1, m0, m1, low, high):
        def rows(i, dens, vel, mag, pick, wide):
            parts = [dens[i, pick(REACH)], vel[2, i, pick(REACH)], vel[0, i, pick(1)], vel[1, i, pick(1)]]
            parts += [mag[0, i, pick(1)], mag[1, i, pick(1)], mag[2, i, pick(wide)]]
            used = sum(p.shape[0] for p in parts)
            parts.append(jnp.zeros((PACKED - used, width), jnp.float32))
            return jnp.concatenate(parts, axis=0)

        for i in range(step):
            low[i] = rows(i, d0, v0, m0, lambda n: slice(0, n), 2)
            high[i] = rows(i, d1, v1, m1, lambda n: slice(TILE - n, TILE), 1)

    def three(b):
        return pl.BlockSpec((3, step, TILE, width), lambda t: (0, t, b, 0))

    def one(b):
        return pl.BlockSpec((step, TILE, width), lambda t: (t, b, 0))

    return pl.pallas_call(
        kernel,
        grid=(radial // step,),
        in_specs=[one(0), one(last), three(0), three(last), three(0), three(last)],
        out_specs=[pl.BlockSpec((step, PACKED, width), lambda t: (t, 0, 0))] * 2,
        out_shape=[jax.ShapeDtypeStruct((radial, PACKED, width), jnp.float32)] * 2,
        name="pack_sides",
    )(density, density, velocity, velocity, magnetic, magnetic)


def interface_value(outer_left, inner_left, inner_right, outer_right):
    guess = 7.0 / 12.0 * (inner_left + inner_right) - 1.0 / 12.0 * (outer_left + outer_right)
    low = jnp.minimum(inner_left, inner_right)
    return jnp.minimum(jnp.maximum(guess, low), jnp.maximum(inner_left, inner_right))


def limited(centre, left_face, right_face):
    to_left = left_face - centre
    to_right = right_face - centre
    reach_right = 2.0 * jnp.abs(to_right)
    reach_left = 2.0 * jnp.abs(to_left)
    left = jnp.minimum(jnp.maximum(to_left, -reach_right), reach_right)
    right = jnp.minimum(jnp.maximum(to_right, -reach_left), reach_left)
    return centre + left, centre + right


def hll_flux(dens_left, dens_right, speed_left, speed_right):
    slowest = jnp.minimum(jnp.minimum(speed_left, speed_right) - SOUND_SPEED, 0.0)
    fastest = jnp.maximum(jnp.maximum(speed_left, speed_right) + SOUND_SPEED, 0.0)
    from_left = fastest * dens_left * (speed_left - slowest)
    from_right = slowest * dens_right * (speed_right - fastest)
    return (from_left - from_right) / (fastest - slowest)


PRIM_ROWS = ((0, 0, 3), (3, 3, 3), (1, 6, 1), (2, 7, 1))
MAG_ROWS_LOW = ((4, 8, 1), (5, 9, 1), (6, 10, 1))
MAG_ROWS_HIGH = ((4, 8, 1), (5, 9, 1), (6, 10, 2))
PACKED = 16


def stencil_kernel(middle, radial, azimuth, parts, starts, refs, ghosts, outs, scratch):
    (s0, s1, s2, s3, s4, s5, s6, er, et, ep) = scratch[:10]
    carry_rho, carry_u, carry_flux, face_of_rho, face_of_u = scratch[10:]
    state = (s0, s1, s2, s3, s4, s5, s6)
    t = pl.program_id(0)
    width = s0.shape[-1]
    half = NPOL // 2
    slot = lax.rem(t, 8)
    layer = starts[0] + t - 3
    own = slice(FRONT, FRONT + azimuth)
    dens_out, mag_out = outs

    def low_lanes(rows):
        return lax.broadcasted_iota(jnp.int32, (rows, NPOL), 1) < half

    def ring(x):
        full = x.shape[1]
        mixed = jnp.where(low_lanes(x.shape[0]), x[:, full - NPOL :], x[:, :NPOL])
        return jnp.concatenate([x[:, NPOL : full - NPOL], mixed], axis=1)

    def outer(x, pol=None):
        lanes = low_lanes(x.shape[0])
        a, b = x[:, :NPOL], x[:, x.shape[1] - NPOL :]
        if pol is not None:
            a, b = jnp.where(lanes, pol, a), jnp.where(lanes, b, pol)
        return jnp.concatenate([a, b], axis=1)

    edge = azimuth + REACH

    def fill(fields, pols, low, high):
        for f, x in enumerate(fields):
            if middle:
                state[f][slot, own] = ring(x())
            elif f < 4:
                state[f][slot, own] = outer(x(), pols[f][:azimuth])
            else:
                state[f][slot, own] = outer(x())
        for f, row, n in PRIM_ROWS:
            a, b = low[row : row + n], high[row : row + n]
            if middle:
                a, b = ring(a), ring(b)
            else:
                a = outer(a, pols[f][edge - n : edge])
                b = outer(b, pols[f][edge : edge + n])
            state[f][slot, FRONT - n : FRONT] = a
            state[f][slot, FRONT + azimuth : FRONT + azimuth + n] = b
        shape = ring if middle else outer
        for f, row, n in MAG_ROWS_LOW:
            state[f][slot, FRONT - n : FRONT] = shape(low[row : row + n])
        for f, row, n in MAG_ROWS_HIGH:
            state[f][slot, FRONT + azimuth : FRONT + azimuth + n] = shape(high[row : row + n])

    mid_dens = mid_mag = None
    if middle:
        dens, vel, mag, side_low, side_high = refs
        fields = [lambda: dens[0]]
        fields += [lambda c=c: vel[c, 0] for c in range(3)]
        fields += [lambda c=c: mag[c, 0] for c in range(3)]
        choices = [(None, None)]
    else:
        d0, d1, v0, v1, m0, m1, pols, side_low, side_high, mid_dens, mid_mag = refs

        def both(a, b):
            return jnp.concatenate([a, b], axis=1)

        fields = [lambda: both(d0[0], d1[0])]
        fields += [lambda c=c: both(v0[c, 0], v1[c, 0]) for c in range(3)]
        fields += [lambda c=c: both(m0[c, 0], m1[c, 0]) for c in range(3)]
        choices = []
        for (first, slots, depth), pol in zip(parts, pols):
            inside = None
            if len(pols) > 1:
                block = jnp.clip(layer, 0, radial - 1) // depth
                place = (block - starts[2]) * starts[3] - first
                inside = (place >= 0) & (place < slots)
            choices.append((pol, inside))
    mine = None if ghosts is None else (layer >= 0) & (layer < radial)
    for pol, inside in choices:
        def load(pol=pol):
            pieces = None if pol is None else [pol.at[c, 0, 0] for c in range(4)]
            fill(fields, pieces, side_low.at[0], side_high.at[0])

        cond = mine if inside is None else inside if mine is None else mine & inside
        if cond is None:
            load()
        else:
            pl.when(cond)(load)
    if ghosts is not None:
        @pl.when(jnp.logical_not(mine))
        def _():
            planes = [lambda r=r: r[0] for r in ghosts[:7]]
            pieces = [r.at[0] for r in ghosts[9:]]
            fill(planes, pieces, ghosts[7].at[0], ghosts[8].at[0])

    shape = (TILE, width)
    lane = lax.broadcasted_iota(jnp.int32, shape, 1)
    sub = lax.broadcasted_iota(jnp.int32, shape, 0)

    def shifted(ref, index, base, off):
        here = ref[index, pl.ds(base, TILE), :]
        if off > 0:
            other = ref[index, pl.ds(base + TILE, TILE), :]
            return pltpu.roll(jnp.where(sub < off, other, here), TILE - off, 0)
        if off < 0:
            other = ref[index, pl.ds(base - TILE, TILE), :]
            return pltpu.roll(jnp.where(sub >= TILE + off, other, here), -off, 0)
        return here

    def at(ref, d, base, off=0):
        return shifted(ref, lax.rem(t - 3 + d + 8, 8), base, off)

    def up(x):
        rolled = pltpu.roll(x, width - 1, 1)
        return rolled if middle else jnp.where(lane == width - 1, x, rolled)

    def down(x):
        rolled = pltpu.roll(x, 1, 1)
        return rolled if middle else jnp.where(lane == 0, x, rolled)

    def before(x, previous):
        return jnp.where(sub == 0, pltpu.roll(previous, 1, 0), pltpu.roll(x, 1, 0))

    def azimuth_step(base, carry):
        rights, lefts, kept = [], [], []
        for field, past_face, past_right in ((s0, carry[0], carry[2]), (s3, carry[1], carry[3])):
            q = [at(field, 0, base, o) for o in (-1, 0, 1, 2)]
            face = interface_value(*q)
            left, right = limited(q[1], before(face, past_face), face)
            rights.append(before(right, past_right))
            lefts.append(left)
            kept.append((face, right))
        flux = hll_flux(rights[0], lefts[0], rights[1], lefts[1])
        return (kept[0][0], kept[1][0], kept[0][1], kept[1][1]), flux

    def theta_edges(q):
        below = down(q)
        face = interface_value(down(below), below, q, up(q))
        rolled = pltpu.roll(face, width - 1, 1)
        above = rolled if middle else jnp.where(lane == width - 1, q, rolled)
        return limited(q, face, above)

    here = lax.rem(t, 4)

    def emf_tile(j, _):
        base = pl.multiple_of(FRONT - TILE + j * TILE, TILE)
        u_r, u_t, u_p = (at(s, 1, base) for s in (s1, s2, s3))
        b_r = at(s4, 1, base) + at(s4, 2, base)
        b_t = at(s5, 1, base)
        b_t = b_t + up(b_t)
        b_p = at(s6, 1, base) + at(s6, 1, base, 1)
        rows = pl.ds(base, TILE)
        er[here, rows, :] = u_p * b_t - u_t * b_p
        et[here, rows, :] = u_r * b_p - u_p * b_r
        ep[here, rows, :] = u_t * b_r - u_r * b_t
        return 0

    @pl.when(t >= 4)
    def _():
        lax.fori_loop(0, azimuth // TILE + 2, emf_tile, 0, unroll=math.gcd(azimuth // TILE + 2, 6))

    def emf(ref, d, base, off=0):
        return shifted(ref, lax.rem(t - 1 + d + 4, 4), base, off)

    def radial_face(field, base):
        return interface_value(*(at(field, d, base) for d in (0, 1, 2, 3)))

    def radial_step(rows, base):
        face_rho, face_u = radial_face(s0, base), radial_face(s1, base)
        left_r, right_r = limited(at(s0, 1, base), face_of_rho[rows, :], face_rho)
        left_u, right_v = limited(at(s1, 1, base), face_of_u[rows, :], face_u)
        flux = hll_flux(carry_rho[rows, :], left_r, carry_u[rows, :], left_u)
        total = COURANT_RAD * (flux - carry_flux[rows, :])
        face_of_rho[rows, :] = face_rho
        face_of_u[rows, :] = face_u
        carry_rho[rows, :] = right_r
        carry_u[rows, :] = right_v
        carry_flux[rows, :] = flux
        return total

    def put(ref, index, rows, value, mid):
        if middle:
            ref[index + (rows, slice(None))] = value
            return
        inner = width + NPOL
        keep = lax.broadcasted_iota(jnp.int32, (TILE, NPOL), 1)
        mixed = mid[:, inner - NPOL :]
        quarter = half // 2
        first = jnp.where(keep < half + quarter, value[:, :NPOL], mixed)
        last = jnp.where(keep >= quarter, value[:, NPOL:], mixed)
        ref[index + (rows, slice(0, NPOL))] = first
        ref[index + (rows, slice(NPOL, inner))] = mid[:, : inner - NPOL]
        ref[index + (rows, slice(inner, inner + NPOL))] = last

    def middle_of(rows, c=None):
        if middle:
            return None
        return mid_dens[0, rows, :] if c is None else mid_mag[c, 0, rows, :]

    def tile(j, carry):
        kept, flux_low = carry
        start = pl.multiple_of(j * TILE, TILE)
        base = pl.multiple_of(FRONT + j * TILE, TILE)
        rows = pl.ds(start, TILE)

        total = radial_step(rows, base)

        kept, flux = azimuth_step(base + TILE, kept)
        flux_high = pltpu.roll(jnp.where(sub < 1, flux, flux_low), TILE - 1, 0)
        total = total + COURANT_AZI * (flux_high - flux_low)
        flux_low = flux

        rho = at(s0, 0, base)
        left_r, right_r = theta_edges(rho)
        left_u, right_v = theta_edges(at(s2, 0, base))
        theta_flux = hll_flux(down(right_r), left_r, down(right_v), left_u)
        if not middle:
            theta_flux = jnp.where(lane == 0, 0.0, theta_flux)
        above = pltpu.roll(theta_flux, width - 1, 1)
        if not middle:
            above = jnp.where(lane == width - 1, 0.0, above)
        total = total + COURANT_POL * (above - theta_flux)
        put(dens_out, (0,), rows, rho - total, middle_of(rows))

        er_low, er_here, er_high = (emf(er, 0, base, o) for o in (-1, 0, 1))
        ep_low, ep_here, ep_high = (emf(ep, d, base) for d in (-1, 0, 1))
        below_k = emf(et, -1, base, -1)
        edge_a = ep_low + ep_here
        edge_r = er_low + er_here
        mixed = (0.125 * COURANT_RAD) * (ep_high - ep_low) - (0.125 * COURANT_AZI) * (er_high - er_low)
        across = emf(et, -1, base, 1) + emf(et, 0, base, 1) - below_k - emf(et, 0, base, -1)
        along = emf(et, 1, base, -1) + emf(et, 1, base) - below_k - emf(et, -1, base)
        put(mag_out, (0, 0), rows,
            at(s4, 0, base)
            - (0.125 * COURANT_POL) * (up(edge_a) - down(edge_a))
            + (0.125 * COURANT_AZI) * across, middle_of(rows, 0))
        put(mag_out, (1, 0), rows, at(s5, 0, base) + (down(mixed) + mixed), middle_of(rows, 1))
        put(mag_out, (2, 0), rows,
            at(s6, 0, base)
            - (0.125 * COURANT_RAD) * along
            + (0.125 * COURANT_POL) * (up(edge_r) - down(edge_r)), middle_of(rows, 2))
        return kept, flux_low

    @pl.when(t == 3)
    def _():
        def warm_face(j, _):
            rows = pl.ds(pl.multiple_of(j * TILE, TILE), TILE)
            base = pl.multiple_of(FRONT + j * TILE, TILE)
            face_of_rho[rows, :] = radial_face(s0, base)
            face_of_u[rows, :] = radial_face(s1, base)
            return 0

        lax.fori_loop(0, azimuth // TILE, warm_face, 0, unroll=2)

    @pl.when((t >= 4) & (t < 6))
    def _():
        def warm(j, _):
            start = pl.multiple_of(j * TILE, TILE)
            radial_step(pl.ds(start, TILE), pl.multiple_of(FRONT + j * TILE, TILE))
            return 0

        lax.fori_loop(0, azimuth // TILE, warm, 0, unroll=2)

    @pl.when(t >= 6)
    def _():
        zero = jnp.zeros(shape, jnp.float32)
        kept, _ = azimuth_step(FRONT - TILE, (zero, zero, zero, zero))
        first = azimuth_step(FRONT, kept)
        unroll = math.gcd(azimuth // TILE, 4 if middle else 8)
        lax.fori_loop(0, azimuth // TILE, tile, first, unroll=unroll)


def stencil(middle, count, starts, fields, sides, ghosts=None, polar=None, mids=None, into=None):
    density, velocity, magnetic = fields
    radial, azimuth, width = density.shape
    tiles = width // NPOL

    def own(t, s):
        return jnp.clip(s[0] + t - 3, 0, radial - 1)

    def out(t, s):
        return s[1] + jnp.clip(t - 6, 0, count - 1)

    def one(w, index=0):
        return pl.BlockSpec((1, azimuth, w), lambda t, s: (own(t, s), 0, index))

    def three(w, index=0):
        return pl.BlockSpec((3, 1, azimuth, w), lambda t, s: (0, own(t, s), 0, index))

    def deep(t, s):
        g = s[0] + t - 3
        return jnp.clip(jnp.where(g < 0, g + 3, g - radial), 0, 2)

    def two(t, s):
        g = s[0] + t - 3
        return jnp.clip(jnp.where(g < 0, g + 2, g - radial), 0, 1)

    side = pl.BlockSpec((1, PACKED, width), lambda t, s: (own(t, s), 0, 0))
    parts = []
    if middle:
        ring = width - NPOL
        out_width = ring
        args = [density, velocity, magnetic, *sides]
        specs = [one(width), three(width), three(width), side, side]
    else:
        ring = 2 * NPOL
        out_width = width
        parts = [(first, p.shape[2], p.shape[1]) for first, p in polar]
        polar = [p for _, p in polar]
        args = [density, density, velocity, velocity, magnetic, magnetic, *polar, *sides, *mids]
        specs = [one(NPOL), one(NPOL, tiles - 1), three(NPOL), three(NPOL, tiles - 1),
                 three(NPOL), three(NPOL, tiles - 1)]

        def place(t, s, part):
            first, slots, depth = part
            block = own(t, s) // depth
            return jnp.clip((block - s[2]) * s[3] - first, 0, slots - 1)

        for part in parts:
            specs.append(pl.BlockSpec(
                (4, 1, 1, azimuth + HALO, NPOL),
                lambda t, s, part=part: (0, own(t, s) % part[2], place(t, s, part), 0, 0)))
        specs += [side, side]
        mid_width = width - NPOL
        specs += [pl.BlockSpec((1, azimuth, mid_width), lambda t, s: (out(t, s), 0, 0)),
                  pl.BlockSpec((3, 1, azimuth, mid_width), lambda t, s: (0, out(t, s), 0, 0))]
    used = len(args)
    extra = 0
    if ghosts is not None:
        planes, corner, filtered = ghosts
        where = [lambda t, s: deep(t, s), lambda t, s: 3 + deep(t, s), lambda t, s: 6, lambda t, s: 7]
        index = where + [lambda t, s: 8 + two(t, s), lambda t, s: 10, lambda t, s: 11]
        for f in index:
            args.append(planes)
            specs.append(pl.BlockSpec((1, azimuth, width), lambda t, s, f=f: (f(t, s), 0, 0)))
        for first in (0, 2):
            args.append(corner)
            specs.append(pl.BlockSpec(
                (1, PACKED, width), lambda t, s, first=first: (first + two(t, s), 0, 0)))
        if filtered is not None:
            for f in where:
                args.append(filtered)
                specs.append(pl.BlockSpec(
                    (1, azimuth + HALO, NPOL), lambda t, s, f=f: (f(t, s), 0, 0)))
        extra = len(args) - used
    aliases = {}
    if into is not None:
        for i, x in enumerate(into):
            aliases[1 + len(args)] = i
            args.append(x)
            specs.append(pl.BlockSpec(memory_space=pl.ANY))

    def kernel(starts, *refs):
        ins, outs, scratch = refs[:used], refs[len(args) : len(args) + 2], refs[len(args) + 2 :]
        spare = refs[used : used + extra] if extra else None
        if not middle:
            n = len(polar)
            ins = ins[:6] + (ins[6 : 6 + n],) + ins[6 + n :]
        stencil_kernel(middle, radial, azimuth, parts, starts, ins, spare, outs, scratch)

    rows = FRONT + azimuth + 2 * TILE
    scratch = (
        [pltpu.VMEM((8, rows, ring), jnp.float32)] * 7
        + [pltpu.VMEM((4, rows, ring), jnp.float32)] * 3
        + [pltpu.VMEM((azimuth, ring), jnp.float32)] * 5
    )
    return pl.pallas_call(
        kernel,
        grid_spec=pltpu.PrefetchScalarGridSpec(
            num_scalar_prefetch=1,
            grid=(count + 6,),
            in_specs=specs,
            out_specs=[
                pl.BlockSpec((1, azimuth, out_width), lambda t, s: (out(t, s), 0, 0)),
                pl.BlockSpec((3, 1, azimuth, out_width), lambda t, s: (0, out(t, s), 0, 0)),
            ],
            scratch_shapes=scratch,
        ),
        out_shape=[
            jax.ShapeDtypeStruct((radial, azimuth, out_width), jnp.float32),
            jax.ShapeDtypeStruct((3, radial, azimuth, out_width), jnp.float32),
        ],
        input_output_aliases=aliases,
        compiler_params=pltpu.CompilerParams(
            dimension_semantics=("arbitrary",), vmem_limit_bytes=62 * 1024 * 1024
        ),
        cost_estimate=pl.CostEstimate(
            flops=1000 * count * azimuth * ring, bytes_accessed=48 * count * azimuth * width,
            transcendentals=0,
        ),
        name="section_mid" if middle else "section_polar",
    )(starts, *args)


def swap_rows(x):
    return lax.ppermute(x, "row", [(0, 1), (1, 0)])


def section(density, velocity, magnetic):
    radial, azimuth, width = density.shape
    devices = lax.axis_size("phi")
    pairs = 4 * radial // devices
    depth = radial // pairs
    sent = [(0, pairs - 1), (pairs - 1, 1)] if pairs > 1 else [(0, 1)]
    returned = [(0, 1)]
    if pairs > 2:
        returned.append((1, pairs - 2))
    if pairs > 1:
        returned.append((pairs - 1, 1))
    split = pairs > 1
    low = lax.axis_index("row") == 0
    fields = (density, velocity, magnetic)

    def pick(a, b):
        return jnp.where(low, jnp.int32(a), jnp.int32(b))

    def transpose(x, share, rows):
        x = x.reshape(devices, share, rows, NPOL)
        return lax.all_to_all(x, "phi", split_axis=0, concat_axis=0, tiled=True)

    order = jnp.stack([pick(pairs - 1, 0), pick(-1, 1)])
    packed = [pack_lines(density, velocity, order, a, n, depth) for a, n in sent]
    first_rows, last_rows = pack_sides(density, velocity, magnetic)

    far, near, pair = pick(radial - 3, 0), pick(radial - 1, 0), pick(radial - 2, 0)

    def plane(x, c, n, start, size):
        return lax.dynamic_slice(x, (c, start, 0, 0), (n, size, azimuth, width)).reshape(
            n * size, azimuth, width)

    planes = jnp.concatenate(
        [lax.dynamic_slice_in_dim(density, far, 3, 0), plane(velocity, 0, 1, far, 3),
         plane(velocity, 1, 2, near, 1), plane(magnetic, 0, 1, pair, 2),
         plane(magnetic, 1, 2, near, 1)], axis=0)
    around = [(i, (i + 1) % devices) for i in range(devices)]
    back = [(j, i) for i, j in around]

    side_low = lax.ppermute(last_rows, "phi", around)
    side_high = lax.ppermute(first_rows, "phi", back)
    sides = (side_low, side_high)
    lines = [transpose(packed[0], sent[0][1], azimuth)]
    planes = swap_rows(planes)

    def starts(s):
        return jnp.concatenate([jnp.stack([s, s]), order])

    deep = radial - REACH
    mids = stencil(True, deep, starts(pick(0, REACH)), fields, sides)
    if split:
        packed[1], mids = lax.optimization_barrier((packed[1], tuple(mids)))
        lines.append(transpose(packed[1], sent[1][1], azimuth))
    corner = swap_rows(
        jnp.concatenate([lax.dynamic_slice_in_dim(x, pair, 2, 0) for x in sides], axis=0))

    smooth = [filter_lines(lines[0], a, n, width) for a, n in returned[: max(1, len(returned) - 1)]]
    if split:
        smooth.append(filter_lines(lines[1], 0, 1, width))
    mids = stencil(True, REACH, starts(pick(deep, 0)), fields, sides,
                   ghosts=(planes, corner, None), into=mids)
    polar = []
    for i, (a, n) in enumerate(returned):
        if i + 1 < len(returned):
            smooth[i], smooth[i + 1] = lax.optimization_barrier((smooth[i], smooth[i + 1]))
        elif i > 0:
            smooth[i], mids = lax.optimization_barrier((smooth[i], tuple(mids)))
        back_again = transpose(smooth[i], n, azimuth + HALO)
        polar.append((a, back_again.reshape(4, depth, n, azimuth + HALO, NPOL)))

    first = polar[0][1][:, :, 0]
    far, near = pick(depth - 3, 0), pick(depth - 1, 0)
    ends = lax.dynamic_slice_in_dim(first[:2], far, 3, 1).reshape(6, azimuth + HALO, NPOL)
    close = lax.dynamic_slice_in_dim(first[2:], near, 1, 1).reshape(2, azimuth + HALO, NPOL)
    filtered = swap_rows(jnp.concatenate([ends, close], axis=0))

    edge = depth * sent[0][1] - REACH
    early = polar[:-1] if split else polar
    out = stencil(False, edge, starts(pick(radial - edge, 0)), fields, sides,
                  ghosts=(planes, corner, filtered), polar=early, mids=mids)
    if split:
        late, out = lax.optimization_barrier((polar[-1][1], tuple(out)))
        polar[-1] = (polar[-1][0], late)
    out = stencil(False, radial - edge, starts(pick(0, edge)), fields, sides, polar=polar,
                  mids=mids, into=out)
    return tuple(out)


def solution(mesh):
    placed = (P("row", "phi", None), P(None, "row", "phi", None), P(None, "row", "phi", None))
    return jax.shard_map(
        section,
        mesh=mesh,
        in_specs=placed,
        out_specs=(P("row", "phi", None), P(None, "row", "phi", None)),
        check_vma=False,
    )
```

```python
import math

import jax
import jax.numpy as jnp
import numpy as np
from jax import lax
from jax.experimental import pallas as pl
from jax.experimental.pallas import tpu as pltpu
from jax.sharding import PartitionSpec as P


NPOL = 128
RADIX = 16
FRONT = 16
TILE = 8
HALO = 8
REACH = 3

COURANT_RAD = 0.3
COURANT_POL = 0.25
COURANT_AZI = 0.35
SOUND_SPEED = 1.0


def rotate(value, angle):
    re, im = value
    c, s = math.cos(angle), math.sin(angle)
    if im is None:
        return (re * c, re * s)
    return (re * c - im * s, re * s + im * c)


def add(a, b, sign=1.0):
    def part(x, y):
        if y is None:
            return x
        if x is None:
            return y if sign > 0 else -y
        return x + y if sign > 0 else x - y

    return (part(a[0], b[0]), part(a[1], b[1]))


def conj(a):
    return (a[0], None if a[1] is None else -a[1])


def real_fft(xs):
    n = len(xs)
    if n == 1:
        return [(xs[0], None)]
    if n == 2:
        return [(xs[0] + xs[1], None), (xs[0] - xs[1], None)]
    even, odd = real_fft(xs[0::2]), real_fft(xs[1::2])
    half = n // 2

    def at(spec, k):
        return spec[k] if k <= half // 2 else conj(spec[half - k])

    result = []
    for k in range(half + 1):
        e, o = at(even, k % half), at(odd, k % half)
        if k == 0:
            result.append(add(e, o))
        elif k == half:
            result.append(add(e, o, -1.0))
        elif 4 * k == n:
            result.append((e[0], -o[0]))
        else:
            result.append(add(e, rotate(o, -2.0 * math.pi * k / n)))
    return result


def real_ifft(spec, n):
    if n == 2:
        a, b = spec[0][0], spec[1][0]
        return [a + b, a - b]
    half = n // 2
    even, odd = [], []
    for k in range(half // 2 + 1):
        a, b = spec[k], conj(spec[half - k])
        if k == 0:
            a, b = (spec[0][0], None), (spec[half][0], None)
            even.append(add(a, b))
            odd.append(add(a, b, -1.0))
        elif 4 * k == n:
            even.append((2.0 * spec[k][0], None))
            odd.append((-2.0 * spec[k][1], None))
        else:
            even.append(add(a, b))
            odd.append(rotate(add(a, b, -1.0), 2.0 * math.pi * k / n))
    evens, odds = real_ifft(even, half), real_ifft(odd, half)
    return [v for pair in zip(evens, odds) for v in pair]


def filter_tables(cells, theta_count):
    inner = cells // RADIX
    half_polar = NPOL // 2
    k2 = np.arange(RADIX // 2 + 1)[:, None]
    mode = k2 + RADIX * np.arange(inner)[None, :]
    angle = 2.0 * np.pi / cells * ((mode[:, :, None] * np.arange(inner)) % cells)
    waves = np.concatenate([np.cos(angle), np.sin(angle)], 2).astype(np.float32)
    rows = np.arange(NPOL)
    theta = np.where(rows < half_polar, rows, theta_count - NPOL + rows)
    row_square = np.sin(np.pi * (theta + 0.5) / theta_count) ** 2
    edge = np.sin(np.pi * (half_polar + 0.5) / theta_count)
    mode_square = (edge * np.sin(np.pi * mode / cells)) ** 2
    return (
        waves,
        np.broadcast_to(row_square, (TILE, NPOL)).astype(np.float32),
        np.ascontiguousarray(mode_square.T).astype(np.float32),
    )


def filter_kernel(group, inner, blocks, *refs):
    x_refs = refs[:group]
    waves_ref, row_ref, mode_ref, out_ref = refs[group:]
    devices, _, azimuth, _ = x_refs[0].shape

    def slab(d):
        parts = [
            x_refs[g][d * blocks : (d + 1) * blocks, 0].reshape(inner, NPOL) for g in range(group)
        ]
        return jnp.concatenate(parts, axis=1) if group > 1 else parts[0]

    spectrum = real_fft([slab(d) for d in range(RADIX)])
    filtered = []
    for k, (re, im) in enumerate(spectrum):
        waves = waves_ref[k]
        cos, sin = waves[:, :inner], waves[:, inner:]
        turned = jnp.concatenate([-sin, cos], axis=1)
        basis = jnp.concatenate([waves, turned], axis=0)
        if im is None:
            forward = basis[:, :inner]
            stacked = re
        else:
            forward = basis
            stacked = jnp.concatenate([re, im], axis=0)
        modes = jnp.dot(
            forward, stacked, precision=lax.Precision.HIGHEST, preferred_element_type=jnp.float32
        )
        row_square = row_ref[0:1, :]
        damp = row_square / jnp.maximum(row_square, mode_ref[:, k : k + 1])
        damp = damp * (1.0 / (inner * RADIX))
        damp = jnp.concatenate([damp, damp], axis=0)
        if group > 1:
            damp = jnp.concatenate([damp] * group, axis=1)
        back = lax.dot_general(
            forward,
            modes * damp,
            (((0,), (0,)), ((), ())),
            precision=lax.Precision.HIGHEST,
            preferred_element_type=jnp.float32,
        )
        filtered.append((back, None) if im is None else (back[:inner], back[inner:]))
    for d, value in enumerate(real_ifft(filtered, RADIX)):
        for g in range(group):
            out_ref[d * blocks : (d + 1) * blocks, g, :azimuth] = value[
                :, g * NPOL : (g + 1) * NPOL
            ].reshape(blocks, azimuth, NPOL)
    blank = jnp.zeros((HALO - 2 * REACH, NPOL), jnp.float32)
    for d in range(devices):
        for g in range(group):
            below = out_ref[(d - 1) % devices, g, azimuth - REACH : azimuth]
            above = out_ref[(d + 1) % devices, g, :REACH]
            out_ref[d, g, azimuth:] = jnp.concatenate([below, above, blank], axis=0)


def filter_lines(lines, first, group, theta_count):
    devices, _, azimuth, _ = lines.shape
    cells = devices * azimuth
    inner = cells // RADIX
    blocks = inner // azimuth
    tables = filter_tables(cells, theta_count)

    def slot(g):
        return pl.BlockSpec((devices, 1, azimuth, NPOL), lambda p: (0, first + g, 0, 0))

    shape = (devices, group, azimuth + HALO, NPOL)
    return pl.pallas_call(
        lambda *refs: filter_kernel(group, inner, blocks, *refs),
        grid=(1,),
        in_specs=[slot(g) for g in range(group)]
        + [pl.BlockSpec(x.shape, lambda p, n=x.ndim: (0,) * n) for x in tables],
        out_specs=pl.BlockSpec(shape, lambda p: (0, 0, 0, 0)),
        out_shape=jax.ShapeDtypeStruct(shape, jnp.float32),
        compiler_params=pltpu.CompilerParams(vmem_limit_bytes=56 * 1024 * 1024),
        cost_estimate=pl.CostEstimate(
            flops=32 * inner * cells * NPOL * group, bytes_accessed=8 * lines.size, transcendentals=0
        ),
        name="polar_filter",
    )(*[lines] * group, *[jnp.asarray(x) for x in tables])


def pack_lines(density, velocity, order, first, slots, depth):
    _, azimuth, width = density.shape
    half = NPOL // 2
    last = width // NPOL - 1

    cut = 2 if depth % 2 == 0 else 1
    step = depth // cut

    def kernel(order, d0, d1, v0, v1, out):
        lane = lax.broadcasted_iota(jnp.int32, (azimuth, NPOL), 1)
        for i in range(step):
            out[0, i, 0] = jnp.where(lane < half, d0[i], d1[i])
            for c in range(3):
                out[1 + c, i, 0] = jnp.where(lane < half, v0[c, i], v1[c, i])

    def block(t, h, s):
        return (s[0] + (first + t) * s[1]) * cut + h

    def dens(tile):
        return pl.BlockSpec((step, azimuth, NPOL), lambda t, h, s: (block(t, h, s), 0, tile))

    def vel(tile):
        return pl.BlockSpec((3, step, azimuth, NPOL), lambda t, h, s: (0, block(t, h, s), 0, tile))

    return pl.pallas_call(
        kernel,
        grid_spec=pltpu.PrefetchScalarGridSpec(
            num_scalar_prefetch=1,
            grid=(slots, cut),
            in_specs=[dens(0), dens(last), vel(0), vel(last)],
            out_specs=pl.BlockSpec(
                (4, step, 1, azimuth, NPOL), lambda t, h, s: (0, h, t, 0, 0)),
        ),
        out_shape=jax.ShapeDtypeStruct((4, depth, slots, azimuth, NPOL), jnp.float32),
        name="pack_lines",
    )(order, density, density, velocity, velocity)


def pack_sides(density, velocity, magnetic):
    radial, azimuth, width = density.shape
    last = azimuth // TILE - 1
    step = 4 if radial % 4 == 0 else 1

    def kernel(d0, d1, v0, v1, m0, m1, low, high):
        def rows(i, dens, vel, mag, pick, wide):
            parts = [dens[i, pick(REACH)], vel[2, i, pick(REACH)], vel[0, i, pick(1)], vel[1, i, pick(1)]]
            parts += [mag[0, i, pick(1)], mag[1, i, pick(1)], mag[2, i, pick(wide)]]
            used = sum(p.shape[0] for p in parts)
            parts.append(jnp.zeros((PACKED - used, width), jnp.float32))
            return jnp.concatenate(parts, axis=0)

        for i in range(step):
            low[i] = rows(i, d0, v0, m0, lambda n: slice(0, n), 2)
            high[i] = rows(i, d1, v1, m1, lambda n: slice(TILE - n, TILE), 1)

    def three(b):
        return pl.BlockSpec((3, step, TILE, width), lambda t: (0, t, b, 0))

    def one(b):
        return pl.BlockSpec((step, TILE, width), lambda t: (t, b, 0))

    return pl.pallas_call(
        kernel,
        grid=(radial // step,),
        in_specs=[one(0), one(last), three(0), three(last), three(0), three(last)],
        out_specs=[pl.BlockSpec((step, PACKED, width), lambda t: (t, 0, 0))] * 2,
        out_shape=[jax.ShapeDtypeStruct((radial, PACKED, width), jnp.float32)] * 2,
        name="pack_sides",
    )(density, density, velocity, velocity, magnetic, magnetic)


def interface_value(outer_left, inner_left, inner_right, outer_right):
    guess = 7.0 / 12.0 * (inner_left + inner_right) - 1.0 / 12.0 * (outer_left + outer_right)
    low = jnp.minimum(inner_left, inner_right)
    return jnp.minimum(jnp.maximum(guess, low), jnp.maximum(inner_left, inner_right))


def limited(centre, left_face, right_face):
    to_left = left_face - centre
    to_right = right_face - centre
    reach_right = 2.0 * jnp.abs(to_right)
    reach_left = 2.0 * jnp.abs(to_left)
    left = jnp.minimum(jnp.maximum(to_left, -reach_right), reach_right)
    right = jnp.minimum(jnp.maximum(to_right, -reach_left), reach_left)
    return centre + left, centre + right


def hll_flux(dens_left, dens_right, speed_left, speed_right):
    slowest = jnp.minimum(jnp.minimum(speed_left, speed_right) - SOUND_SPEED, 0.0)
    fastest = jnp.maximum(jnp.maximum(speed_left, speed_right) + SOUND_SPEED, 0.0)
    from_left = fastest * dens_left * (speed_left - slowest)
    from_right = slowest * dens_right * (speed_right - fastest)
    return (from_left - from_right) / (fastest - slowest)


PRIM_ROWS = ((0, 0, 3), (3, 3, 3), (1, 6, 1), (2, 7, 1))
MAG_ROWS_LOW = ((4, 8, 1), (5, 9, 1), (6, 10, 1))
MAG_ROWS_HIGH = ((4, 8, 1), (5, 9, 1), (6, 10, 2))
PACKED = 16


def stencil_kernel(middle, radial, azimuth, parts, starts, refs, ghosts, outs, scratch):
    (s0, s1, s2, s3, s4, s5, s6, er, et, ep) = scratch[:10]
    carry_rho, carry_u, carry_flux, face_of_rho, face_of_u = scratch[10:]
    state = (s0, s1, s2, s3, s4, s5, s6)
    t = pl.program_id(0)
    width = s0.shape[-1]
    half = NPOL // 2
    slot = lax.rem(t, 8)
    layer = starts[0] + t - 3
    own = slice(FRONT, FRONT + azimuth)
    dens_out, mag_out = outs

    def low_lanes(rows):
        return lax.broadcasted_iota(jnp.int32, (rows, NPOL), 1) < half

    def ring(x):
        full = x.shape[1]
        mixed = jnp.where(low_lanes(x.shape[0]), x[:, full - NPOL :], x[:, :NPOL])
        return jnp.concatenate([x[:, NPOL : full - NPOL], mixed], axis=1)

    def outer(x, pol=None):
        lanes = low_lanes(x.shape[0])
        a, b = x[:, :NPOL], x[:, x.shape[1] - NPOL :]
        if pol is not None:
            a, b = jnp.where(lanes, pol, a), jnp.where(lanes, b, pol)
        return jnp.concatenate([a, b], axis=1)

    edge = azimuth + REACH

    def fill(fields, pols, low, high):
        for f, x in enumerate(fields):
            if middle:
                state[f][slot, own] = ring(x())
            elif f < 4:
                state[f][slot, own] = outer(x(), pols[f][:azimuth])
            else:
                state[f][slot, own] = outer(x())
        for f, row, n in PRIM_ROWS:
            a, b = low[row : row + n], high[row : row + n]
            if middle:
                a, b = ring(a), ring(b)
            else:
                a = outer(a, pols[f][edge - n : edge])
                b = outer(b, pols[f][edge : edge + n])
            state[f][slot, FRONT - n : FRONT] = a
            state[f][slot, FRONT + azimuth : FRONT + azimuth + n] = b
        shape = ring if middle else outer
        for f, row, n in MAG_ROWS_LOW:
            state[f][slot, FRONT - n : FRONT] = shape(low[row : row + n])
        for f, row, n in MAG_ROWS_HIGH:
            state[f][slot, FRONT + azimuth : FRONT + azimuth + n] = shape(high[row : row + n])

    mid_dens = mid_mag = None
    if middle:
        dens, vel, mag, side_low, side_high = refs
        fields = [lambda: dens[0]]
        fields += [lambda c=c: vel[c, 0] for c in range(3)]
        fields += [lambda c=c: mag[c, 0] for c in range(3)]
        choices = [(None, None)]
    else:
        d0, d1, v0, v1, m0, m1, pols, side_low, side_high, mid_dens, mid_mag = refs

        def both(a, b):
            return jnp.concatenate([a, b], axis=1)

        fields = [lambda: both(d0[0], d1[0])]
        fields += [lambda c=c: both(v0[c, 0], v1[c, 0]) for c in range(3)]
        fields += [lambda c=c: both(m0[c, 0], m1[c, 0]) for c in range(3)]
        choices = []
        for (first, slots, depth), pol in zip(parts, pols):
            inside = None
            if len(pols) > 1:
                block = jnp.clip(layer, 0, radial - 1) // depth
                place = (block - starts[2]) * starts[3] - first
                inside = (place >= 0) & (place < slots)
            choices.append((pol, inside))
    mine = None if ghosts is None else (layer >= 0) & (layer < radial)
    for pol, inside in choices:
        def load(pol=pol):
            pieces = None if pol is None else [pol.at[c, 0, 0] for c in range(4)]
            fill(fields, pieces, side_low.at[0], side_high.at[0])

        cond = mine if inside is None else inside if mine is None else mine & inside
        if cond is None:
            load()
        else:
            pl.when(cond)(load)
    if ghosts is not None:
        @pl.when(jnp.logical_not(mine))
        def _():
            planes = [lambda r=r: r[0] for r in ghosts[:7]]
            pieces = [r.at[0] for r in ghosts[9:]]
            fill(planes, pieces, ghosts[7].at[0], ghosts[8].at[0])

    shape = (TILE, width)
    lane = lax.broadcasted_iota(jnp.int32, shape, 1)
    sub = lax.broadcasted_iota(jnp.int32, shape, 0)

    def shifted(ref, index, base, off):
        here = ref[index, pl.ds(base, TILE), :]
        if off > 0:
            other = ref[index, pl.ds(base + TILE, TILE), :]
            return pltpu.roll(jnp.where(sub < off, other, here), TILE - off, 0)
        if off < 0:
            other = ref[index, pl.ds(base - TILE, TILE), :]
            return pltpu.roll(jnp.where(sub >= TILE + off, other, here), -off, 0)
        return here

    def at(ref, d, base, off=0):
        return shifted(ref, lax.rem(t - 3 + d + 8, 8), base, off)

    def up(x):
        rolled = pltpu.roll(x, width - 1, 1)
        return rolled if middle else jnp.where(lane == width - 1, x, rolled)

    def down(x):
        rolled = pltpu.roll(x, 1, 1)
        return rolled if middle else jnp.where(lane == 0, x, rolled)

    def before(x, previous):
        return jnp.where(sub == 0, pltpu.roll(previous, 1, 0), pltpu.roll(x, 1, 0))

    def azimuth_step(base, carry):
        rights, lefts, kept = [], [], []
        for field, past_face, past_right in ((s0, carry[0], carry[2]), (s3, carry[1], carry[3])):
            q = [at(field, 0, base, o) for o in (-1, 0, 1, 2)]
            face = interface_value(*q)
            left, right = limited(q[1], before(face, past_face), face)
            rights.append(before(right, past_right))
            lefts.append(left)
            kept.append((face, right))
        flux = hll_flux(rights[0], lefts[0], rights[1], lefts[1])
        return (kept[0][0], kept[1][0], kept[0][1], kept[1][1]), flux

    def theta_edges(q):
        below = down(q)
        face = interface_value(down(below), below, q, up(q))
        rolled = pltpu.roll(face, width - 1, 1)
        above = rolled if middle else jnp.where(lane == width - 1, q, rolled)
        return limited(q, face, above)

    here = lax.rem(t, 4)

    def emf_tile(j, _):
        base = pl.multiple_of(FRONT - TILE + j * TILE, TILE)
        u_r, u_t, u_p = (at(s, 1, base) for s in (s1, s2, s3))
        b_r = at(s4, 1, base) + at(s4, 2, base)
        b_t = at(s5, 1, base)
        b_t = b_t + up(b_t)
        b_p = at(s6, 1, base) + at(s6, 1, base, 1)
        rows = pl.ds(base, TILE)
        er[here, rows, :] = u_p * b_t - u_t * b_p
        et[here, rows, :] = u_r * b_p - u_p * b_r
        ep[here, rows, :] = u_t * b_r - u_r * b_t
        return 0

    @pl.when(t >= 4)
    def _():
        lax.fori_loop(0, azimuth // TILE + 2, emf_tile, 0, unroll=math.gcd(azimuth // TILE + 2, 6))

    def emf(ref, d, base, off=0):
        return shifted(ref, lax.rem(t - 1 + d + 4, 4), base, off)

    def radial_face(field, base):
        return interface_value(*(at(field, d, base) for d in (0, 1, 2, 3)))

    def radial_step(rows, base):
        face_rho, face_u = radial_face(s0, base), radial_face(s1, base)
        left_r, right_r = limited(at(s0, 1, base), face_of_rho[rows, :], face_rho)
        left_u, right_v = limited(at(s1, 1, base), face_of_u[rows, :], face_u)
        flux = hll_flux(carry_rho[rows, :], left_r, carry_u[rows, :], left_u)
        total = COURANT_RAD * (flux - carry_flux[rows, :])
        face_of_rho[rows, :] = face_rho
        face_of_u[rows, :] = face_u
        carry_rho[rows, :] = right_r
        carry_u[rows, :] = right_v
        carry_flux[rows, :] = flux
        return total

    def put(ref, index, rows, value, mid):
        if middle:
            ref[index + (rows, slice(None))] = value
            return
        inner = width + NPOL
        keep = lax.broadcasted_iota(jnp.int32, (TILE, NPOL), 1)
        mixed = mid[:, inner - NPOL :]
        quarter = half // 2
        first = jnp.where(keep < half + quarter, value[:, :NPOL], mixed)
        last = jnp.where(keep >= quarter, value[:, NPOL:], mixed)
        ref[index + (rows, slice(0, NPOL))] = first
        ref[index + (rows, slice(NPOL, inner))] = mid[:, : inner - NPOL]
        ref[index + (rows, slice(inner, inner + NPOL))] = last

    def middle_of(rows, c=None):
        if middle:
            return None
        return mid_dens[0, rows, :] if c is None else mid_mag[c, 0, rows, :]

    def tile(j, carry):
        kept, flux_low = carry
        start = pl.multiple_of(j * TILE, TILE)
        base = pl.multiple_of(FRONT + j * TILE, TILE)
        rows = pl.ds(start, TILE)

        total = radial_step(rows, base)

        kept, flux = azimuth_step(base + TILE, kept)
        flux_high = pltpu.roll(jnp.where(sub < 1, flux, flux_low), TILE - 1, 0)
        total = total + COURANT_AZI * (flux_high - flux_low)
        flux_low = flux

        rho = at(s0, 0, base)
        left_r, right_r = theta_edges(rho)
        left_u, right_v = theta_edges(at(s2, 0, base))
        theta_flux = hll_flux(down(right_r), left_r, down(right_v), left_u)
        if not middle:
            theta_flux = jnp.where(lane == 0, 0.0, theta_flux)
        above = pltpu.roll(theta_flux, width - 1, 1)
        if not middle:
            above = jnp.where(lane == width - 1, 0.0, above)
        total = total + COURANT_POL * (above - theta_flux)
        put(dens_out, (0,), rows, rho - total, middle_of(rows))

        er_low, er_here, er_high = (emf(er, 0, base, o) for o in (-1, 0, 1))
        ep_low, ep_here, ep_high = (emf(ep, d, base) for d in (-1, 0, 1))
        below_k = emf(et, -1, base, -1)
        edge_a = ep_low + ep_here
        edge_r = er_low + er_here
        mixed = (0.125 * COURANT_RAD) * (ep_high - ep_low) - (0.125 * COURANT_AZI) * (er_high - er_low)
        across = emf(et, -1, base, 1) + emf(et, 0, base, 1) - below_k - emf(et, 0, base, -1)
        along = emf(et, 1, base, -1) + emf(et, 1, base) - below_k - emf(et, -1, base)
        put(mag_out, (0, 0), rows,
            at(s4, 0, base)
            - (0.125 * COURANT_POL) * (up(edge_a) - down(edge_a))
            + (0.125 * COURANT_AZI) * across, middle_of(rows, 0))
        put(mag_out, (1, 0), rows, at(s5, 0, base) + (down(mixed) + mixed), middle_of(rows, 1))
        put(mag_out, (2, 0), rows,
            at(s6, 0, base)
            - (0.125 * COURANT_RAD) * along
            + (0.125 * COURANT_POL) * (up(edge_r) - down(edge_r)), middle_of(rows, 2))
        return kept, flux_low

    @pl.when(t == 3)
    def _():
        def warm_face(j, _):
            rows = pl.ds(pl.multiple_of(j * TILE, TILE), TILE)
            base = pl.multiple_of(FRONT + j * TILE, TILE)
            face_of_rho[rows, :] = radial_face(s0, base)
            face_of_u[rows, :] = radial_face(s1, base)
            return 0

        lax.fori_loop(0, azimuth // TILE, warm_face, 0, unroll=2)

    @pl.when((t >= 4) & (t < 6))
    def _():
        def warm(j, _):
            start = pl.multiple_of(j * TILE, TILE)
            radial_step(pl.ds(start, TILE), pl.multiple_of(FRONT + j * TILE, TILE))
            return 0

        lax.fori_loop(0, azimuth // TILE, warm, 0, unroll=2)

    @pl.when(t >= 6)
    def _():
        zero = jnp.zeros(shape, jnp.float32)
        kept, _ = azimuth_step(FRONT - TILE, (zero, zero, zero, zero))
        first = azimuth_step(FRONT, kept)
        unroll = math.gcd(azimuth // TILE, 4 if middle else 8)
        lax.fori_loop(0, azimuth // TILE, tile, first, unroll=unroll)


def stencil(middle, count, starts, fields, sides, ghosts=None, polar=None, mids=None, into=None):
    density, velocity, magnetic = fields
    radial, azimuth, width = density.shape
    tiles = width // NPOL

    def own(t, s):
        return jnp.clip(s[0] + t - 3, 0, radial - 1)

    def out(t, s):
        return s[1] + jnp.clip(t - 6, 0, count - 1)

    def one(w, index=0):
        return pl.BlockSpec((1, azimuth, w), lambda t, s: (own(t, s), 0, index))

    def three(w, index=0):
        return pl.BlockSpec((3, 1, azimuth, w), lambda t, s: (0, own(t, s), 0, index))

    def deep(t, s):
        g = s[0] + t - 3
        return jnp.clip(jnp.where(g < 0, g + 3, g - radial), 0, 2)

    def two(t, s):
        g = s[0] + t - 3
        return jnp.clip(jnp.where(g < 0, g + 2, g - radial), 0, 1)

    side = pl.BlockSpec((1, PACKED, width), lambda t, s: (own(t, s), 0, 0))
    parts = []
    if middle:
        ring = width - NPOL
        out_width = ring
        args = [density, velocity, magnetic, *sides]
        specs = [one(width), three(width), three(width), side, side]
    else:
        ring = 2 * NPOL
        out_width = width
        parts = [(first, p.shape[2], p.shape[1]) for first, p in polar]
        polar = [p for _, p in polar]
        args = [density, density, velocity, velocity, magnetic, magnetic, *polar, *sides, *mids]
        specs = [one(NPOL), one(NPOL, tiles - 1), three(NPOL), three(NPOL, tiles - 1),
                 three(NPOL), three(NPOL, tiles - 1)]

        def place(t, s, part):
            first, slots, depth = part
            block = own(t, s) // depth
            return jnp.clip((block - s[2]) * s[3] - first, 0, slots - 1)

        for part in parts:
            specs.append(pl.BlockSpec(
                (4, 1, 1, azimuth + HALO, NPOL),
                lambda t, s, part=part: (0, own(t, s) % part[2], place(t, s, part), 0, 0)))
        specs += [side, side]
        mid_width = width - NPOL
        specs += [pl.BlockSpec((1, azimuth, mid_width), lambda t, s: (out(t, s), 0, 0)),
                  pl.BlockSpec((3, 1, azimuth, mid_width), lambda t, s: (0, out(t, s), 0, 0))]
    used = len(args)
    extra = 0
    if ghosts is not None:
        planes, corner, filtered = ghosts
        where = [lambda t, s: deep(t, s), lambda t, s: 3 + deep(t, s), lambda t, s: 6, lambda t, s: 7]
        index = where + [lambda t, s: 8 + two(t, s), lambda t, s: 10, lambda t, s: 11]
        for f in index:
            args.append(planes)
            specs.append(pl.BlockSpec((1, azimuth, width), lambda t, s, f=f: (f(t, s), 0, 0)))
        for first in (0, 2):
            args.append(corner)
            specs.append(pl.BlockSpec(
                (1, PACKED, width), lambda t, s, first=first: (first + two(t, s), 0, 0)))
        if filtered is not None:
            for f in where:
                args.append(filtered)
                specs.append(pl.BlockSpec(
                    (1, azimuth + HALO, NPOL), lambda t, s, f=f: (f(t, s), 0, 0)))
        extra = len(args) - used
    aliases = {}
    if into is not None:
        for i, x in enumerate(into):
            aliases[1 + len(args)] = i
            args.append(x)
            specs.append(pl.BlockSpec(memory_space=pl.ANY))

    def kernel(starts, *refs):
        ins, outs, scratch = refs[:used], refs[len(args) : len(args) + 2], refs[len(args) + 2 :]
        spare = refs[used : used + extra] if extra else None
        if not middle:
            n = len(polar)
            ins = ins[:6] + (ins[6 : 6 + n],) + ins[6 + n :]
        stencil_kernel(middle, radial, azimuth, parts, starts, ins, spare, outs, scratch)

    rows = FRONT + azimuth + 2 * TILE
    scratch = (
        [pltpu.VMEM((8, rows, ring), jnp.float32)] * 7
        + [pltpu.VMEM((4, rows, ring), jnp.float32)] * 3
        + [pltpu.VMEM((azimuth, ring), jnp.float32)] * 5
    )
    return pl.pallas_call(
        kernel,
        grid_spec=pltpu.PrefetchScalarGridSpec(
            num_scalar_prefetch=1,
            grid=(count + 6,),
            in_specs=specs,
            out_specs=[
                pl.BlockSpec((1, azimuth, out_width), lambda t, s: (out(t, s), 0, 0)),
                pl.BlockSpec((3, 1, azimuth, out_width), lambda t, s: (0, out(t, s), 0, 0)),
            ],
            scratch_shapes=scratch,
        ),
        out_shape=[
            jax.ShapeDtypeStruct((radial, azimuth, out_width), jnp.float32),
            jax.ShapeDtypeStruct((3, radial, azimuth, out_width), jnp.float32),
        ],
        input_output_aliases=aliases,
        compiler_params=pltpu.CompilerParams(
            dimension_semantics=("arbitrary",), vmem_limit_bytes=62 * 1024 * 1024
        ),
        cost_estimate=pl.CostEstimate(
            flops=1000 * count * azimuth * ring, bytes_accessed=48 * count * azimuth * width,
            transcendentals=0,
        ),
        name="section_mid" if middle else "section_polar",
    )(starts, *args)


def swap_rows(x):
    return lax.ppermute(x, "row", [(0, 1), (1, 0)])


def section(density, velocity, magnetic):
    radial, azimuth, width = density.shape
    devices = lax.axis_size("phi")
    pairs = 4 * radial // devices
    depth = radial // pairs
    sent = [(0, pairs - 1), (pairs - 1, 1)] if pairs > 1 else [(0, 1)]
    returned = [(0, 1)]
    if pairs > 2:
        returned.append((1, pairs - 2))
    if pairs > 1:
        returned.append((pairs - 1, 1))
    split = pairs > 1
    low = lax.axis_index("row") == 0
    fields = (density, velocity, magnetic)

    def pick(a, b):
        return jnp.where(low, jnp.int32(a), jnp.int32(b))

    def transpose(x, share, rows):
        x = x.reshape(devices, share, rows, NPOL)
        return lax.all_to_all(x, "phi", split_axis=0, concat_axis=0, tiled=True)

    order = jnp.stack([pick(pairs - 1, 0), pick(-1, 1)])
    packed = [pack_lines(density, velocity, order, a, n, depth) for a, n in sent]
    first_rows, last_rows = pack_sides(density, velocity, magnetic)

    far, near, pair = pick(radial - 3, 0), pick(radial - 1, 0), pick(radial - 2, 0)

    def plane(x, c, n, start, size):
        return lax.dynamic_slice(x, (c, start, 0, 0), (n, size, azimuth, width)).reshape(
            n * size, azimuth, width)

    planes = jnp.concatenate(
        [lax.dynamic_slice_in_dim(density, far, 3, 0), plane(velocity, 0, 1, far, 3),
         plane(velocity, 1, 2, near, 1), plane(magnetic, 0, 1, pair, 2),
         plane(magnetic, 1, 2, near, 1)], axis=0)
    around = [(i, (i + 1) % devices) for i in range(devices)]
    back = [(j, i) for i, j in around]

    side_low = lax.ppermute(last_rows, "phi", around)
    side_high = lax.ppermute(first_rows, "phi", back)
    sides = (side_low, side_high)
    lines = [transpose(packed[0], sent[0][1], azimuth)]
    planes = swap_rows(planes)

    def starts(s):
        return jnp.concatenate([jnp.stack([s, s]), order])

    deep = radial - REACH
    mids = stencil(True, deep, starts(pick(0, REACH)), fields, sides)
    if split:
        packed[1], mids = lax.optimization_barrier((packed[1], tuple(mids)))
        lines.append(transpose(packed[1], sent[1][1], azimuth))
    corner = swap_rows(
        jnp.concatenate([lax.dynamic_slice_in_dim(x, pair, 2, 0) for x in sides], axis=0))

    smooth = [filter_lines(lines[0], a, n, width) for a, n in returned[: max(1, len(returned) - 1)]]
    if split:
        smooth.append(filter_lines(lines[1], 0, 1, width))
    mids = stencil(True, REACH, starts(pick(deep, 0)), fields, sides,
                   ghosts=(planes, corner, None), into=mids)
    polar = []
    for i, (a, n) in enumerate(returned):
        if i + 1 < len(returned):
            smooth[i], smooth[i + 1] = lax.optimization_barrier((smooth[i], smooth[i + 1]))
        elif i > 0:
            smooth[i], mids = lax.optimization_barrier((smooth[i], tuple(mids)))
        back_again = transpose(smooth[i], n, azimuth + HALO)
        polar.append((a, back_again.reshape(4, depth, n, azimuth + HALO, NPOL)))

    first = polar[0][1][:, :, 0]
    far, near = pick(depth - 3, 0), pick(depth - 1, 0)
    ends = lax.dynamic_slice_in_dim(first[:2], far, 3, 1).reshape(6, azimuth + HALO, NPOL)
    close = lax.dynamic_slice_in_dim(first[2:], near, 1, 1).reshape(2, azimuth + HALO, NPOL)
    filtered = swap_rows(jnp.concatenate([ends, close], axis=0))

    edge = depth * sent[0][1] - REACH
    early = polar[:-1] if split else polar
    out = stencil(False, edge, starts(pick(radial - edge, 0)), fields, sides,
                  ghosts=(planes, corner, filtered), polar=early, mids=mids)
    if split:
        late, out = lax.optimization_barrier((polar[-1][1], tuple(out)))
        polar[-1] = (polar[-1][0], late)
    out = stencil(False, radial - edge, starts(pick(0, edge)), fields, sides, polar=polar,
                  mids=mids, into=out)
    return tuple(out)


def solution(mesh):
    placed = (P("row", "phi", None), P(None, "row", "phi", None), P(None, "row", "phi", None))
    return jax.shard_map(
        section,
        mesh=mesh,
        in_specs=placed,
        out_specs=(P("row", "phi", None), P(None, "row", "phi", None)),
        check_vma=False,
    )
```
